32 devices in a mesh: gx: 4 (over y, x), gy: 2 (over core), gz: 4 (over z).
Axes of the slice: x: 2, y: 2, z: 4, core: 2. Of those that a mesh axis runs over, the one named last changes fastest.
Arguments:
- data: float32 [128, 64, 512], P('gx', 'gy', 'gz'), may hold values from -120 to 120
- weights: float32 [8, 512], P(None, 'gz'), may hold values from -3 to 3
Outputs:
- solution: float32 [128, 64, 512], P('gx', 'gy', 'gz')
- residual: float32 [128, 64, 512], P('gx', 'gy', 'gz')
- norms: float32 [4], replicated
The draws below stay inside these ranges and needn't reach their ends.
All inputs are finite; a program needn't handle non-finite values.
Results may differ from the reference program's by a relative error of at most 0.0001.
Values sent between devices are 32-bit elements; how exact they have to be, the bound alone decides.
A program may use at most 128 MiB of HBM per device.

```python
import math
import jax
import jax.numpy as jnp
from jax import lax

HALF = 4
BAND = 8
NX = 128
NY = 64
NZ = 512


def draw_data(key, part):
    key_x, key_y, key_z, key_n = jax.random.split(key, 4)
    reach = math.log(10.0) / 3.0
    along_x = jnp.exp(jax.random.uniform(key_x, (NX,), jnp.float32, 0.0, reach)) * 3.0 ** (jnp.arange(NX, dtype=jnp.float32) / NX)
    along_y = jnp.exp(jax.random.uniform(key_y, (NY,), jnp.float32, 0.0, reach)) * 3.0 ** (jnp.arange(NY, dtype=jnp.float32) / NY)
    along_z = jnp.exp(jax.random.uniform(key_z, (NZ,), jnp.float32, 0.0, reach)) * 3.0 ** (jnp.arange(NZ, dtype=jnp.float32) / NZ)
    scales = along_x[:, None, None] * along_y[None, :, None] * along_z[None, None, :] / 15.0
    base = jnp.clip(jax.random.normal(key_n, (NX, NY, NZ), jnp.float32), -6.0, 6.0)
    return (base * scales).astype(jnp.float32)


def block_levels(own_key, dims, cuts, low, top_value):
    factor_of, own = 1.0, jax.random.fold_in(own_key, 6)
    for position, parts in cuts:
        steps = jnp.exp(jax.random.uniform(jax.random.fold_in(own, position), (parts,), jnp.float32, low / len(cuts), top_value / len(cuts)))
        factor_of = factor_of * jnp.repeat(steps, dims[position] // parts).reshape([-1 if axis == position else 1 for axis in range(len(dims))])
    return factor_of


def normal_values(own_key, dims, scale, bound, cuts=(), kind=jnp.bfloat16):
    factor_of = block_levels(own_key, dims, cuts, -0.22, 0.18) if cuts else 1.0
    values = jax.random.normal(own_key, dims, jnp.float32) * scale * factor_of
    return jnp.minimum(jnp.maximum(values, -bound), bound).astype(kind)


def setup_inputs(seed: int = 0) -> dict:
    keys = jax.random.split(jax.random.key(seed), 3)
    return {
        "data": draw_data(jax.random.fold_in(keys[2], 71), 0),
        "weights": normal_values(keys[1], (BAND, NZ), 0.2, 3.0, ((1, 4),), jnp.float32),
    }


relaxation = 0.45

def band_offsets():
    return [j - HALF for j in range(HALF)] + [j - HALF + 1 for j in range(HALF, 2 * HALF)]

def forward_band(padded, weights):
    count = weights.shape[1]
    result = padded[:, :, HALF:HALF + count]
    for j, offset in enumerate(band_offsets()):
        result = result + weights[j][None, None, :] * padded[:, :, HALF + offset:HALF + offset + count]
    return result

def backward_band(padded, transposed):
    count = transposed.shape[1]
    result = padded[:, :, HALF:HALF + count]
    for j, offset in enumerate(band_offsets()):
        result = result + transposed[j][None, None, :] * padded[:, :, HALF - offset:HALF - offset + count]
    return result

def transposed_weights(padded, count):
    return jnp.stack([padded[j, HALF - offset:HALF - offset + count] for j, offset in enumerate(band_offsets())])

def neighbours(padded, width, shape):

    def part(a, b, c):
        return padded[width + a:width + a + shape[0], width + b:width + b + shape[1], width + c:width + c + shape[2]]
    return part(1, 0, 0) + part(-1, 0, 0) + part(0, 1, 0) + part(0, -1, 0) + part(0, 0, 1) + part(0, 0, -1)

def combine(field, back, near, stiffness):
    return back + stiffness * (6.0 * field - near)

def diagonal_of(transposed, stiffness):
    return 1.0 + lax.optimization_barrier(jnp.sum(transposed * transposed, axis=0)) + 6.0 * stiffness

def coarsen(weights):
    return 0.5 * (weights[:, 0::2] + weights[:, 1::2])

def restrict_dim(padded, dim):
    half_count = (padded.shape[dim] - 2) // 2
    s0 = jax.lax.slice_in_dim(padded, 0, 2 * half_count - 1, 2, dim)
    s1 = jax.lax.slice_in_dim(padded, 1, 2 * half_count, 2, dim)
    s2 = jax.lax.slice_in_dim(padded, 2, 2 * half_count + 1, 2, dim)
    s3 = jax.lax.slice_in_dim(padded, 3, 2 * half_count + 2, 2, dim)
    return (s0 + 3.0 * s1 + 3.0 * s2 + s3) * 0.125

def prolong_dim(padded, dim):
    count = padded.shape[dim] - 2
    below = jax.lax.slice_in_dim(padded, 0, count, 1, dim)
    centre = jax.lax.slice_in_dim(padded, 1, count + 1, 1, dim)
    above = jax.lax.slice_in_dim(padded, 2, count + 2, 1, dim)
    even = 0.75 * centre + 0.25 * below
    odd = 0.75 * centre + 0.25 * above
    joined = jnp.stack([even, odd], dim + 1)
    shape = list(centre.shape)
    shape[dim] = 2 * count
    return joined.reshape(shape)

def restrict_all(padded):
    for dim in range(3):
        padded = restrict_dim(padded, dim)
    return padded

def prolong_all(padded):
    for dim in range(3):
        padded = prolong_dim(padded, dim)
    return padded

def zpad(field):
    return jnp.pad(field, ((0, 0), (0, 0), (HALF, HALF)))

def whole_transposed(weights):
    return transposed_weights(jnp.pad(weights, ((0, 0), (HALF, HALF))), weights.shape[1])

def whole_operate(field, weights, transposed, stiffness):
    back = backward_band(zpad(forward_band(zpad(field), weights)), transposed)
    near = neighbours(jnp.pad(field, 1), 1, field.shape)
    return combine(field, back, near, stiffness)

def sweep(error, right, apply_fn, diag):
    return error + relaxation * (right - apply_fn(error)) / diag

def reference(data, weights):
    level_weights = [weights]
    for level in range(3):
        level_weights.append(coarsen(level_weights[-1]))
    level_trans = [whole_transposed(w) for w in level_weights]
    rhs = backward_band(zpad(data), level_trans[0])
    right = rhs
    rights, errors, diags, totals = ([], [], [], [])
    for level in range(3):
        stiffness = 0.25 ** level
        diag = diagonal_of(level_trans[level], stiffness)
        apply_fn = partial_apply(level_weights[level], level_trans[level], stiffness)
        error = relaxation * right / diag
        error = sweep(error, right, apply_fn, diag)
        defect = right - apply_fn(error)
        totals.append(jnp.sum(defect * defect) / defect.size)
        rights.append(right)
        errors.append(error)
        diags.append(diag)
        right = restrict_all(jnp.pad(defect, 1))
    stiffness = 0.25 ** 3
    diag = diagonal_of(level_trans[3], stiffness)
    apply_fn = partial_apply(level_weights[3], level_trans[3], stiffness)
    coarse = relaxation * right / diag
    coarse = sweep(coarse, right, apply_fn, diag)
    for level in (2, 1, 0):
        apply_fn = partial_apply(level_weights[level], level_trans[level], 0.25 ** level)
        update = errors[level] + prolong_all(jnp.pad(coarse, 1))
        update = sweep(update, rights[level], apply_fn, diags[level])
        update = sweep(update, rights[level], apply_fn, diags[level])
        coarse = update
    solution = coarse
    residual = rhs - whole_operate(solution, level_weights[0], level_trans[0], 1.0)
    totals.append(jnp.sum(residual * residual) / residual.size)
    norms = jnp.sqrt(jnp.stack(totals))
    return (solution, residual, norms)

def partial_apply(weights, transposed, stiffness):

    def apply_fn(field):
        return whole_operate(field, weights, transposed, stiffness)
    return apply_fn
```

```python
import functools
import jax
import jax.numpy as jnp
from jax import lax
from jax.experimental import pallas as pl
from jax.experimental.pallas import tpu as pltpu
from jax.sharding import PartitionSpec as P

HALF = 4
RELAX = 0.45
F32 = jnp.float32
BF16 = jnp.bfloat16
HX = (4, 6)
OFFSETS = [j - HALF for j in range(HALF)] + [j - HALF + 1 for j in range(HALF, 2 * HALF)]


def iota(shape, dim):
    return lax.broadcasted_iota(jnp.int32, shape, dim)


def cyclic(index, size, own):
    cut = (size + own) // 2
    return jnp.where(index < cut, index, index - size)


def split(x):
    high = x.astype(BF16)
    return high, (x - high.astype(F32)).astype(BF16)


def dot(a, b):
    return lax.dot_general(a, b, (((1,), (0,)), ((), ())), preferred_element_type=F32)


def dot3(x, mh, ml):
    h, l = split(x)
    return dot(h, mh) + dot(h, ml) + dot(l, mh)


def dot2(x, m):
    h, l = split(x)
    return dot(h, m) + dot(l, m)


def dot2l(m, x):
    h, l = split(x)
    return dot(m, h) + dot(m, l)


def restrict_matrix(fine, coarse, axis):
    k = fine - 2 * coarse + 1
    m = jnp.where((k == 0) | (k == 3), 0.125, jnp.where((k == 1) | (k == 2), 0.375, 0.0))
    return m.astype(F32)


def prolong_matrix(fine, coarse, limit):
    centre = fine >> 1
    other = jnp.where((fine & 1) == 1, centre + 1, centre - 1)
    m = jnp.where(coarse == centre, 0.75, jnp.where(coarse == other, 0.25, 0.0))
    return jnp.where((fine >= 0) & (fine < limit), m, 0.0).astype(F32)


def build_matrices(nz, whole, wall, *outs):
    z0 = lax.axis_index("gz") * nz
    for level in range(4):
        own = nz >> level
        total = whole >> level
        size = 2 * nz if level < 2 else total
        base = z0 >> level if level < 2 else 0

        def place(index):
            return cyclic(index, size, own) if level < 2 else index

        g = iota((whole, size), 0) >> level
        p = place(iota((whole, size), 1)) + base
        pick = jnp.where(g == p, 0.5**level, 0.0).astype(F32)
        w = lax.dot_general(
            wall, pick, (((1,), (0,)), ((), ())),
            preferred_element_type=F32, precision=lax.Precision.HIGHEST,
        )
        pr = place(iota((size, size), 0))
        pc = place(iota((size, size), 1))
        ok = (pr + base >= 0) & (pr + base < total) & (pc + base >= 0) & (pc + base < total)
        diff = pr - pc
        at = jnp.where(diff == 0, 1.0, 0.0).astype(F32)
        for j, offset in enumerate(OFFSETS):
            at = at + jnp.where(diff == offset, w[j : j + 1, :], 0.0)
        at = jnp.where(ok, at, 0.0)
        a = at.T
        stiff = 0.25**level
        m = lax.dot_general(
            at, a, (((1,), (0,)), ((), ())),
            preferred_element_type=F32, precision=lax.Precision.HIGHEST,
        )
        lap = jnp.where(diff == 0, 6.0, jnp.where((diff == 1) | (diff == -1), -1.0, 0.0))
        m = m + jnp.where(ok, stiff * lap, 0.0)
        d = jnp.sum(jnp.where(diff == 0, m, 0.0), axis=0, keepdims=True)
        col = place(iota((1, size), 1)) + base
        inside = (col >= 0) & (col < total)
        safe = jnp.where(inside, d, 1.0)
        c = jnp.where(inside, RELAX / safe, 0.0)
        inv = jnp.where(inside, safe * (1.0 / RELAX), 0.0)
        mh, ml = split(m * c)
        o = outs[3 * level : 3 * level + 3]
        o[0][...] = mh
        o[1][...] = ml
        o[2][0:1, :] = c
        o[2][1:2, :] = inv
        if level == 0:
            ah, al = split(a)
            outs[12][...] = ah
            outs[13][...] = al


def chunk_of(count, rows, most):
    best = 1
    for planes in range(1, count + 1):
        if count % planes == 0 and planes * rows <= most:
            best = planes
    return best


def sweep(src, r_at, emit, first, count, stiff, mats, xmask, ymask, init=None, own=None, most=800):
    mh, ml, cv = mats
    rows, size = src.shape[1], src.shape[2]
    planes = chunk_of(count, rows, most)
    keep, lanes = own or (rows, size)
    c = cv[0:1, 0:lanes]
    inv = cv[1:2, 0:lanes]
    yi = iota((rows, lanes), 0)

    def step(k, carry):
        x0 = first + k * planes
        u = src[pl.ds(x0, planes), 0:keep, :]
        um = dot3(u.reshape(planes * keep, size), mh[:, 0:lanes], ml[:, 0:lanes])
        for p in range(planes):
            x = x0 + p
            uc = src[x, :, 0:lanes]
            low = pltpu.roll(uc, 1, 0)
            high = pltpu.roll(uc, rows - 1, 0)
            if ymask is None:
                low = jnp.where(yi == 0, 0.0, low)
                high = jnp.where(yi == rows - 1, 0.0, high)
            side = src[x - 1, 0:keep, 0:lanes] + src[x + 1, 0:keep, 0:lanes]
            nb = side + (low + high)[0:keep]
            if ymask is None:
                nb = nb * stiff
            else:
                nb = nb * (ymask[0:keep, 0:lanes] * (xmask(x) * stiff))
            delta = c * (r_at(x)[0:keep, 0:lanes] + nb) - um[p * keep : (p + 1) * keep]
            carry = emit(x, uc[0:keep], delta, inv, carry)
        return carry

    return lax.fori_loop(0, count // planes, step, init)


def restrict(gz, first, count, ry, out, lanes):
    group = chunk_of(count, 1, 8)

    def step(k, carry):
        values = []
        for j in range(group):
            x = first + 2 * (k * group + j)
            t = (gz[x - 1] + 3.0 * gz[x] + 3.0 * gz[x + 1] + gz[x + 2]) * 0.125
            values.append(dot2l(ry, t))
        for j in range(group):
            out(k * group + j, values[j])
        return carry

    lax.fori_loop(0, count // group, step, 0)


def inside_mask(base, limit, pad):
    def mask(x):
        g = base + x - pad
        return jnp.where((g >= 0) & (g < limit), 1.0, 0.0).astype(F32)

    return mask


def y_mask(rows, size, own, base, limit):
    y = cyclic(iota((rows, size), 0), rows, own) + base
    return jnp.where((y >= 0) & (y < limit), 1.0, 0.0).astype(F32)


def zero_planes(ref, *planes):
    for x in planes:
        ref[x] = jnp.zeros(ref.shape[1:], F32)


def geometry(level, dims):
    nx, ny, nz = (v >> level for v in dims)
    gx, gy = lax.axis_size("gx"), lax.axis_size("gy")
    return dict(
        nx=nx, ny=ny, nz=nz, x0=lax.axis_index("gx") * nx, y0=lax.axis_index("gy") * ny,
        z0=lax.axis_index("gz") * nz, NX=nx * gx, NY=ny * gy, NZ=nz * lax.axis_size("gz"),
    )


def down_kernel(level, dims, *refs):
    if level == 0:
        ext, ah, al, mh, ml, cv, rhs, eb, r_next, part, ua, gz = refs
    else:
        rhs, mh, ml, cv, eb, r_next, part, ua, gz = refs
    geo = geometry(level, dims)
    nx, ny, nz = geo["nx"], geo["ny"], geo["nz"]
    hx = HX[level]
    count = nx + 2 * hx
    rows, size = ua.shape[1], ua.shape[2]
    pad = hx + 1
    c = cv[0:1, :]
    zero_planes(ua, 0, count + 1)
    reach = hx - 1 - level
    zero_planes(eb, *range(pad - reach), *range(pad + nx + reach, count + 2))
    if level == 0:
        planes = chunk_of(count, rows, 448)

        def first(k, carry):
            x0 = k * planes
            r = dot3(ext[pl.ds(x0, planes)].reshape(planes * rows, size), ah[...], al[...])
            for p in range(planes):
                rp = r[p * rows : (p + 1) * rows]
                rhs[x0 + p] = rp
                ua[x0 + p + 1] = c * rp
            return carry

        lax.fori_loop(0, count // planes, first, 0)
    else:

        def first(x, carry):
            ua[x + 1] = c * rhs[x]
            return carry

        lax.fori_loop(0, count, first, 0)
    xmask = inside_mask(geo["x0"], geo["NX"], pad)
    ymask = y_mask(rows, size, ny, geo["y0"], geo["NY"])
    mats = (mh, ml, cv)
    stiff = 0.25**level

    def r_at(x):
        return rhs[x - 1]

    def keep(x, u, delta, inv, carry):
        eb[x] = u + delta
        return carry

    sweep(ua, r_at, keep, pad - reach, nx + 2 * reach, stiff, mats, xmask, ymask, 0)
    lanes = gz.shape[2]
    fine = cyclic(iota((size, lanes), 0), size, nz)
    coarse = iota((size, lanes), 1)
    rz = jnp.where(coarse < nz // 2, restrict_matrix(fine, coarse, 0), 0.0).astype(BF16)
    ry = restrict_matrix(
        cyclic(iota((ny // 2, rows), 1), rows, ny), iota((ny // 2, rows), 0), 1
    ).astype(BF16)

    def defect(x, u, delta, inv, carry):
        g = delta * inv
        gz[x] = dot2(g, rz)
        mine = g[0:ny, 0:nz]
        return carry + mine * mine * jnp.where((x >= pad) & (x < pad + nx), 1.0, 0.0).astype(F32)

    total = sweep(
        eb, r_at, defect, pad - 1, nx + 2, stiff, mats, xmask, ymask, jnp.zeros((ny, nz), F32)
    )
    part[...] = jnp.full(part.shape, jnp.sum(total), F32)

    def put(i, value):
        r_next[i] = value

    restrict(gz, pad, nx // 2, ry, put, lanes)


def prolong_into(coarse_ref, coarse_first, coarse_count, pz, py, buf, error, dst, xmask):
    group = chunk_of(coarse_count, 1, 11)
    rows, size = coarse_ref.shape[1:]

    def step(k, carry):
        z = coarse_ref[pl.ds(coarse_first + k * group, group)]
        z = dot2(z.reshape(group * rows, size), pz)
        values = [dot2l(py, z[j * rows : (j + 1) * rows]) for j in range(group)]
        for j in range(group):
            buf[k * group + j] = values[j]
        return carry

    lax.fori_loop(0, coarse_count // group, step, 0)

    def join(i, carry):
        x = 1 + 2 * (i - 1)
        mid = 0.75 * buf[i]
        dst[x] = error(x) + xmask(x) * (mid + 0.25 * buf[i - 1])
        dst[x + 1] = error(x + 1) + xmask(x + 1) * (mid + 0.25 * buf[i + 1])
        return carry

    lax.fori_loop(1, coarse_count - 1, join, 0)


def coarse_kernel(dims, r2, m2h, m2l, c2, m3h, m3l, c3, u2, part, ua, ub, gz, r3, e3a, e3b, buf):
    g2 = geometry(2, dims)
    g3 = geometry(3, dims)
    N2, N3 = g2["NX"], g3["NX"]
    pad = 4
    one = lambda x: 1.0
    for ref in (ua, ub):
        zero_planes(ref, 0, N2 + 1)
    zero_planes(e3a, 0, N3 + 1)
    zero_planes(e3b, 0, N3 + 1)
    zero_planes(gz, 0, N2 + 1)
    zero_planes(u2, *range(pad), *range(N2 + pad, N2 + 2 * pad))
    mats2, mats3 = (m2h, m2l, c2), (m3h, m3l, c3)
    cc = c2[0:1, :]

    def first(x, carry):
        ua[x + 1] = cc * r2[x]
        return carry

    lax.fori_loop(0, N2, first, 0)
    r_at = lambda x: r2[x - 1]

    def into(ref, shift=0):
        def emit(x, u, delta, inv, carry):
            ref[x + shift] = u + delta
            return carry

        return emit

    s2, s3 = 0.25**2, 0.25**3
    sweep(ua, r_at, into(ub), 1, N2, s2, mats2, one, None, 0)
    NY2, NZ2, NY3, NZ3 = g2["NY"], g2["NZ"], g3["NY"], g3["NZ"]
    rz = restrict_matrix(iota((NZ2, NZ3), 0), iota((NZ2, NZ3), 1), 0).astype(BF16)
    ry = restrict_matrix(iota((NY3, NY2), 1), iota((NY3, NY2), 0), 1).astype(BF16)

    def defect(x, u, delta, inv, carry):
        g = delta * inv
        gz[x] = dot2(g, rz)
        return carry + g * g

    total = sweep(ub, r_at, defect, 1, N2, s2, mats2, one, None, jnp.zeros((NY2, NZ2), F32))
    part[...] = jnp.full(part.shape, jnp.sum(total), F32)
    c3v = c3[0:1, :]

    def put(i, value):
        r3[i] = value
        e3a[i + 1] = c3v * value

    restrict(gz, 1, N3, ry, put, NZ3)
    sweep(e3a, lambda x: r3[x - 1], into(e3b), 1, N3, s3, mats3, one, None, 0)
    pz = prolong_matrix(iota((NZ3, NZ2), 1), iota((NZ3, NZ2), 0), NZ2).astype(BF16)
    py = prolong_matrix(iota((NY2, NY3), 0), iota((NY2, NY3), 1), NY2).astype(BF16)
    prolong_into(e3b, 0, N3 + 2, pz, py, buf, lambda x: ub[x], ua, one)
    sweep(ua, r_at, into(ub), 1, N2, s2, mats2, one, None, 0)
    sweep(ub, r_at, into(u2, pad - 1), 1, N2, s2, mats2, one, None, 0)


def up_kernel(dims, u2, r1, e1, m1h, m1l, c1, rhs, e0, m0h, m0l, c0, sol, res, part,
              va, vb, vbuf, ua, ub, ubuf):
    g0, g1, g2 = geometry(0, dims), geometry(1, dims), geometry(2, dims)
    rows, size = va.shape[1], va.shape[2]
    count = g1["nx"] + 2 * HX[1]
    zero_planes(va, 0, count + 1)
    zero_planes(vb, 0, count + 1)
    xmask = inside_mask(g1["x0"], g1["NX"], HX[1] + 1)
    ymask = y_mask(rows, size, g1["ny"], g1["y0"], g1["NY"])
    NY2, NZ2 = g2["NY"], g2["NZ"]
    pz = prolong_matrix(
        cyclic(iota((NZ2, size), 1), size, g1["nz"]) + g1["z0"], iota((NZ2, size), 0), g1["NZ"]
    ).astype(BF16)
    py = prolong_matrix(
        cyclic(iota((rows, NY2), 0), rows, g1["ny"]) + g1["y0"], iota((rows, NY2), 1), g1["NY"]
    ).astype(BF16)
    first = g2["x0"] + 4 - HX[1] // 2 - 1
    prolong_into(u2, first, count // 2 + 2, pz, py, vbuf, lambda x: e1[x], va, xmask)
    mats = (m1h, m1l, c1)

    def into(ref):
        def emit(x, u, delta, inv, carry):
            ref[x] = u + delta
            return carry

        return emit

    r1_at = lambda x: r1[x - 1]
    q, n1 = HX[1] + 1, g1["nx"]
    sweep(va, r1_at, into(vb), q - 3, n1 + 6, 0.25, mats, xmask, ymask, 0)
    sweep(vb, r1_at, into(va), q - 2, n1 + 4, 0.25, mats, xmask, ymask, 0)
    rows0, size0 = ua.shape[1], ua.shape[2]
    count0 = g0["nx"] + 2 * HX[0]
    nx, ny, nz = g0["nx"], g0["ny"], g0["nz"]
    pad = HX[0] + 1
    zero_planes(ua, 0, count0 + 1)
    zero_planes(ub, 0, count0 + 1)
    xmask0 = inside_mask(g0["x0"], g0["NX"], pad)
    ymask0 = y_mask(rows0, size0, ny, g0["y0"], g0["NY"])
    pz = prolong_matrix(
        cyclic(iota((size, size0), 1), size0, nz) + g0["z0"],
        cyclic(iota((size, size0), 0), size, g1["nz"]) + g1["z0"], g0["NZ"],
    ).astype(BF16)
    py = prolong_matrix(
        cyclic(iota((rows0, rows), 0), rows0, ny) + g0["y0"],
        cyclic(iota((rows0, rows), 1), rows, g1["ny"]) + g1["y0"], g0["NY"],
    ).astype(BF16)
    first = HX[1] + 1 - HX[0] // 2 - 1
    prolong_into(va, first, count0 // 2 + 2, pz, py, ubuf, lambda x: e0[x], ua, xmask0)
    mats0 = (m0h, m0l, c0)
    r0_at = lambda x: rhs[x - 1]
    sweep(ua, r0_at, into(ub), pad - 2, nx + 4, 1.0, mats0, xmask0, ymask0, 0)
    sweep(ub, r0_at, into(ua), pad - 1, nx + 2, 1.0, mats0, xmask0, ymask0, 0)

    def final(x, u, delta, inv, carry):
        g = delta * inv
        sol[x - pad] = u
        res[x - pad] = g
        return carry + g * g

    total = sweep(
        ua, r0_at, final, pad, nx, 1.0, mats0, xmask0, ymask0, jnp.zeros((ny, nz), F32), (ny, nz)
    )
    part[...] = jnp.full(part.shape, jnp.sum(total), F32)


AXES = ("gx", "gy", "gz")
MESH = pl.DeviceIdType.MESH
WIDTH = 40


class Pair:
    def __init__(self, axis, up, down, sends, recvs, slot):
        n, me = lax.axis_size(axis), lax.axis_index(axis)
        self.has_low, self.has_high = me > 0, me < n - 1

        def copy(refs, k, target):
            return pltpu.make_async_remote_copy(
                src_ref=refs[0], dst_ref=refs[1], send_sem=sends.at[k], recv_sem=recvs.at[k],
                device_id={axis: target}, device_id_type=MESH,
            )

        self.up = copy(up, slot, lax.rem(me + 1, n))
        self.down = copy(down, slot + 1, lax.rem(me + n - 1, n))

    def start(self):
        pl.when(self.has_high)(self.up.start)
        pl.when(self.has_low)(self.down.start)

    def wait(self):
        pl.when(self.has_low)(self.up.wait_recv)
        pl.when(self.has_high)(self.down.wait_recv)

    def sent(self):
        pl.when(self.has_high)(self.up.wait_send)
        pl.when(self.has_low)(self.down.wait_send)

    def clear(self, low, high):
        @pl.when(jnp.logical_not(self.has_low))
        def _():
            low[...] = jnp.zeros(low.shape, F32)

        @pl.when(jnp.logical_not(self.has_high))
        def _():
            high[...] = jnp.zeros(high.shape, F32)


def linear():
    gy, gz = lax.axis_size("gy"), lax.axis_size("gz")
    return (lax.axis_index("gx") * gy + lax.axis_index("gy")) * gz + lax.axis_index("gz")


def coordinates(t):
    gy, gz = lax.axis_size("gy"), lax.axis_size("gz")
    return (t // (gy * gz), lax.rem(t // gz, gy), lax.rem(t, gz))


def device_count():
    return lax.axis_size("gx") * lax.axis_size("gy") * lax.axis_size("gz")


def near_devices():
    out = []
    for axis, reach in (("gx", 1), ("gy", 1), ("gz", lax.axis_size("gz") - 1)):
        n, me = lax.axis_size(axis), lax.axis_index(axis)
        for d in range(1, reach + 1):
            out.append((me + d < n, {axis: lax.rem(me + d, n)}))
            out.append((me >= d, {axis: lax.rem(me + n - d, n)}))
    return out


def reached():
    return lax.axis_size("gx") <= 4 and lax.axis_size("gy") <= 2


def signal_all():
    n, me = device_count(), linear()
    barrier = pltpu.get_barrier_semaphore()
    if reached():
        for there, device in near_devices():

            @pl.when(there)
            def _():
                pl.semaphore_signal(barrier, inc=1, device_id=device, device_id_type=MESH)

        return

    def step(k, carry):
        pl.semaphore_signal(
            barrier, inc=1, device_id=coordinates(lax.rem(me + k, n)), device_id_type=MESH
        )
        return carry

    lax.fori_loop(1, n, step, 0)


def wait_all():
    if reached():
        count = sum(there.astype(jnp.int32) for there, _ in near_devices())
        pl.semaphore_wait(pltpu.get_barrier_semaphore(), count)
        return
    pl.semaphore_wait(pltpu.get_barrier_semaphore(), device_count() - 1)


def everyone(block, buf, sends, recvs):
    n, me = device_count(), linear()

    def copy(k, slot):
        return pltpu.make_async_remote_copy(
            src_ref=block, dst_ref=buf.at[slot], send_sem=sends.at[k], recv_sem=recvs.at[k],
            device_id=coordinates(lax.rem(me + k, n)), device_id_type=MESH,
        )

    def start(k, carry):
        copy(k, me).start()
        return carry

    def wait(k, carry):
        c = copy(k, lax.rem(me + n - k, n))
        c.wait_recv()
        c.wait_send()
        return carry

    lax.fori_loop(1, n, start, 0)
    buf[me] = block[...]
    lax.fori_loop(1, n, wait, 0)


def pack_faces(data, low, high):
    nx, ny, nz = data.shape
    slots = nz // WIDTH
    per = -(-nx // slots)
    rest = jnp.zeros((ny, nz - slots * WIDTH), F32)
    for i in range(per):
        planes = [min(k * per + i, nx - 1) for k in range(slots)]
        low[i] = jnp.concatenate([data[x][:, :WIDTH] for x in planes] + [rest], axis=1)
        high[i] = jnp.concatenate([data[x][:, nz - WIDTH :] for x in planes] + [rest], axis=1)


def unpack_faces(dims, from_low, from_high, ext, pad):
    nx, ny, nz = dims
    slots = nz // WIDTH
    per = -(-nx // slots)
    gap = jnp.zeros((ny, nz - 2 * WIDTH), F32)
    for x in range(nx):
        k, i = x // per, x % per
        part = slice(k * WIDTH, (k + 1) * WIDTH)
        ext[pad + x, 0:ny, nz:] = jnp.concatenate(
            [from_high[i][:, part], gap, from_low[i][:, part]], axis=1
        )


def gather_weights(weights, parts, sends, recvs):
    n, me = lax.axis_size("gz"), lax.axis_index("gz")

    def copy(k, slot):
        return pltpu.make_async_remote_copy(
            src_ref=weights, dst_ref=parts.at[slot], send_sem=sends.at[k], recv_sem=recvs.at[k],
            device_id={"gz": lax.rem(me + k, n)}, device_id_type=MESH,
        )

    for k in range(1, n):
        copy(k, me).start()

    def finish():
        parts[me] = weights[...]
        for k in range(1, n):
            c = copy(k, lax.rem(me + n - k, n))
            c.wait_recv()
            c.wait_send()
        return jnp.concatenate([parts[i] for i in range(n)], axis=1)

    return finish


def whole_kernel(names, dims, data, weights, sol, res, norms, *scratch):
    r = dict(zip(names, scratch))
    nx, ny, nz = dims
    n, gz = device_count(), lax.axis_size("gz")
    ns, nr = r["near_send"], r["near_recv"]
    signal_all()
    pack_faces(data, r["f_low"], r["f_high"])
    ext, hx = r["ext"], HX[0]
    for x in range(nx):
        ext[hx + x, 0:ny, 0:nz] = data[x]
    wait_all()
    finish = gather_weights(weights, r["wparts"], r["w_send"], r["w_recv"])
    faces = Pair("gz", (r["f_high"], r["g_low"]), (r["f_low"], r["g_high"]), ns, nr, 0)
    faces.clear(r["g_low"], r["g_high"])
    faces.start()

    def x_pair(lanes, slot):
        return Pair(
            "gx",
            (ext.at[nx : nx + hx, 0:ny, lanes], ext.at[0:hx, 0:ny, lanes]),
            (ext.at[hx : 2 * hx, 0:ny, lanes], ext.at[nx + hx : nx + 2 * hx, 0:ny, lanes]),
            ns, nr, slot,
        )

    near = x_pair(slice(0, nz), 2)
    near.clear(ext.at[0:hx, 0:ny, :], ext.at[nx + hx : nx + 2 * hx, 0:ny, :])
    near.start()
    level = [[r["m%d%s" % (k, t)] for t in "hlc"] for k in range(4)]
    build_matrices(nz, nz * gz, finish(), *(level[0] + level[1] + level[2] + level[3]), r["ah"], r["al"])
    faces.wait()
    unpack_faces(dims, r["g_low"], r["g_high"], ext, hx)
    far = x_pair(slice(nz, 2 * nz), 4)
    far.start()
    near.wait()
    far.wait()
    ys = Pair("gy", (ext.at[:, ny - 8 : ny, :], r["y_low"]), (ext.at[:, 0:8, :], r["y_high"]), ns, nr, 6)
    ys.clear(r["y_low"], r["y_high"])
    ys.start()
    ys.wait()
    near.sent()
    far.sent()
    faces.sent()
    ys.sent()
    upper = iota((8, 2 * nz), 0) < 4

    def join(x, carry):
        ext[x, ny : ny + 8, :] = jnp.where(upper, r["y_high"][x], r["y_low"][x])
        return carry

    lax.fori_loop(0, nx + 2 * hx, join, 0)
    down_kernel(0, dims, ext, r["ah"], r["al"], *level[0], r["rhs"], r["e0"], r["r1"], r["p0"], r["ua"], r["gz0"])
    n1, m1, k1 = nx // 2, ny // 2, nz // 2
    h1 = HX[1]
    x1, r1, half = r["x1"], r["r1"], n1 // 2
    for a in range(half):
        r["b_own"][a] = jnp.concatenate([r1[a][:, :k1], r1[a + half][:, :k1]], axis=1)
    zs = Pair("gz", (r["b_own"], r["b_low"]), (r["b_own"], r["b_high"]), ns, nr, 8)
    zs.clear(r["b_low"], r["b_high"])
    zs.start()
    zs.wait()
    blank = jnp.zeros((m1, k1), F32)
    for x in range(n1):
        a, part = x % half, slice((x // half) * k1, (x // half + 1) * k1)
        x1[h1 + x, 0:m1, :] = jnp.concatenate(
            [r1[x][:, :k1], r["b_high"][a][:, part], blank, r["b_low"][a][:, part]], axis=1
        )
    xs = Pair(
        "gx",
        (x1.at[n1 : n1 + h1, 0:m1, :], x1.at[0:h1, 0:m1, :]),
        (x1.at[h1 : 2 * h1, 0:m1, :], x1.at[n1 + h1 : n1 + 2 * h1, 0:m1, :]),
        ns, nr, 10,
    )
    xs.clear(x1.at[0:h1, 0:m1, :], x1.at[n1 + h1 : n1 + 2 * h1, 0:m1, :])
    xs.start()
    xs.wait()
    ys = Pair(
        "gy",
        (x1.at[:, m1 - 8 : m1, :], x1.at[:, m1 + 8 : m1 + 16, :]),
        (x1.at[:, 0:8, :], x1.at[:, m1 : m1 + 8, :]),
        ns, nr, 12,
    )
    ys.clear(x1.at[:, m1 + 8 : m1 + 16, :], x1.at[:, m1 : m1 + 8, :])
    ys.start()
    ys.wait()
    zs.sent()
    xs.sent()
    ys.sent()
    down_kernel(1, dims, x1, *level[1], r["e1"], r["r2"], r["p1"], r["va"], r["gz1"])
    n2, m2, k2 = nx // 4, ny // 4, nz // 4
    slots = nz // k2
    per = n2 // slots
    for a in range(per):
        r["c_own"][a] = jnp.concatenate([r["r2"][q * per + a][:, :k2] for q in range(slots)], axis=1)
    everyone(r["c_own"], r["c_all"], r["c_send"], r["c_recv"])
    gy = lax.axis_size("gy")

    def place(i, carry):
        for j in range(gy):
            for x in range(n2):
                q, a = x // per, x % per
                r["r2all"][i * n2 + x, j * m2 : (j + 1) * m2, :] = jnp.concatenate(
                    [r["c_all"][(i * gy + j) * gz + k, a][:, q * k2 : (q + 1) * k2] for k in range(gz)],
                    axis=1,
                )
        return carry

    lax.fori_loop(0, lax.axis_size("gx"), place, 0)
    coarse_kernel(
        dims, r["r2all"], *level[2], *level[3], r["u2"], r["p2"],
        r["ca"], r["cb"], r["cz"], r["r3"], r["e3a"], r["e3b"], r["cbuf"],
    )
    up_kernel(
        dims, r["u2"], x1, r["e1"], *level[1], r["rhs"], r["e0"], *level[0], sol, res, r["p3"],
        r["va"], r["vb"], r["vbuf"], r["ua"], r["ub"], r["ubuf"],
    )
    row = iota((8, nz), 0)
    mine = jnp.where(row == 0, r["p0"][...], jnp.where(row == 1, r["p1"][...], r["p3"][...]))
    r["n_own"][...] = mine
    everyone(r["n_own"], r["n_all"], r["n_send"], r["n_recv"])
    total = lax.fori_loop(0, n, lambda i, t: t + r["n_all"][i], jnp.zeros((8, nz), F32))
    cells = float(nx * ny * nz * n)
    total = jnp.where(row == 2, r["p2"][...], total)
    scale = jnp.where(row == 1, 8.0 / cells, jnp.where(row == 2, 64.0 / cells, 1.0 / cells))
    norms[...] = jnp.sqrt(total * scale)


def body(data, weights):
    dims = data.shape
    nx, ny, nz = dims
    gx, gy, gz = (lax.axis_size(a) for a in AXES)
    n = gx * gy * gz
    c0, y0, l0 = nx + 2 * HX[0], ny + 8, 2 * nz
    c1, y1 = nx // 2 + 2 * HX[1], ny // 2 + 16
    N2 = (nx // 4 * gx, ny // 4 * gy, nz // 4 * gz)
    N3 = tuple(v // 2 for v in N2)
    per = -(-nx // (nz // WIDTH))
    pad2 = (N2[0] + 2,) + N2[1:]
    pad3 = (N3[0] + 2,) + N3[1:]
    own2 = (nx // 4 // 4, ny // 4, nz)
    shapes = dict(
        f_low=(per, ny, nz), f_high=(per, ny, nz), g_low=(per, ny, nz), g_high=(per, ny, nz),
        ext=(c0, y0, l0), wparts=(gz, 8, nz), y_low=(c0, 8, l0), y_high=(c0, 8, l0),
        rhs=(c0, y0, l0), e0=(c0 + 2, y0, l0), r1=(nx // 2, ny // 2, nz),
        ua=(c0 + 2, y0, l0), ub=(c0 + 2, y0, l0), gz0=(c0 + 2, y0, nz), ubuf=(c0 // 2 + 2, y0, l0),
        b_own=(nx // 4, ny // 2, nz), b_low=(nx // 4, ny // 2, nz), b_high=(nx // 4, ny // 2, nz),
        x1=(c1, y1, l0), e1=(c1 + 2, y1, l0), r2=(nx // 4, ny // 4, nz),
        va=(c1 + 2, y1, l0), vb=(c1 + 2, y1, l0), gz1=(c1 + 2, y1, nz), vbuf=(c1 // 2 + 2, y1, l0),
        c_own=own2, c_all=(n,) + own2, r2all=N2, u2=(N2[0] + 8,) + N2[1:],
        ca=pad2, cb=pad2, cz=(N2[0] + 2, N2[1], N3[2]), r3=N3, e3a=pad3, e3b=pad3,
        cbuf=(N3[0] + 2,) + N2[1:], n_own=(8, nz), n_all=(n, 8, nz),
        p0=(8, nz), p1=(8, nz), p2=(8, nz), p3=(8, nz),
    )
    scratch = {k: pltpu.VMEM(v, F32) for k, v in shapes.items()}
    for k, size in enumerate((l0, l0, N2[2], N3[2])):
        scratch["m%dh" % k] = pltpu.VMEM((size, size), BF16)
        scratch["m%dl" % k] = pltpu.VMEM((size, size), BF16)
        scratch["m%dc" % k] = pltpu.VMEM((8, size), F32)
    scratch["ah"] = scratch["al"] = pltpu.VMEM((l0, l0), BF16)
    dma = pltpu.SemaphoreType.DMA
    scratch.update(near_send=dma((14,)), near_recv=dma((14,)), w_send=dma((gz,)), w_recv=dma((gz,)))
    for k in "cn":
        scratch[k + "_send"] = dma((n,))
        scratch[k + "_recv"] = dma((n,))
    vmem = pl.BlockSpec(memory_space=pltpu.VMEM)
    sol, res, norms = pl.pallas_call(
        functools.partial(whole_kernel, tuple(scratch), dims),
        out_shape=[jax.ShapeDtypeStruct(s, F32) for s in (dims, dims, (8, nz))],
        in_specs=[vmem] * 2,
        out_specs=[vmem] * 3,
        scratch_shapes=list(scratch.values()),
        compiler_params=pltpu.CompilerParams(
            collective_id=0, has_side_effects=True, vmem_limit_bytes=60 * 1024 * 1024
        ),
    )(data, weights)
    return sol, res, norms[:4, 0]


def solution(mesh):
    in_specs = (P("gx", "gy", "gz"), P(None, "gz"))
    out_specs = (P("gx", "gy", "gz"), P("gx", "gy", "gz"), P())
    return jax.shard_map(body, mesh=mesh, in_specs=in_specs, out_specs=out_specs, check_vma=False)
```

```python
import functools
import math
import jax
import jax.numpy as jnp
from jax import lax
from jax.experimental import pallas as pl
from jax.experimental.pallas import tpu as pltpu
from jax.sharding import PartitionSpec as P

HALF = 4
RELAX = 0.45
F32 = jnp.float32
BF16 = jnp.bfloat16
HX = (4, 6)
OFFSETS = [j - HALF for j in range(HALF)] + [j - HALF + 1 for j in range(HALF, 2 * HALF)]


def iota(shape, dim):
    return lax.broadcasted_iota(jnp.int32, shape, dim)


def cyclic(index, size, own):
    cut = (size + own) // 2
    return jnp.where(index < cut, index, index - size)


def split(x):
    high = x.astype(BF16)
    return high, (x - high.astype(F32)).astype(BF16)


def dot(a, b):
    return lax.dot_general(a, b, (((1,), (0,)), ((), ())), preferred_element_type=F32)


def dot3(x, mh, ml):
    h, l = split(x)
    return dot(h, mh) + dot(h, ml) + dot(l, mh)


def dot2(x, m):
    h, l = split(x)
    return dot(h, m) + dot(l, m)


def dot2l(m, x):
    h, l = split(x)
    return dot(m, h) + dot(m, l)


def restrict_matrix(fine, coarse, axis):
    k = fine - 2 * coarse + 1
    m = jnp.where((k == 0) | (k == 3), 0.125, jnp.where((k == 1) | (k == 2), 0.375, 0.0))
    return m.astype(F32)


def prolong_matrix(fine, coarse, limit):
    centre = fine >> 1
    other = jnp.where((fine & 1) == 1, centre + 1, centre - 1)
    m = jnp.where(coarse == centre, 0.75, jnp.where(coarse == other, 0.25, 0.0))
    return jnp.where((fine >= 0) & (fine < limit), m, 0.0).astype(F32)


def build_matrices(nz, whole, wall, *outs):
    z0 = lax.axis_index("gz") * nz
    for level in range(4):
        own = nz >> level
        total = whole >> level
        size = 2 * nz if level < 2 else total
        base = z0 >> level if level < 2 else 0

        def place(index):
            return cyclic(index, size, own) if level < 2 else index

        g = iota((whole, size), 0) >> level
        p = place(iota((whole, size), 1)) + base
        pick = jnp.where(g == p, 0.5**level, 0.0).astype(F32)
        w = lax.dot_general(
            wall, pick, (((1,), (0,)), ((), ())),
            preferred_element_type=F32, precision=lax.Precision.HIGHEST,
        )
        pr = place(iota((size, size), 0))
        pc = place(iota((size, size), 1))
        ok = (pr + base >= 0) & (pr + base < total) & (pc + base >= 0) & (pc + base < total)
        diff = pr - pc
        at = jnp.where(diff == 0, 1.0, 0.0).astype(F32)
        for j, offset in enumerate(OFFSETS):
            at = at + jnp.where(diff == offset, w[j : j + 1, :], 0.0)
        at = jnp.where(ok, at, 0.0)
        a = at.T
        stiff = 0.25**level
        m = lax.dot_general(
            at, a, (((1,), (0,)), ((), ())),
            preferred_element_type=F32, precision=lax.Precision.HIGHEST,
        )
        lap = jnp.where(diff == 0, 6.0, jnp.where((diff == 1) | (diff == -1), -1.0, 0.0))
        m = m + jnp.where(ok, stiff * lap, 0.0)
        d = jnp.sum(jnp.where(diff == 0, m, 0.0), axis=0, keepdims=True)
        col = place(iota((1, size), 1)) + base
        inside = (col >= 0) & (col < total)
        safe = jnp.where(inside, d, 1.0)
        c = jnp.where(inside, RELAX / safe, 0.0)
        inv = jnp.where(inside, safe * (1.0 / RELAX), 0.0)
        mh, ml = split(m * c)
        o = outs[3 * level : 3 * level + 3]
        o[0][...] = mh
        o[1][...] = ml
        o[2][0:1, :] = c
        o[2][1:2, :] = inv
        if level == 0:
            ah, al = split(a)
            outs[12][...] = ah
            outs[13][...] = al


def chunk_of(count, rows, most):
    best = 1
    for planes in range(1, count + 1):
        if count % planes == 0 and planes * rows <= most:
            best = planes
    return best


def sweep(src, r_at, emit, first, count, stiff, mats, xmask, ymask, init=None, own=None, most=800):
    mh, ml, cv = mats
    rows, size = src.shape[1], src.shape[2]
    planes = chunk_of(count, rows, most)
    keep, lanes = own or (rows, size)
    c = cv[0:1, 0:lanes]
    inv = cv[1:2, 0:lanes]
    yi = iota((rows, lanes), 0)

    def step(k, carry):
        x0 = first + k * planes
        u = src[pl.ds(x0, planes), 0:keep, :]
        um = dot3(u.reshape(planes * keep, size), mh[:, 0:lanes], ml[:, 0:lanes])
        for p in range(planes):
            x = x0 + p
            uc = src[x, :, 0:lanes]
            low = pltpu.roll(uc, 1, 0)
            high = pltpu.roll(uc, rows - 1, 0)
            if ymask is None:
                low = jnp.where(yi == 0, 0.0, low)
                high = jnp.where(yi == rows - 1, 0.0, high)
            side = src[x - 1, 0:keep, 0:lanes] + src[x + 1, 0:keep, 0:lanes]
            nb = side + (low + high)[0:keep]
            if ymask is None:
                nb = nb * stiff
            else:
                nb = nb * (ymask[0:keep, 0:lanes] * (xmask(x) * stiff))
            delta = c * (r_at(x)[0:keep, 0:lanes] + nb) - um[p * keep : (p + 1) * keep]
            carry = emit(x, uc[0:keep], delta, inv, carry)
        return carry

    return lax.fori_loop(0, count // planes, step, init)


def restrict(gz, first, count, ry, out, lanes):
    group = chunk_of(count, 1, 8)

    def step(k, carry):
        values = []
        for j in range(group):
            x = first + 2 * (k * group + j)
            t = (gz[x - 1] + 3.0 * gz[x] + 3.0 * gz[x + 1] + gz[x + 2]) * 0.125
            values.append(dot2l(ry, t))
        for j in range(group):
            out(k * group + j, values[j])
        return carry

    lax.fori_loop(0, count // group, step, 0)


def inside_mask(base, limit, pad):
    def mask(x):
        g = base + x - pad
        return jnp.where((g >= 0) & (g < limit), 1.0, 0.0).astype(F32)

    return mask


def y_mask(rows, size, own, base, limit):
    y = cyclic(iota((rows, size), 0), rows, own) + base
    return jnp.where((y >= 0) & (y < limit), 1.0, 0.0).astype(F32)


def zero_planes(ref, *planes):
    for x in planes:
        ref[x] = jnp.zeros(ref.shape[1:], F32)


def geometry(level, dims):
    nx, ny, nz = (v >> level for v in dims)
    gx, gy = lax.axis_size("gx"), lax.axis_size("gy")
    return dict(
        nx=nx, ny=ny, nz=nz, x0=lax.axis_index("gx") * nx, y0=lax.axis_index("gy") * ny,
        z0=lax.axis_index("gz") * nz, NX=nx * gx, NY=ny * gy, NZ=nz * lax.axis_size("gz"),
    )


def down_kernel(level, dims, *refs):
    if level == 0:
        ext, ah, al, mh, ml, cv, rhs, eb, r_next, part, ua, gz = refs
    else:
        rhs, mh, ml, cv, eb, r_next, part, ua, gz = refs
    geo = geometry(level, dims)
    nx, ny, nz = geo["nx"], geo["ny"], geo["nz"]
    hx = HX[level]
    count = nx + 2 * hx
    rows, size = ua.shape[1], ua.shape[2]
    pad = hx + 1
    c = cv[0:1, :]
    zero_planes(ua, 0, count + 1)
    reach = hx - 1 - level
    zero_planes(eb, *range(pad - reach), *range(pad + nx + reach, count + 2))
    if level == 0:
        planes = chunk_of(count, rows, 448)

        def first(k, carry):
            x0 = k * planes
            r = dot3(ext[pl.ds(x0, planes)].reshape(planes * rows, size), ah[...], al[...])
            for p in range(planes):
                rp = r[p * rows : (p + 1) * rows]
                rhs[x0 + p] = rp
                ua[x0 + p + 1] = c * rp
            return carry

        lax.fori_loop(0, count // planes, first, 0)
    else:

        def first(x, carry):
            ua[x + 1] = c * rhs[x]
            return carry

        lax.fori_loop(0, count, first, 0)
    xmask = inside_mask(geo["x0"], geo["NX"], pad)
    ymask = y_mask(rows, size, ny, geo["y0"], geo["NY"])
    mats = (mh, ml, cv)
    stiff = 0.25**level

    def r_at(x):
        return rhs[x - 1]

    def keep(x, u, delta, inv, carry):
        eb[x] = u + delta
        return carry

    sweep(ua, r_at, keep, pad - reach, nx + 2 * reach, stiff, mats, xmask, ymask, 0)
    lanes = gz.shape[2]
    fine = cyclic(iota((size, lanes), 0), size, nz)
    coarse = iota((size, lanes), 1)
    rz = jnp.where(coarse < nz // 2, restrict_matrix(fine, coarse, 0), 0.0).astype(BF16)
    ry = restrict_matrix(
        cyclic(iota((ny // 2, rows), 1), rows, ny), iota((ny // 2, rows), 0), 1
    ).astype(BF16)

    def defect(x, u, delta, inv, carry):
        g = delta * inv
        gz[x] = dot2(g, rz)
        mine = g[0:ny, 0:nz]
        return carry + mine * mine * jnp.where((x >= pad) & (x < pad + nx), 1.0, 0.0).astype(F32)

    total = sweep(
        eb, r_at, defect, pad - 1, nx + 2, stiff, mats, xmask, ymask, jnp.zeros((ny, nz), F32)
    )
    part[...] = jnp.full(part.shape, jnp.sum(total), F32)

    def put(i, value):
        r_next[i] = value

    restrict(gz, pad, nx // 2, ry, put, lanes)


def prolong_into(coarse_ref, coarse_first, coarse_count, pz, py, buf, error, dst, xmask):
    group = chunk_of(coarse_count, 1, 11)
    rows, size = coarse_ref.shape[1:]

    def step(k, carry):
        z = coarse_ref[pl.ds(coarse_first + k * group, group)]
        z = dot2(z.reshape(group * rows, size), pz)
        values = [dot2l(py, z[j * rows : (j + 1) * rows]) for j in range(group)]
        for j in range(group):
            buf[k * group + j] = values[j]
        return carry

    lax.fori_loop(0, coarse_count // group, step, 0)

    def join(i, carry):
        x = 1 + 2 * (i - 1)
        mid = 0.75 * buf[i]
        dst[x] = error(x) + xmask(x) * (mid + 0.25 * buf[i - 1])
        dst[x + 1] = error(x + 1) + xmask(x + 1) * (mid + 0.25 * buf[i + 1])
        return carry

    lax.fori_loop(1, coarse_count - 1, join, 0)


def coarse_kernel(dims, r2, m2h, m2l, c2, m3h, m3l, c3, u2, part, ua, ub, gz, r3, e3a, e3b, buf):
    g2 = geometry(2, dims)
    g3 = geometry(3, dims)
    N2, N3 = g2["NX"], g3["NX"]
    pad = 4
    one = lambda x: 1.0
    for ref in (ua, ub):
        zero_planes(ref, 0, N2 + 1)
    zero_planes(e3a, 0, N3 + 1)
    zero_planes(e3b, 0, N3 + 1)
    zero_planes(gz, 0, N2 + 1)
    zero_planes(u2, *range(pad), *range(N2 + pad, N2 + 2 * pad))
    mats2, mats3 = (m2h, m2l, c2), (m3h, m3l, c3)
    cc = c2[0:1, :]

    def first(x, carry):
        ua[x + 1] = cc * r2[x]
        return carry

    lax.fori_loop(0, N2, first, 0)
    r_at = lambda x: r2[x - 1]

    def into(ref, shift=0):
        def emit(x, u, delta, inv, carry):
            ref[x + shift] = u + delta
            return carry

        return emit

    s2, s3 = 0.25**2, 0.25**3
    sweep(ua, r_at, into(ub), 1, N2, s2, mats2, one, None, 0)
    NY2, NZ2, NY3, NZ3 = g2["NY"], g2["NZ"], g3["NY"], g3["NZ"]
    rz = restrict_matrix(iota((NZ2, NZ3), 0), iota((NZ2, NZ3), 1), 0).astype(BF16)
    ry = restrict_matrix(iota((NY3, NY2), 1), iota((NY3, NY2), 0), 1).astype(BF16)

    def defect(x, u, delta, inv, carry):
        g = delta * inv
        gz[x] = dot2(g, rz)
        return carry + g * g

    total = sweep(ub, r_at, defect, 1, N2, s2, mats2, one, None, jnp.zeros((NY2, NZ2), F32))
    part[...] = jnp.full(part.shape, jnp.sum(total), F32)
    c3v = c3[0:1, :]

    def put(i, value):
        r3[i] = value
        e3a[i + 1] = c3v * value

    restrict(gz, 1, N3, ry, put, NZ3)
    sweep(e3a, lambda x: r3[x - 1], into(e3b), 1, N3, s3, mats3, one, None, 0)
    pz = prolong_matrix(iota((NZ3, NZ2), 1), iota((NZ3, NZ2), 0), NZ2).astype(BF16)
    py = prolong_matrix(iota((NY2, NY3), 0), iota((NY2, NY3), 1), NY2).astype(BF16)
    prolong_into(e3b, 0, N3 + 2, pz, py, buf, lambda x: ub[x], ua, one)
    sweep(ua, r_at, into(ub), 1, N2, s2, mats2, one, None, 0)
    sweep(ub, r_at, into(u2, pad - 1), 1, N2, s2, mats2, one, None, 0)


def up_kernel(dims, u2, r1, e1, m1h, m1l, c1, rhs, e0, m0h, m0l, c0, sol, res, part,
              va, vb, vbuf, ua, ub, ubuf):
    g0, g1, g2 = geometry(0, dims), geometry(1, dims), geometry(2, dims)
    rows, size = va.shape[1], va.shape[2]
    count = g1["nx"] + 2 * HX[1]
    zero_planes(va, 0, count + 1)
    zero_planes(vb, 0, count + 1)
    xmask = inside_mask(g1["x0"], g1["NX"], HX[1] + 1)
    ymask = y_mask(rows, size, g1["ny"], g1["y0"], g1["NY"])
    NY2, NZ2 = g2["NY"], g2["NZ"]
    pz = prolong_matrix(
        cyclic(iota((NZ2, size), 1), size, g1["nz"]) + g1["z0"], iota((NZ2, size), 0), g1["NZ"]
    ).astype(BF16)
    py = prolong_matrix(
        cyclic(iota((rows, NY2), 0), rows, g1["ny"]) + g1["y0"], iota((rows, NY2), 1), g1["NY"]
    ).astype(BF16)
    first = g2["x0"] + 4 - HX[1] // 2 - 1
    prolong_into(u2, first, count // 2 + 2, pz, py, vbuf, lambda x: e1[x], va, xmask)
    mats = (m1h, m1l, c1)

    def into(ref):
        def emit(x, u, delta, inv, carry):
            ref[x] = u + delta
            return carry

        return emit

    r1_at = lambda x: r1[x - 1]
    q, n1 = HX[1] + 1, g1["nx"]
    sweep(va, r1_at, into(vb), q - 3, n1 + 6, 0.25, mats, xmask, ymask, 0)
    sweep(vb, r1_at, into(va), q - 2, n1 + 4, 0.25, mats, xmask, ymask, 0)
    rows0, size0 = ua.shape[1], ua.shape[2]
    count0 = g0["nx"] + 2 * HX[0]
    nx, ny, nz = g0["nx"], g0["ny"], g0["nz"]
    pad = HX[0] + 1
    zero_planes(ua, 0, count0 + 1)
    zero_planes(ub, 0, count0 + 1)
    xmask0 = inside_mask(g0["x0"], g0["NX"], pad)
    ymask0 = y_mask(rows0, size0, ny, g0["y0"], g0["NY"])
    pz = prolong_matrix(
        cyclic(iota((size, size0), 1), size0, nz) + g0["z0"],
        cyclic(iota((size, size0), 0), size, g1["nz"]) + g1["z0"], g0["NZ"],
    ).astype(BF16)
    py = prolong_matrix(
        cyclic(iota((rows0, rows), 0), rows0, ny) + g0["y0"],
        cyclic(iota((rows0, rows), 1), rows, g1["ny"]) + g1["y0"], g0["NY"],
    ).astype(BF16)
    first = HX[1] + 1 - HX[0] // 2 - 1
    prolong_into(va, first, count0 // 2 + 2, pz, py, ubuf, lambda x: e0[x], ua, xmask0)
    mats0 = (m0h, m0l, c0)
    r0_at = lambda x: rhs[x - 1]
    sweep(ua, r0_at, into(ub), pad - 2, nx + 4, 1.0, mats0, xmask0, ymask0, 0)
    sweep(ub, r0_at, into(ua), pad - 1, nx + 2, 1.0, mats0, xmask0, ymask0, 0)

    def final(x, u, delta, inv, carry):
        g = delta * inv
        sol[x - pad] = u
        res[x - pad] = g
        return carry + g * g

    total = sweep(
        ua, r0_at, final, pad, nx, 1.0, mats0, xmask0, ymask0, jnp.zeros((ny, nz), F32), (ny, nz)
    )
    part[...] = jnp.full(part.shape, jnp.sum(total), F32)


AXES = ("gx", "gy", "gz")
MESH = pl.DeviceIdType.MESH
WIDTH = 40


class Pair:
    def __init__(self, axis, up, down, sends, recvs, slot):
        n, me = lax.axis_size(axis), lax.axis_index(axis)
        self.has_low, self.has_high = me > 0, me < n - 1

        def copy(refs, k, target):
            return pltpu.make_async_remote_copy(
                src_ref=refs[0], dst_ref=refs[1], send_sem=sends.at[k], recv_sem=recvs.at[k],
                device_id={axis: target}, device_id_type=MESH,
            )

        self.up = copy(up, slot, lax.rem(me + 1, n))
        self.down = copy(down, slot + 1, lax.rem(me + n - 1, n))

    def start(self):
        pl.when(self.has_high)(self.up.start)
        pl.when(self.has_low)(self.down.start)

    def wait(self):
        pl.when(self.has_low)(self.up.wait_recv)
        pl.when(self.has_high)(self.down.wait_recv)

    def sent(self):
        pl.when(self.has_high)(self.up.wait_send)
        pl.when(self.has_low)(self.down.wait_send)

    def clear(self, low, high):
        @pl.when(jnp.logical_not(self.has_low))
        def _():
            low[...] = jnp.zeros(low.shape, F32)

        @pl.when(jnp.logical_not(self.has_high))
        def _():
            high[...] = jnp.zeros(high.shape, F32)


def linear():
    gy, gz = lax.axis_size("gy"), lax.axis_size("gz")
    return (lax.axis_index("gx") * gy + lax.axis_index("gy")) * gz + lax.axis_index("gz")


def coordinates(t):
    gy, gz = lax.axis_size("gy"), lax.axis_size("gz")
    return (t // (gy * gz), lax.rem(t // gz, gy), lax.rem(t, gz))


def device_count():
    return lax.axis_size("gx") * lax.axis_size("gy") * lax.axis_size("gz")


def near_devices():
    out = []
    for axis, reach in (("gx", 1), ("gy", 1), ("gz", lax.axis_size("gz") - 1)):
        n, me = lax.axis_size(axis), lax.axis_index(axis)
        for d in range(1, reach + 1):
            out.append((me + d < n, {axis: lax.rem(me + d, n)}))
            out.append((me >= d, {axis: lax.rem(me + n - d, n)}))
    return out


def reached():
    return lax.axis_size("gx") <= 4 and lax.axis_size("gy") <= 2


def signal_all():
    n, me = device_count(), linear()
    barrier = pltpu.get_barrier_semaphore()
    if reached():
        for there, device in near_devices():

            @pl.when(there)
            def _():
                pl.semaphore_signal(barrier, inc=1, device_id=device, device_id_type=MESH)

        return

    def step(k, carry):
        pl.semaphore_signal(
            barrier, inc=1, device_id=coordinates(lax.rem(me + k, n)), device_id_type=MESH
        )
        return carry

    lax.fori_loop(1, n, step, 0)


def wait_all():
    if reached():
        count = sum(there.astype(jnp.int32) for there, _ in near_devices())
        pl.semaphore_wait(pltpu.get_barrier_semaphore(), count)
        return
    pl.semaphore_wait(pltpu.get_barrier_semaphore(), device_count() - 1)


def shifted(axis, d):
    n = lax.axis_size(axis)
    t = lax.axis_index(axis) + d
    return jnp.where(t >= n, t - n, t)


def arrived(buf, count, sends, recvs, k, axis):
    part = buf.at[0:count]
    return pltpu.make_async_remote_copy(
        src_ref=part, dst_ref=part, send_sem=sends.at[k], recv_sem=recvs.at[k],
        device_id={axis: shifted(axis, 1)}, device_id_type=MESH,
    )


def spread(block, buf, slot, sends, recvs, k, sizes):
    for dx in range(sizes[0]):
        for dy in range(sizes[1]):
            for dz in range(sizes[2]):
                if dx or dy or dz:
                    pltpu.make_async_remote_copy(
                        src_ref=block, dst_ref=buf.at[slot], send_sem=sends.at[k], recv_sem=recvs.at[k],
                        device_id=(shifted("gx", dx), shifted("gy", dy), shifted("gz", dz)),
                        device_id_type=MESH,
                    ).start()


def everyone(block, buf, sends, recvs):
    n, me = device_count(), linear()
    spread(block, buf, me, sends, recvs, 0, [lax.axis_size(a) for a in AXES])
    buf[me] = block[...]
    done = arrived(buf, n - 1, sends, recvs, 0, "gz")
    done.wait_recv()
    return done


def by_columns(block, buf, sends, recvs):
    gx, gy, gz = (lax.axis_size(a) for a in AXES)
    m, y = gx * gz, lax.axis_index("gy")
    slot = y * m + lax.axis_index("gx") * gz + lax.axis_index("gz")
    spread(block, buf, slot, sends, recvs, 0, (gx, 1, gz))
    buf[slot] = block[...]
    first = arrived(buf, m - 1, sends, recvs, 0, "gz")
    first.wait_recv()
    mine = buf.at[pl.ds(y * m, m)]
    for d in range(1, gy):
        pltpu.make_async_remote_copy(
            src_ref=mine, dst_ref=mine, send_sem=sends.at[1], recv_sem=recvs.at[1],
            device_id={"gy": shifted("gy", d)}, device_id_type=MESH,
        ).start()
    second = arrived(buf, (gy - 1) * m, sends, recvs, 1, "gy")
    second.wait_recv()
    return first, second


def pack_faces(data, low, high):
    nx, ny, nz = data.shape
    slots = nz // WIDTH
    per = -(-nx // slots)
    rest = jnp.zeros((ny, nz - slots * WIDTH), F32)
    for i in range(per):
        planes = [min(k * per + i, nx - 1) for k in range(slots)]
        low[i] = jnp.concatenate([data[x][:, :WIDTH] for x in planes] + [rest], axis=1)
        high[i] = jnp.concatenate([data[x][:, nz - WIDTH :] for x in planes] + [rest], axis=1)


def unpack_faces(dims, from_low, from_high, ext, pad):
    nx, ny, nz = dims
    slots = nz // WIDTH
    per = -(-nx // slots)
    gap = jnp.zeros((ny, nz - 2 * WIDTH), F32)
    for x in range(nx):
        k, i = x // per, x % per
        part = slice(k * WIDTH, (k + 1) * WIDTH)
        ext[pad + x, 0:ny, nz:] = jnp.concatenate(
            [from_high[i][:, part], gap, from_low[i][:, part]], axis=1
        )


def gather_weights(weights, parts, sends, recvs):
    n, me = lax.axis_size("gz"), lax.axis_index("gz")

    def copy(k, slot):
        return pltpu.make_async_remote_copy(
            src_ref=weights, dst_ref=parts.at[slot], send_sem=sends.at[k], recv_sem=recvs.at[k],
            device_id={"gz": lax.rem(me + k, n)}, device_id_type=MESH,
        )

    for k in range(1, n):
        copy(k, me).start()

    def finish():
        parts[me] = weights[...]
        for k in range(1, n):
            c = copy(k, lax.rem(me + n - k, n))
            c.wait_recv()
            c.wait_send()
        return jnp.concatenate([parts[i] for i in range(n)], axis=1)

    return finish


def whole_kernel(names, dims, data, weights, sol, res, norms, *scratch):
    r = dict(zip(names, scratch))
    nx, ny, nz = dims
    n, gz = device_count(), lax.axis_size("gz")
    ns, nr = r["near_send"], r["near_recv"]
    signal_all()
    pack_faces(data, r["f_low"], r["f_high"])
    ext, hx = r["ext"], HX[0]
    for x in range(nx):
        ext[hx + x, 0:ny, 0:nz] = data[x]
    wait_all()
    finish = gather_weights(weights, r["wparts"], r["w_send"], r["w_recv"])
    faces = Pair("gz", (r["f_high"], r["g_low"]), (r["f_low"], r["g_high"]), ns, nr, 0)
    faces.clear(r["g_low"], r["g_high"])
    faces.start()

    def x_pair(lanes, slot):
        return Pair(
            "gx",
            (ext.at[nx : nx + hx, 0:ny, lanes], ext.at[0:hx, 0:ny, lanes]),
            (ext.at[hx : 2 * hx, 0:ny, lanes], ext.at[nx + hx : nx + 2 * hx, 0:ny, lanes]),
            ns, nr, slot,
        )

    near = x_pair(slice(0, nz), 2)
    near.clear(ext.at[0:hx, 0:ny, :], ext.at[nx + hx : nx + 2 * hx, 0:ny, :])
    near.start()
    level = [[r["m%d%s" % (k, t)] for t in "hlc"] for k in range(4)]
    build_matrices(nz, nz * gz, finish(), *(level[0] + level[1] + level[2] + level[3]), r["ah"], r["al"])
    faces.wait()
    unpack_faces(dims, r["g_low"], r["g_high"], ext, hx)
    far = x_pair(slice(nz, 2 * nz), 4)
    far.start()
    near.wait()
    far.wait()
    ys = Pair("gy", (ext.at[:, ny - 8 : ny, :], r["y_low"]), (ext.at[:, 0:8, :], r["y_high"]), ns, nr, 6)
    ys.clear(r["y_low"], r["y_high"])
    ys.start()
    ys.wait()
    near.sent()
    far.sent()
    faces.sent()
    ys.sent()
    upper = iota((8, 2 * nz), 0) < 4

    def join(x, carry):
        ext[x, ny : ny + 8, :] = jnp.where(upper, r["y_high"][x], r["y_low"][x])
        return carry

    lax.fori_loop(0, nx + 2 * hx, join, 0)
    down_kernel(0, dims, ext, r["ah"], r["al"], *level[0], r["rhs"], r["e0"], r["r1"], r["p0"], r["ua"], r["gz0"])
    n1, m1, k1 = nx // 2, ny // 2, nz // 2
    h1 = HX[1]
    x1, r1, half = r["x1"], r["r1"], n1 // 2
    for a in range(half):
        r["b_own"][a] = jnp.concatenate([r1[a][:, :k1], r1[a + half][:, :k1]], axis=1)
    zs = Pair("gz", (r["b_own"], r["b_low"]), (r["b_own"], r["b_high"]), ns, nr, 8)
    zs.clear(r["b_low"], r["b_high"])
    zs.start()
    zs.wait()
    blank = jnp.zeros((m1, k1), F32)
    for x in range(n1):
        a, part = x % half, slice((x // half) * k1, (x // half + 1) * k1)
        x1[h1 + x, 0:m1, :] = jnp.concatenate(
            [r1[x][:, :k1], r["b_high"][a][:, part], blank, r["b_low"][a][:, part]], axis=1
        )
    xs = Pair(
        "gx",
        (x1.at[n1 : n1 + h1, 0:m1, :], x1.at[0:h1, 0:m1, :]),
        (x1.at[h1 : 2 * h1, 0:m1, :], x1.at[n1 + h1 : n1 + 2 * h1, 0:m1, :]),
        ns, nr, 10,
    )
    xs.clear(x1.at[0:h1, 0:m1, :], x1.at[n1 + h1 : n1 + 2 * h1, 0:m1, :])
    xs.start()
    xs.wait()
    ys = Pair(
        "gy",
        (x1.at[:, m1 - 8 : m1, :], x1.at[:, m1 + 8 : m1 + 16, :]),
        (x1.at[:, 0:8, :], x1.at[:, m1 : m1 + 8, :]),
        ns, nr, 12,
    )
    ys.clear(x1.at[:, m1 + 8 : m1 + 16, :], x1.at[:, m1 : m1 + 8, :])
    ys.start()
    ys.wait()
    zs.sent()
    xs.sent()
    ys.sent()
    down_kernel(1, dims, x1, *level[1], r["e1"], r["r2"], r["p1"], r["va"], r["gz1"])
    n2, m2, k2 = nx // 4, ny // 4, nz // 4
    slots = nz // k2
    per = n2 // slots
    for a in range(per):
        r["c_own"][a] = jnp.concatenate([r["r2"][q * per + a][:, :k2] for q in range(slots)], axis=1)
    gathered = by_columns(r["c_own"], r["c_all"], r["c_send"], r["c_recv"])
    gx, gy = lax.axis_size("gx"), lax.axis_size("gy")

    def place(i, carry):
        for j in range(gy):
            for x in range(n2):
                q, a = x // per, x % per
                r["r2all"][i * n2 + x, j * m2 : (j + 1) * m2, :] = jnp.concatenate(
                    [r["c_all"][(j * gx + i) * gz + k, a][:, q * k2 : (q + 1) * k2] for k in range(gz)],
                    axis=1,
                )
        return carry

    lax.fori_loop(0, lax.axis_size("gx"), place, 0)
    coarse_kernel(
        dims, r["r2all"], *level[2], *level[3], r["u2"], r["p2"],
        r["ca"], r["cb"], r["cz"], r["r3"], r["e3a"], r["e3b"], r["cbuf"],
    )
    up_kernel(
        dims, r["u2"], x1, r["e1"], *level[1], r["rhs"], r["e0"], *level[0], sol, res, r["p3"],
        r["va"], r["vb"], r["vbuf"], r["ua"], r["ub"], r["ubuf"],
    )
    for g in gathered:
        g.wait_send()
    lane = iota((1, nz), 1)
    p0, p1, p2, p3 = (r["p%d" % k][0:1, :] for k in range(4))
    mine = jnp.where(lane == 0, p0, jnp.where(lane == 1, p1, p3))
    r["n_own"][...] = mine
    last = everyone(r["n_own"], r["n_all"], r["n_send"], r["n_recv"])
    total = jnp.sum(r["n_all"][...], axis=0)
    cells = float(nx * ny * nz * n)
    total = jnp.where(lane == 2, p2, total)
    scale = jnp.where(lane == 1, 8.0 / cells, jnp.where(lane == 2, 64.0 / cells, 1.0 / cells))
    norms[...] = jnp.sqrt(total * scale)
    last.wait_send()


def body(data, weights):
    dims = data.shape
    nx, ny, nz = dims
    gx, gy, gz = (lax.axis_size(a) for a in AXES)
    n = gx * gy * gz
    c0, y0, l0 = nx + 2 * HX[0], ny + 8, 2 * nz
    c1, y1 = nx // 2 + 2 * HX[1], ny // 2 + 16
    N2 = (nx // 4 * gx, ny // 4 * gy, nz // 4 * gz)
    N3 = tuple(v // 2 for v in N2)
    per = -(-nx // (nz // WIDTH))
    pad2 = (N2[0] + 2,) + N2[1:]
    pad3 = (N3[0] + 2,) + N3[1:]
    own2 = (nx // 4 // 4, ny // 4, nz)
    shapes = dict(
        f_low=(per, ny, nz), f_high=(per, ny, nz), g_low=(per, ny, nz), g_high=(per, ny, nz),
        ext=(c0, y0, l0), wparts=(gz, 8, nz), y_low=(c0, 8, l0), y_high=(c0, 8, l0),
        rhs=(c0, y0, l0), e0=(c0 + 2, y0, l0), r1=(nx // 2, ny // 2, nz),
        ua=(c0 + 2, y0, l0), ub=(c0 + 2, y0, l0), gz0=(c0 + 2, y0, nz), ubuf=(c0 // 2 + 2, y0, l0),
        b_own=(nx // 4, ny // 2, nz), b_low=(nx // 4, ny // 2, nz), b_high=(nx // 4, ny // 2, nz),
        x1=(c1, y1, l0), e1=(c1 + 2, y1, l0), r2=(nx // 4, ny // 4, nz),
        va=(c1 + 2, y1, l0), vb=(c1 + 2, y1, l0), gz1=(c1 + 2, y1, nz), vbuf=(c1 // 2 + 2, y1, l0),
        c_own=own2, c_all=(n,) + own2, r2all=N2, u2=(N2[0] + 8,) + N2[1:],
        ca=pad2, cb=pad2, cz=(N2[0] + 2, N2[1], N3[2]), r3=N3, e3a=pad3, e3b=pad3,
        cbuf=(N3[0] + 2,) + N2[1:], n_own=(1, nz), n_all=(n, 1, nz),
        p0=(8, nz), p1=(8, nz), p2=(8, nz), p3=(8, nz),
    )
    scratch = {k: pltpu.VMEM(v, F32) for k, v in shapes.items()}
    for k, size in enumerate((l0, l0, N2[2], N3[2])):
        scratch["m%dh" % k] = pltpu.VMEM((size, size), BF16)
        scratch["m%dl" % k] = pltpu.VMEM((size, size), BF16)
        scratch["m%dc" % k] = pltpu.VMEM((8, size), F32)
    scratch["ah"] = scratch["al"] = pltpu.VMEM((l0, l0), BF16)
    dma = pltpu.SemaphoreType.DMA
    scratch.update(near_send=dma((14,)), near_recv=dma((14,)), w_send=dma((gz,)), w_recv=dma((gz,)))
    for k in "cn":
        scratch[k + "_send"] = dma((2,))
        scratch[k + "_recv"] = dma((2,))
    words = sum(math.prod(v) for v in shapes.values()) + 2 * l0 * l0 * 3 + N2[2] * N2[2] * 2
    vmem = pl.BlockSpec(memory_space=pltpu.VMEM)
    sol, res, norms = pl.pallas_call(
        functools.partial(whole_kernel, tuple(scratch), dims),
        out_shape=[jax.ShapeDtypeStruct(s, F32) for s in (dims, dims, (1, nz))],
        in_specs=[vmem] * 2,
        out_specs=[vmem] * 3,
        scratch_shapes=list(scratch.values()),
        compiler_params=pltpu.CompilerParams(
            collective_id=0, has_side_effects=True, vmem_limit_bytes=4 * words + 6 * 1024 * 1024
        ),
    )(data, weights)
    return sol, res, norms[0, :4]


def solution(mesh):
    in_specs = (P("gx", "gy", "gz"), P(None, "gz"))
    out_specs = (P("gx", "gy", "gz"), P("gx", "gy", "gz"), P())
    return jax.shard_map(body, mesh=mesh, in_specs=in_specs, out_specs=out_specs, check_vma=False)
```

```python
import functools
import math
import jax
import jax.numpy as jnp
from jax import lax
from jax.experimental import pallas as pl
from jax.experimental.pallas import tpu as pltpu
from jax.sharding import PartitionSpec as P

HALF = 4
RELAX = 0.45
F32 = jnp.float32
BF16 = jnp.bfloat16
HX = (4, 6)
OFFSETS = [j - HALF for j in range(HALF)] + [j - HALF + 1 for j in range(HALF, 2 * HALF)]


def iota(shape, dim):
    return lax.broadcasted_iota(jnp.int32, shape, dim)


def cyclic(index, size, own):
    cut = (size + own) // 2
    return jnp.where(index < cut, index, index - size)


def split(x):
    high = x.astype(BF16)
    return high, (x - high.astype(F32)).astype(BF16)


def dot(a, b):
    return lax.dot_general(a, b, (((1,), (0,)), ((), ())), preferred_element_type=F32)


def dot3(x, mh, ml):
    h, l = split(x)
    return dot(h, mh) + dot(h, ml) + dot(l, mh)


def dot2(x, m):
    h, l = split(x)
    return dot(h, m) + dot(l, m)


def dot2l(m, x):
    h, l = split(x)
    return dot(m, h) + dot(m, l)


def restrict_matrix(fine, coarse, axis):
    k = fine - 2 * coarse + 1
    m = jnp.where((k == 0) | (k == 3), 0.125, jnp.where((k == 1) | (k == 2), 0.375, 0.0))
    return m.astype(F32)


def prolong_matrix(fine, coarse, limit):
    centre = fine >> 1
    other = jnp.where((fine & 1) == 1, centre + 1, centre - 1)
    m = jnp.where(coarse == centre, 0.75, jnp.where(coarse == other, 0.25, 0.0))
    return jnp.where((fine >= 0) & (fine < limit), m, 0.0).astype(F32)


def build_matrices(nz, whole, wall, *outs):
    z0 = lax.axis_index("gz") * nz
    for level in range(4):
        own = nz >> level
        total = whole >> level
        size = 2 * nz if level < 2 else total
        base = z0 >> level if level < 2 else 0

        def place(index):
            return cyclic(index, size, own) if level < 2 else index

        g = iota((whole, size), 0) >> level
        p = place(iota((whole, size), 1)) + base
        pick = jnp.where(g == p, 0.5**level, 0.0).astype(F32)
        w = lax.dot_general(
            wall, pick, (((1,), (0,)), ((), ())),
            preferred_element_type=F32, precision=lax.Precision.HIGHEST,
        )
        pr = place(iota((size, size), 0))
        pc = place(iota((size, size), 1))
        ok = (pr + base >= 0) & (pr + base < total) & (pc + base >= 0) & (pc + base < total)
        diff = pr - pc
        at = jnp.where(diff == 0, 1.0, 0.0).astype(F32)
        for j, offset in enumerate(OFFSETS):
            at = at + jnp.where(diff == offset, w[j : j + 1, :], 0.0)
        at = jnp.where(ok, at, 0.0)
        a = at.T
        stiff = 0.25**level
        m = lax.dot_general(
            at, a, (((1,), (0,)), ((), ())),
            preferred_element_type=F32, precision=lax.Precision.HIGHEST,
        )
        lap = jnp.where(diff == 0, 6.0, jnp.where((diff == 1) | (diff == -1), -1.0, 0.0))
        m = m + jnp.where(ok, stiff * lap, 0.0)
        d = jnp.sum(jnp.where(diff == 0, m, 0.0), axis=0, keepdims=True)
        col = place(iota((1, size), 1)) + base
        inside = (col >= 0) & (col < total)
        safe = jnp.where(inside, d, 1.0)
        c = jnp.where(inside, RELAX / safe, 0.0)
        inv = jnp.where(inside, safe * (1.0 / RELAX), 0.0)
        mh, ml = split(m * c)
        o = outs[3 * level : 3 * level + 3]
        o[0][...] = mh
        o[1][...] = ml
        o[2][0:1, :] = c
        o[2][1:2, :] = inv
        if level == 0:
            ah, al = split(a)
            outs[12][...] = ah
            outs[13][...] = al


def chunk_of(count, rows, most):
    best = 1
    for planes in range(1, count + 1):
        if count % planes == 0 and planes * rows <= most:
            best = planes
    return best


def sweep(src, r_at, emit, first, count, stiff, mats, xmask, ymask, init=None, own=None, most=800):
    mh, ml, cv = mats
    rows, size = src.shape[1], src.shape[2]
    planes = chunk_of(count, rows, most)
    keep, lanes = own or (rows, size)
    c = cv[0:1, 0:lanes]
    inv = cv[1:2, 0:lanes]
    yi = iota((rows, lanes), 0)

    def step(k, carry):
        x0 = first + k * planes
        u = src[pl.ds(x0, planes), 0:keep, :]
        um = dot3(u.reshape(planes * keep, size), mh[:, 0:lanes], ml[:, 0:lanes])
        for p in range(planes):
            x = x0 + p
            uc = src[x, :, 0:lanes]
            low = pltpu.roll(uc, 1, 0)
            high = pltpu.roll(uc, rows - 1, 0)
            if ymask is None:
                low = jnp.where(yi == 0, 0.0, low)
                high = jnp.where(yi == rows - 1, 0.0, high)
            side = src[x - 1, 0:keep, 0:lanes] + src[x + 1, 0:keep, 0:lanes]
            nb = side + (low + high)[0:keep]
            if ymask is None:
                nb = nb * stiff
            else:
                nb = nb * (ymask[0:keep, 0:lanes] * (xmask(x) * stiff))
            delta = c * (r_at(x)[0:keep, 0:lanes] + nb) - um[p * keep : (p + 1) * keep]
            carry = emit(x, uc[0:keep], delta, inv, carry)
        return carry

    return lax.fori_loop(0, count // planes, step, init)


def restrict(gz, first, count, ry, out, lanes):
    group = chunk_of(count, 1, 8)

    def step(k, carry):
        values = []
        for j in range(group):
            x = first + 2 * (k * group + j)
            t = (gz[x - 1] + 3.0 * gz[x] + 3.0 * gz[x + 1] + gz[x + 2]) * 0.125
            values.append(dot2l(ry, t))
        for j in range(group):
            out(k * group + j, values[j])
        return carry

    lax.fori_loop(0, count // group, step, 0)


def inside_mask(base, limit, pad):
    def mask(x):
        g = base + x - pad
        return jnp.where((g >= 0) & (g < limit), 1.0, 0.0).astype(F32)

    return mask


def y_mask(rows, size, own, base, limit):
    y = cyclic(iota((rows, size), 0), rows, own) + base
    return jnp.where((y >= 0) & (y < limit), 1.0, 0.0).astype(F32)


def zero_planes(ref, *planes):
    for x in planes:
        ref[x] = jnp.zeros(ref.shape[1:], F32)


def geometry(level, dims):
    nx, ny, nz = (v >> level for v in dims)
    gx, gy = lax.axis_size("gx"), lax.axis_size("gy")
    return dict(
        nx=nx, ny=ny, nz=nz, x0=lax.axis_index("gx") * nx, y0=lax.axis_index("gy") * ny,
        z0=lax.axis_index("gz") * nz, NX=nx * gx, NY=ny * gy, NZ=nz * lax.axis_size("gz"),
    )


def down_kernel(level, dims, *refs):
    if level == 0:
        ext, ah, al, mh, ml, cv, rhs, eb, r_next, part, ua, gz = refs
    else:
        rhs, mh, ml, cv, eb, r_next, part, ua, gz = refs
    geo = geometry(level, dims)
    nx, ny, nz = geo["nx"], geo["ny"], geo["nz"]
    hx = HX[level]
    count = nx + 2 * hx
    rows, size = ua.shape[1], ua.shape[2]
    pad = hx + 1
    c = cv[0:1, :]
    zero_planes(ua, 0, count + 1)
    reach = hx - 1 - level
    zero_planes(eb, *range(pad - reach), *range(pad + nx + reach, count + 2))
    if level == 0:
        planes = chunk_of(count, rows, 448)

        def first(k, carry):
            x0 = k * planes
            r = dot3(ext[pl.ds(x0, planes)].reshape(planes * rows, size), ah[...], al[...])
            for p in range(planes):
                rp = r[p * rows : (p + 1) * rows]
                rhs[x0 + p] = rp
                ua[x0 + p + 1] = c * rp
            return carry

        lax.fori_loop(0, count // planes, first, 0)
    else:

        def first(x, carry):
            ua[x + 1] = c * rhs[x]
            return carry

        lax.fori_loop(0, count, first, 0)
    xmask = inside_mask(geo["x0"], geo["NX"], pad)
    ymask = y_mask(rows, size, ny, geo["y0"], geo["NY"])
    mats = (mh, ml, cv)
    stiff = 0.25**level

    def r_at(x):
        return rhs[x - 1]

    def keep(x, u, delta, inv, carry):
        eb[x] = u + delta
        return carry

    sweep(ua, r_at, keep, pad - reach, nx + 2 * reach, stiff, mats, xmask, ymask, 0)
    lanes = gz.shape[2]
    fine = cyclic(iota((size, lanes), 0), size, nz)
    coarse = iota((size, lanes), 1)
    rz = jnp.where(coarse < nz // 2, restrict_matrix(fine, coarse, 0), 0.0).astype(BF16)
    ry = restrict_matrix(
        cyclic(iota((ny // 2, rows), 1), rows, ny), iota((ny // 2, rows), 0), 1
    ).astype(BF16)

    def defect(x, u, delta, inv, carry):
        g = delta * inv
        gz[x] = dot2(g, rz)
        mine = g[0:ny, 0:nz]
        return carry + mine * mine * jnp.where((x >= pad) & (x < pad + nx), 1.0, 0.0).astype(F32)

    total = sweep(
        eb, r_at, defect, pad - 1, nx + 2, stiff, mats, xmask, ymask, jnp.zeros((ny, nz), F32)
    )
    part[...] = jnp.full(part.shape, jnp.sum(total), F32)

    def put(i, value):
        r_next[i] = value

    restrict(gz, pad, nx // 2, ry, put, lanes)


def prolong_into(coarse_ref, coarse_first, coarse_count, pz, py, buf, error, dst, xmask):
    group = chunk_of(coarse_count, 1, 11)
    rows, size = coarse_ref.shape[1:]

    def step(k, carry):
        z = coarse_ref[pl.ds(coarse_first + k * group, group)]
        z = dot2(z.reshape(group * rows, size), pz)
        values = [dot2l(py, z[j * rows : (j + 1) * rows]) for j in range(group)]
        for j in range(group):
            buf[k * group + j] = values[j]
        return carry

    lax.fori_loop(0, coarse_count // group, step, 0)

    def join(i, carry):
        x = 1 + 2 * (i - 1)
        mid = 0.75 * buf[i]
        dst[x] = error(x) + xmask(x) * (mid + 0.25 * buf[i - 1])
        dst[x + 1] = error(x + 1) + xmask(x + 1) * (mid + 0.25 * buf[i + 1])
        return carry

    lax.fori_loop(1, coarse_count - 1, join, 0)


def coarse_kernel(dims, r2, m2h, m2l, c2, m3h, m3l, c3, u2, part, ua, ub, gz, r3, e3a, e3b, buf):
    g2 = geometry(2, dims)
    g3 = geometry(3, dims)
    N2, N3 = g2["NX"], g3["NX"]
    pad = 4
    one = lambda x: 1.0
    for ref in (ua, ub):
        zero_planes(ref, 0, N2 + 1)
    zero_planes(e3a, 0, N3 + 1)
    zero_planes(e3b, 0, N3 + 1)
    zero_planes(gz, 0, N2 + 1)
    zero_planes(u2, *range(pad), *range(N2 + pad, N2 + 2 * pad))
    mats2, mats3 = (m2h, m2l, c2), (m3h, m3l, c3)
    cc = c2[0:1, :]

    def first(x, carry):
        ua[x + 1] = cc * r2[x]
        return carry

    lax.fori_loop(0, N2, first, 0)
    r_at = lambda x: r2[x - 1]

    def into(ref, shift=0):
        def emit(x, u, delta, inv, carry):
            ref[x + shift] = u + delta
            return carry

        return emit

    s2, s3 = 0.25**2, 0.25**3
    sweep(ua, r_at, into(ub), 1, N2, s2, mats2, one, None, 0)
    NY2, NZ2, NY3, NZ3 = g2["NY"], g2["NZ"], g3["NY"], g3["NZ"]
    rz = restrict_matrix(iota((NZ2, NZ3), 0), iota((NZ2, NZ3), 1), 0).astype(BF16)
    ry = restrict_matrix(iota((NY3, NY2), 1), iota((NY3, NY2), 0), 1).astype(BF16)

    def defect(x, u, delta, inv, carry):
        g = delta * inv
        gz[x] = dot2(g, rz)
        return carry + g * g

    total = sweep(ub, r_at, defect, 1, N2, s2, mats2, one, None, jnp.zeros((NY2, NZ2), F32))
    part[...] = jnp.full(part.shape, jnp.sum(total), F32)
    c3v = c3[0:1, :]

    def put(i, value):
        r3[i] = value
        e3a[i + 1] = c3v * value

    restrict(gz, 1, N3, ry, put, NZ3)
    sweep(e3a, lambda x: r3[x - 1], into(e3b), 1, N3, s3, mats3, one, None, 0)
    pz = prolong_matrix(iota((NZ3, NZ2), 1), iota((NZ3, NZ2), 0), NZ2).astype(BF16)
    py = prolong_matrix(iota((NY2, NY3), 0), iota((NY2, NY3), 1), NY2).astype(BF16)
    prolong_into(e3b, 0, N3 + 2, pz, py, buf, lambda x: ub[x], ua, one)
    sweep(ua, r_at, into(ub), 1, N2, s2, mats2, one, None, 0)
    sweep(ub, r_at, into(u2, pad - 1), 1, N2, s2, mats2, one, None, 0)


def up_kernel(dims, u2, r1, e1, m1h, m1l, c1, rhs, e0, m0h, m0l, c0, sol, res, part,
              va, vb, vbuf, ua, ub, ubuf):
    g0, g1, g2 = geometry(0, dims), geometry(1, dims), geometry(2, dims)
    rows, size = va.shape[1], va.shape[2]
    count = g1["nx"] + 2 * HX[1]
    zero_planes(va, 0, count + 1)
    zero_planes(vb, 0, count + 1)
    xmask = inside_mask(g1["x0"], g1["NX"], HX[1] + 1)
    ymask = y_mask(rows, size, g1["ny"], g1["y0"], g1["NY"])
    NY2, NZ2 = g2["NY"], g2["NZ"]
    pz = prolong_matrix(
        cyclic(iota((NZ2, size), 1), size, g1["nz"]) + g1["z0"], iota((NZ2, size), 0), g1["NZ"]
    ).astype(BF16)
    py = prolong_matrix(
        cyclic(iota((rows, NY2), 0), rows, g1["ny"]) + g1["y0"], iota((rows, NY2), 1), g1["NY"]
    ).astype(BF16)
    first = g2["x0"] + 4 - HX[1] // 2 - 1
    prolong_into(u2, first, count // 2 + 2, pz, py, vbuf, lambda x: e1[x], va, xmask)
    mats = (m1h, m1l, c1)

    def into(ref):
        def emit(x, u, delta, inv, carry):
            ref[x] = u + delta
            return carry

        return emit

    r1_at = lambda x: r1[x - 1]
    q, n1 = HX[1] + 1, g1["nx"]
    sweep(va, r1_at, into(vb), q - 3, n1 + 6, 0.25, mats, xmask, ymask, 0)
    sweep(vb, r1_at, into(va), q - 2, n1 + 4, 0.25, mats, xmask, ymask, 0)
    rows0, size0 = ua.shape[1], ua.shape[2]
    count0 = g0["nx"] + 2 * HX[0]
    nx, ny, nz = g0["nx"], g0["ny"], g0["nz"]
    pad = HX[0] + 1
    zero_planes(ua, 0, count0 + 1)
    zero_planes(ub, 0, count0 + 1)
    xmask0 = inside_mask(g0["x0"], g0["NX"], pad)
    ymask0 = y_mask(rows0, size0, ny, g0["y0"], g0["NY"])
    pz = prolong_matrix(
        cyclic(iota((size, size0), 1), size0, nz) + g0["z0"],
        cyclic(iota((size, size0), 0), size, g1["nz"]) + g1["z0"], g0["NZ"],
    ).astype(BF16)
    py = prolong_matrix(
        cyclic(iota((rows0, rows), 0), rows0, ny) + g0["y0"],
        cyclic(iota((rows0, rows), 1), rows, g1["ny"]) + g1["y0"], g0["NY"],
    ).astype(BF16)
    first = HX[1] + 1 - HX[0] // 2 - 1
    prolong_into(va, first, count0 // 2 + 2, pz, py, ubuf, lambda x: e0[x], ua, xmask0)
    mats0 = (m0h, m0l, c0)
    r0_at = lambda x: rhs[x - 1]
    sweep(ua, r0_at, into(ub), pad - 2, nx + 4, 1.0, mats0, xmask0, ymask0, 0)
    sweep(ub, r0_at, into(ua), pad - 1, nx + 2, 1.0, mats0, xmask0, ymask0, 0)

    def final(x, u, delta, inv, carry):
        g = delta * inv
        sol[x - pad] = u
        res[x - pad] = g
        return carry + g * g

    total = sweep(
        ua, r0_at, final, pad, nx, 1.0, mats0, xmask0, ymask0, jnp.zeros((ny, nz), F32), (ny, nz)
    )
    part[...] = jnp.full(part.shape, jnp.sum(total), F32)


AXES = ("gx", "gy", "gz")
MESH = pl.DeviceIdType.MESH
WIDTH = 40


class Pair:
    def __init__(self, axis, up, down, sends, recvs, slot):
        n, me = lax.axis_size(axis), lax.axis_index(axis)
        self.has_low, self.has_high = me > 0, me < n - 1

        def copy(refs, k, target):
            return pltpu.make_async_remote_copy(
                src_ref=refs[0], dst_ref=refs[1], send_sem=sends.at[k], recv_sem=recvs.at[k],
                device_id={axis: target}, device_id_type=MESH,
            )

        self.up = copy(up, slot, lax.rem(me + 1, n))
        self.down = copy(down, slot + 1, lax.rem(me + n - 1, n))

    def start(self):
        pl.when(self.has_high)(self.up.start)
        pl.when(self.has_low)(self.down.start)

    def wait(self):
        pl.when(self.has_low)(self.up.wait_recv)
        pl.when(self.has_high)(self.down.wait_recv)

    def sent(self):
        pl.when(self.has_high)(self.up.wait_send)
        pl.when(self.has_low)(self.down.wait_send)

    def clear(self, low, high):
        @pl.when(jnp.logical_not(self.has_low))
        def _():
            low[...] = jnp.zeros(low.shape, F32)

        @pl.when(jnp.logical_not(self.has_high))
        def _():
            high[...] = jnp.zeros(high.shape, F32)


class Star:
    def __init__(self, src, pieces, bufs, sends, recvs, first):
        gx, gz = lax.axis_size("gx"), lax.axis_size("gz")
        mx, mz = lax.axis_index("gx"), lax.axis_index("gz")
        self.moves = []
        order = [(dx, dz) for dx in (-1, 1) for dz in (-1, 1)] + [(0, -1), (0, 1), (-1, 0), (1, 0)]
        for k, (dx, dz) in enumerate(order):
            to = ((mx + dx >= 0) & (mx + dx < gx) & (mz + dz >= 0) & (mz + dz < gz))
            frm = ((mx - dx >= 0) & (mx - dx < gx) & (mz - dz >= 0) & (mz - dz < gz))
            into = bufs[(-dx, -dz)]
            copy = pltpu.make_async_remote_copy(
                src_ref=src[dz].at[pieces[dx]], dst_ref=into,
                send_sem=sends.at[first + k], recv_sem=recvs.at[first + k],
                device_id={"gx": lax.rem(mx + dx + gx, gx), "gz": lax.rem(mz + dz + gz, gz)},
                device_id_type=MESH,
            )
            self.moves.append((to, frm, copy, into))

    def clear(self):
        for _, frm, _, into in self.moves:

            @pl.when(jnp.logical_not(frm))
            def _(into=into):
                into[...] = jnp.zeros(into.shape, F32)

    def start(self):
        for to, _, copy, _ in self.moves:
            pl.when(to)(copy.start)

    def wait(self):
        for _, frm, copy, _ in self.moves:
            pl.when(frm)(copy.wait_recv)

    def sent(self):
        for to, _, copy, _ in self.moves:
            pl.when(to)(copy.wait_send)


STAR = [(dx, dz) for dx in (-1, 0, 1) for dz in (-1, 0, 1) if dx or dz]


def star_name(prefix, d):
    return prefix + "mop"[d[0] + 1] + "mop"[d[1] + 1]


def linear():
    gy, gz = lax.axis_size("gy"), lax.axis_size("gz")
    return (lax.axis_index("gx") * gy + lax.axis_index("gy")) * gz + lax.axis_index("gz")


def coordinates(t):
    gy, gz = lax.axis_size("gy"), lax.axis_size("gz")
    return (t // (gy * gz), lax.rem(t // gz, gy), lax.rem(t, gz))


def device_count():
    return lax.axis_size("gx") * lax.axis_size("gy") * lax.axis_size("gz")


def near_devices():
    out = []
    for axis, reach in (("gx", 1), ("gy", 1), ("gz", lax.axis_size("gz") - 1)):
        n, me = lax.axis_size(axis), lax.axis_index(axis)
        for d in range(1, reach + 1):
            out.append((me + d < n, {axis: lax.rem(me + d, n)}))
            out.append((me >= d, {axis: lax.rem(me + n - d, n)}))
    return out


def reached():
    return lax.axis_size("gx") <= 4 and lax.axis_size("gy") <= 2


def signal_all():
    n, me = device_count(), linear()
    barrier = pltpu.get_barrier_semaphore()
    if reached():
        for there, device in near_devices():

            @pl.when(there)
            def _():
                pl.semaphore_signal(barrier, inc=1, device_id=device, device_id_type=MESH)

        return

    def step(k, carry):
        pl.semaphore_signal(
            barrier, inc=1, device_id=coordinates(lax.rem(me + k, n)), device_id_type=MESH
        )
        return carry

    lax.fori_loop(1, n, step, 0)


def wait_all():
    if reached():
        count = sum(there.astype(jnp.int32) for there, _ in near_devices())
        pl.semaphore_wait(pltpu.get_barrier_semaphore(), count)
        return
    pl.semaphore_wait(pltpu.get_barrier_semaphore(), device_count() - 1)


def shifted(axis, d):
    n = lax.axis_size(axis)
    t = lax.axis_index(axis) + d
    return jnp.where(t >= n, t - n, t)


def arrived(buf, count, sends, recvs, k, axis):
    part = buf.at[0:count]
    return pltpu.make_async_remote_copy(
        src_ref=part, dst_ref=part, send_sem=sends.at[k], recv_sem=recvs.at[k],
        device_id={axis: shifted(axis, 1)}, device_id_type=MESH,
    )


def spread(block, buf, slot, sends, recvs, k, sizes):
    for dx in range(sizes[0]):
        for dy in range(sizes[1]):
            for dz in range(sizes[2]):
                if dx or dy or dz:
                    pltpu.make_async_remote_copy(
                        src_ref=block, dst_ref=buf.at[slot], send_sem=sends.at[k], recv_sem=recvs.at[k],
                        device_id=(shifted("gx", dx), shifted("gy", dy), shifted("gz", dz)),
                        device_id_type=MESH,
                    ).start()


def everyone(block, buf, sends, recvs):
    n, me = device_count(), linear()
    spread(block, buf, me, sends, recvs, 0, [lax.axis_size(a) for a in AXES])
    buf[me] = block[...]
    done = arrived(buf, n - 1, sends, recvs, 0, "gz")
    done.wait_recv()
    return done


def by_columns(block, buf, sends, recvs):
    gx, gy, gz = (lax.axis_size(a) for a in AXES)
    m, y = gx * gz, lax.axis_index("gy")
    slot = y * m + lax.axis_index("gx") * gz + lax.axis_index("gz")
    spread(block, buf, slot, sends, recvs, 0, (gx, 1, gz))
    buf[slot] = block[...]
    first = arrived(buf, m - 1, sends, recvs, 0, "gz")
    first.wait_recv()
    mine = buf.at[pl.ds(y * m, m)]
    for d in range(1, gy):
        pltpu.make_async_remote_copy(
            src_ref=mine, dst_ref=mine, send_sem=sends.at[1], recv_sem=recvs.at[1],
            device_id={"gy": shifted("gy", d)}, device_id_type=MESH,
        ).start()
    second = arrived(buf, (gy - 1) * m, sends, recvs, 1, "gy")
    second.wait_recv()
    return first, second


def pack_faces(data, low, high):
    nx, ny, nz = data.shape
    slots = nz // WIDTH
    per = -(-nx // slots)
    rest = jnp.zeros((ny, nz - slots * WIDTH), F32)
    for i in range(per):
        planes = [min(k * per + i, nx - 1) for k in range(slots)]
        low[i] = jnp.concatenate([data[x][:, :WIDTH] for x in planes] + [rest], axis=1)
        high[i] = jnp.concatenate([data[x][:, nz - WIDTH :] for x in planes] + [rest], axis=1)


def unpack_faces(dims, from_low, from_high, ext, pad):
    nx, ny, nz = dims
    slots = nz // WIDTH
    per = -(-nx // slots)
    gap = jnp.zeros((ny, nz - 2 * WIDTH), F32)
    for x in range(nx):
        k, i = x // per, x % per
        part = slice(k * WIDTH, (k + 1) * WIDTH)
        ext[pad + x, 0:ny, nz:] = jnp.concatenate(
            [from_high[i][:, part], gap, from_low[i][:, part]], axis=1
        )


def gather_weights(weights, parts, sends, recvs):
    n, me = lax.axis_size("gz"), lax.axis_index("gz")

    def copy(k, slot):
        return pltpu.make_async_remote_copy(
            src_ref=weights, dst_ref=parts.at[slot], send_sem=sends.at[k], recv_sem=recvs.at[k],
            device_id={"gz": lax.rem(me + k, n)}, device_id_type=MESH,
        )

    for k in range(1, n):
        copy(k, me).start()

    def finish():
        parts[me] = weights[...]
        for k in range(1, n):
            c = copy(k, lax.rem(me + n - k, n))
            c.wait_recv()
            c.wait_send()
        return jnp.concatenate([parts[i] for i in range(n)], axis=1)

    return finish


def whole_kernel(names, dims, data, weights, sol, res, norms, *scratch):
    r = dict(zip(names, scratch))
    nx, ny, nz = dims
    n, gz = device_count(), lax.axis_size("gz")
    ns, nr = r["near_send"], r["near_recv"]
    signal_all()
    pack_faces(data, r["f_low"], r["f_high"])
    ext, hx = r["ext"], HX[0]
    for x in range(nx):
        ext[hx + x, 0:ny, 0:nz] = data[x]
    wait_all()
    finish = gather_weights(weights, r["wparts"], r["w_send"], r["w_recv"])
    faces = Pair("gz", (r["f_high"], r["g_low"]), (r["f_low"], r["g_high"]), ns, nr, 0)
    faces.clear(r["g_low"], r["g_high"])
    faces.start()

    def x_pair(lanes, slot):
        return Pair(
            "gx",
            (ext.at[nx : nx + hx, 0:ny, lanes], ext.at[0:hx, 0:ny, lanes]),
            (ext.at[hx : 2 * hx, 0:ny, lanes], ext.at[nx + hx : nx + 2 * hx, 0:ny, lanes]),
            ns, nr, slot,
        )

    near = x_pair(slice(0, nz), 2)
    near.clear(ext.at[0:hx, 0:ny, :], ext.at[nx + hx : nx + 2 * hx, 0:ny, :])
    near.start()
    level = [[r["m%d%s" % (k, t)] for t in "hlc"] for k in range(4)]
    build_matrices(nz, nz * gz, finish(), *(level[0] + level[1] + level[2] + level[3]), r["ah"], r["al"])
    faces.wait()
    unpack_faces(dims, r["g_low"], r["g_high"], ext, hx)
    far = x_pair(slice(nz, 2 * nz), 4)
    far.start()
    near.wait()
    far.wait()
    ys = Pair("gy", (ext.at[:, ny - 8 : ny, :], r["y_low"]), (ext.at[:, 0:8, :], r["y_high"]), ns, nr, 6)
    ys.clear(r["y_low"], r["y_high"])
    ys.start()
    ys.wait()
    near.sent()
    far.sent()
    faces.sent()
    ys.sent()
    upper = iota((8, 2 * nz), 0) < 4

    def join(x, carry):
        ext[x, ny : ny + 8, :] = jnp.where(upper, r["y_high"][x], r["y_low"][x])
        return carry

    lax.fori_loop(0, nx + 2 * hx, join, 0)
    down_kernel(0, dims, ext, r["ah"], r["al"], *level[0], r["rhs"], r["e0"], r["r1"], r["p0"], r["ua"], r["gz0"])
    n1, m1, k1 = nx // 2, ny // 2, nz // 2
    h1 = HX[1]
    x1, r1, own = r["x1"], r["r1"], r["b_own"]
    for a in range(n1 // 2):
        own[a] = jnp.concatenate([r1[2 * a][:, :k1], r1[2 * a + 1][:, :k1]], axis=1)
    bufs = {d: r[star_name("b_", d)] for d in STAR}
    rim = h1 // 2
    pieces = {-1: slice(0, rim), 0: slice(0, n1 // 2), 1: slice(n1 // 2 - rim, n1 // 2)}
    star = Star({d: own for d in (-1, 0, 1)}, pieces, bufs, r["b_send"], r["b_recv"], 0)
    star.start()
    star.clear()
    star.wait()
    bufs[(0, 0)] = own
    blank = jnp.zeros((m1, k1), F32)
    for dx in (-1, 0, 1):
        base = h1 + dx * h1 if dx < 1 else h1 + n1
        for x in range(n1 if dx == 0 else h1):
            a, part = x // 2, slice((x % 2) * k1, (x % 2 + 1) * k1)
            low, mid, high = (bufs[(dx, dz)][a][:, part] for dz in (-1, 0, 1))
            x1[base + x, 0:m1, :] = jnp.concatenate([mid, high, blank, low], axis=1)
    ys = Pair(
        "gy",
        (x1.at[:, m1 - 8 : m1, :], x1.at[:, m1 + 8 : m1 + 16, :]),
        (x1.at[:, 0:8, :], x1.at[:, m1 : m1 + 8, :]),
        ns, nr, 8,
    )
    ys.clear(x1.at[:, m1 + 8 : m1 + 16, :], x1.at[:, m1 : m1 + 8, :])
    ys.start()
    ys.wait()
    star.sent()
    ys.sent()
    down_kernel(1, dims, x1, *level[1], r["e1"], r["r2"], r["p1"], r["va"], r["gz1"])
    n2, m2, k2 = nx // 4, ny // 4, nz // 4
    slots = nz // k2
    per = n2 // slots
    for a in range(per):
        r["c_own"][a] = jnp.concatenate([r["r2"][q * per + a][:, :k2] for q in range(slots)], axis=1)
    gathered = by_columns(r["c_own"], r["c_all"], r["c_send"], r["c_recv"])
    gx, gy = lax.axis_size("gx"), lax.axis_size("gy")

    def place(i, carry):
        for j in range(gy):
            for x in range(n2):
                q, a = x // per, x % per
                r["r2all"][i * n2 + x, j * m2 : (j + 1) * m2, :] = jnp.concatenate(
                    [r["c_all"][(j * gx + i) * gz + k, a][:, q * k2 : (q + 1) * k2] for k in range(gz)],
                    axis=1,
                )
        return carry

    lax.fori_loop(0, lax.axis_size("gx"), place, 0)
    coarse_kernel(
        dims, r["r2all"], *level[2], *level[3], r["u2"], r["p2"],
        r["ca"], r["cb"], r["cz"], r["r3"], r["e3a"], r["e3b"], r["cbuf"],
    )
    up_kernel(
        dims, r["u2"], x1, r["e1"], *level[1], r["rhs"], r["e0"], *level[0], sol, res, r["p3"],
        r["va"], r["vb"], r["vbuf"], r["ua"], r["ub"], r["ubuf"],
    )
    for g in gathered:
        g.wait_send()
    lane = iota((1, nz), 1)
    p0, p1, p2, p3 = (r["p%d" % k][0:1, :] for k in range(4))
    mine = jnp.where(lane == 0, p0, jnp.where(lane == 1, p1, p3))
    r["n_own"][...] = mine
    last = everyone(r["n_own"], r["n_all"], r["n_send"], r["n_recv"])
    total = jnp.sum(r["n_all"][...], axis=0)
    cells = float(nx * ny * nz * n)
    total = jnp.where(lane == 2, p2, total)
    scale = jnp.where(lane == 1, 8.0 / cells, jnp.where(lane == 2, 64.0 / cells, 1.0 / cells))
    norms[...] = jnp.sqrt(total * scale)
    last.wait_send()


def body(data, weights):
    dims = data.shape
    nx, ny, nz = dims
    gx, gy, gz = (lax.axis_size(a) for a in AXES)
    n = gx * gy * gz
    c0, y0, l0 = nx + 2 * HX[0], ny + 8, 2 * nz
    c1, y1 = nx // 2 + 2 * HX[1], ny // 2 + 16
    N2 = (nx // 4 * gx, ny // 4 * gy, nz // 4 * gz)
    N3 = tuple(v // 2 for v in N2)
    per = -(-nx // (nz // WIDTH))
    pad2 = (N2[0] + 2,) + N2[1:]
    pad3 = (N3[0] + 2,) + N3[1:]
    own2 = (nx // 4 // 4, ny // 4, nz)
    shapes = dict(
        f_low=(per, ny, nz), f_high=(per, ny, nz), g_low=(per, ny, nz), g_high=(per, ny, nz),
        ext=(c0, y0, l0), wparts=(gz, 8, nz), y_low=(c0, 8, l0), y_high=(c0, 8, l0),
        rhs=(c0, y0, l0), e0=(c0 + 2, y0, l0), r1=(nx // 2, ny // 2, nz),
        ua=(c0 + 2, y0, l0), ub=(c0 + 2, y0, l0), gz0=(c0 + 2, y0, nz), ubuf=(c0 // 2 + 2, y0, l0),
        b_own=(nx // 4, ny // 2, nz),
        x1=(c1, y1, l0), e1=(c1 + 2, y1, l0), r2=(nx // 4, ny // 4, nz),
        va=(c1 + 2, y1, l0), vb=(c1 + 2, y1, l0), gz1=(c1 + 2, y1, nz), vbuf=(c1 // 2 + 2, y1, l0),
        c_own=own2, c_all=(n,) + own2, r2all=N2, u2=(N2[0] + 8,) + N2[1:],
        ca=pad2, cb=pad2, cz=(N2[0] + 2, N2[1], N3[2]), r3=N3, e3a=pad3, e3b=pad3,
        cbuf=(N3[0] + 2,) + N2[1:], n_own=(1, nz), n_all=(n, 1, nz),
        p0=(8, nz), p1=(8, nz), p2=(8, nz), p3=(8, nz),
    )
    for d in STAR:
        shapes[star_name("b_", d)] = (HX[1] // 2 if d[0] else nx // 4, ny // 2, nz)
    scratch = {k: pltpu.VMEM(v, F32) for k, v in shapes.items()}
    for k, size in enumerate((l0, l0, N2[2], N3[2])):
        scratch["m%dh" % k] = pltpu.VMEM((size, size), BF16)
        scratch["m%dl" % k] = pltpu.VMEM((size, size), BF16)
        scratch["m%dc" % k] = pltpu.VMEM((8, size), F32)
    scratch["ah"] = scratch["al"] = pltpu.VMEM((l0, l0), BF16)
    dma = pltpu.SemaphoreType.DMA
    scratch.update(near_send=dma((10,)), near_recv=dma((10,)), w_send=dma((gz,)), w_recv=dma((gz,)))
    scratch.update(b_send=dma((8,)), b_recv=dma((8,)))
    for k in "cn":
        scratch[k + "_send"] = dma((2,))
        scratch[k + "_recv"] = dma((2,))
    words = sum(math.prod(v) for v in shapes.values()) + 2 * l0 * l0 * 3 + N2[2] * N2[2] * 2
    vmem = pl.BlockSpec(memory_space=pltpu.VMEM)
    sol, res, norms = pl.pallas_call(
        functools.partial(whole_kernel, tuple(scratch), dims),
        out_shape=[jax.ShapeDtypeStruct(s, F32) for s in (dims, dims, (1, nz))],
        in_specs=[vmem] * 2,
        out_specs=[vmem] * 3,
        scratch_shapes=list(scratch.values()),
        compiler_params=pltpu.CompilerParams(
            collective_id=0, has_side_effects=True, vmem_limit_bytes=4 * words + 6 * 1024 * 1024
        ),
    )(data, weights)
    return sol, res, norms[0, :4]


def solution(mesh):
    in_specs = (P("gx", "gy", "gz"), P(None, "gz"))
    out_specs = (P("gx", "gy", "gz"), P("gx", "gy", "gz"), P())
    return jax.shard_map(body, mesh=mesh, in_specs=in_specs, out_specs=out_specs, check_vma=False)
```

```python
import functools
import math
import jax
import jax.numpy as jnp
from jax import lax
from jax.experimental import pallas as pl
from jax.experimental.pallas import tpu as pltpu
from jax.sharding import PartitionSpec as P

HALF = 4
RELAX = 0.45
F32 = jnp.float32
BF16 = jnp.bfloat16
HX = (4, 6)
OFFSETS = [j - HALF for j in range(HALF)] + [j - HALF + 1 for j in range(HALF, 2 * HALF)]


def iota(shape, dim):
    return lax.broadcasted_iota(jnp.int32, shape, dim)


def cyclic(index, size, own):
    cut = (size + own) // 2
    return jnp.where(index < cut, index, index - size)


def split(x):
    high = x.astype(BF16)
    return high, (x - high.astype(F32)).astype(BF16)


def dot(a, b):
    return lax.dot_general(a, b, (((1,), (0,)), ((), ())), preferred_element_type=F32)


def dot3(x, mh, ml):
    h, l = split(x)
    return dot(h, mh) + dot(h, ml) + dot(l, mh)


def dot2(x, m):
    h, l = split(x)
    return dot(h, m) + dot(l, m)


def dot2l(m, x):
    h, l = split(x)
    return dot(m, h) + dot(m, l)


def restrict_matrix(fine, coarse, axis):
    k = fine - 2 * coarse + 1
    m = jnp.where((k == 0) | (k == 3), 0.125, jnp.where((k == 1) | (k == 2), 0.375, 0.0))
    return m.astype(F32)


def prolong_matrix(fine, coarse, limit):
    centre = fine >> 1
    other = jnp.where((fine & 1) == 1, centre + 1, centre - 1)
    m = jnp.where(coarse == centre, 0.75, jnp.where(coarse == other, 0.25, 0.0))
    return jnp.where((fine >= 0) & (fine < limit), m, 0.0).astype(F32)


def build_level(level, nz, whole, wall, start, *outs):
    z0 = lax.axis_index("gz") * nz
    own = nz >> level
    total = whole >> level
    size = 2 * nz if level < 2 else total
    base = z0 >> level if level < 2 else 0

    def place(index):
        return cyclic(index, size, own) if level < 2 else index

    g = (iota((wall.shape[1], size), 0) + start) >> level
    p = place(iota((wall.shape[1], size), 1)) + base
    pick = jnp.where(g == p, 0.5**level, 0.0).astype(F32)
    w = lax.dot_general(
        wall, pick, (((1,), (0,)), ((), ())),
        preferred_element_type=F32, precision=lax.Precision.HIGHEST,
    )
    pr = place(iota((size, size), 0))
    pc = place(iota((size, size), 1))
    ok = (pr + base >= 0) & (pr + base < total) & (pc + base >= 0) & (pc + base < total)
    diff = pr - pc
    at = jnp.where(diff == 0, 1.0, 0.0).astype(F32)
    for j, offset in enumerate(OFFSETS):
        at = at + jnp.where(diff == offset, w[j : j + 1, :], 0.0)
    at = jnp.where(ok, at, 0.0)
    a = at.T
    stiff = 0.25**level
    m = lax.dot_general(
        at, a, (((1,), (0,)), ((), ())),
        preferred_element_type=F32, precision=lax.Precision.HIGHEST,
    )
    lap = jnp.where(diff == 0, 6.0, jnp.where((diff == 1) | (diff == -1), -1.0, 0.0))
    m = m + jnp.where(ok, stiff * lap, 0.0)
    d = jnp.sum(jnp.where(diff == 0, m, 0.0), axis=0, keepdims=True)
    col = place(iota((1, size), 1)) + base
    inside = (col >= 0) & (col < total)
    safe = jnp.where(inside, d, 1.0)
    c = jnp.where(inside, RELAX / safe, 0.0)
    inv = jnp.where(inside, safe * (1.0 / RELAX), 0.0)
    mh, ml = split(m * c)
    o = outs
    o[0][...] = mh
    o[1][...] = ml
    o[2][0:1, :] = c
    o[2][1:2, :] = inv
    if level == 0:
        ah, al = split(a)
        o[3][...] = ah
        o[4][...] = al


def chunk_of(count, rows, most):
    best = 1
    for planes in range(1, count + 1):
        if count % planes == 0 and planes * rows <= most:
            best = planes
    return best


def sweep(src, r_at, emit, first, count, stiff, mats, xmask, ymask, init=None, own=None, most=800):
    mh, ml, cv = mats
    rows, size = src.shape[1], src.shape[2]
    planes = chunk_of(count, rows, most)
    keep, lo, hi = own or (rows, 0, size)
    c = cv[0:1, lo:hi]
    inv = cv[1:2, lo:hi]
    yi = iota((rows, hi - lo), 0)

    def step(k, carry):
        x0 = first + k * planes
        u = src[pl.ds(x0, planes), 0:keep, :]
        um = dot3(u.reshape(planes * keep, size), mh[:, lo:hi], ml[:, lo:hi])
        for p in range(planes):
            x = x0 + p
            uc = src[x, :, lo:hi]
            low = pltpu.roll(uc, 1, 0)
            high = pltpu.roll(uc, rows - 1, 0)
            if ymask is None:
                low = jnp.where(yi == 0, 0.0, low)
                high = jnp.where(yi == rows - 1, 0.0, high)
            side = src[x - 1, 0:keep, lo:hi] + src[x + 1, 0:keep, lo:hi]
            nb = side + (low + high)[0:keep]
            if ymask is None:
                nb = nb * stiff
            else:
                nb = nb * (ymask[0:keep, lo:hi] * (xmask(x) * stiff))
            delta = c * (r_at(x)[0:keep, lo:hi] + nb) - um[p * keep : (p + 1) * keep]
            carry = emit(x, uc[0:keep], delta, inv, carry)
        return carry

    return lax.fori_loop(0, count // planes, step, init)


def restrict(gz, first, count, ry, out, lanes):
    group = chunk_of(count, 1, 8)

    def step(k, carry):
        values = []
        for j in range(group):
            x = first + 2 * (k * group + j)
            t = (gz[x - 1] + 3.0 * gz[x] + 3.0 * gz[x + 1] + gz[x + 2]) * 0.125
            values.append(dot2l(ry, t))
        for j in range(group):
            out(k * group + j, values[j])
        return carry

    lax.fori_loop(0, count // group, step, 0)


def inside_mask(base, limit, pad):
    def mask(x):
        g = base + x - pad
        return jnp.where((g >= 0) & (g < limit), 1.0, 0.0).astype(F32)

    return mask


def y_mask(rows, size, own, base, limit):
    y = cyclic(iota((rows, size), 0), rows, own) + base
    return jnp.where((y >= 0) & (y < limit), 1.0, 0.0).astype(F32)


def zero_planes(ref, *planes):
    for x in planes:
        ref[x] = jnp.zeros(ref.shape[1:], F32)


def geometry(level, dims):
    nx, ny, nz = (v >> level for v in dims)
    gx, gy = lax.axis_size("gx"), lax.axis_size("gy")
    return dict(
        nx=nx, ny=ny, nz=nz, x0=lax.axis_index("gx") * nx, y0=lax.axis_index("gy") * ny,
        z0=lax.axis_index("gz") * nz, NX=nx * gx, NY=ny * gy, NZ=nz * lax.axis_size("gz"),
    )


def down_kernel(level, dims, *refs):
    if level == 0:
        ext, ah, al, mh, ml, cv, rhs, eb, r_next, part, ua, gz = refs
    else:
        rhs, mh, ml, cv, eb, r_next, part, ua, gz = refs
    geo = geometry(level, dims)
    nx, ny, nz = geo["nx"], geo["ny"], geo["nz"]
    hx = HX[level]
    count = nx + 2 * hx
    rows, size = ua.shape[1], ua.shape[2]
    pad = hx + 1
    c = cv[0:1, :]
    zero_planes(ua, 0, count + 1)
    reach = hx - 1 - level
    zero_planes(eb, *range(pad - reach), *range(pad + nx + reach, count + 2))
    if level == 0:
        planes = chunk_of(count, rows, 448)

        def first(k, carry):
            x0 = k * planes
            r = dot3(ext[pl.ds(x0, planes)].reshape(planes * rows, size), ah[...], al[...])
            for p in range(planes):
                rp = r[p * rows : (p + 1) * rows]
                rhs[x0 + p] = rp
                ua[x0 + p + 1] = c * rp
            return carry

        lax.fori_loop(0, count // planes, first, 0)
    else:

        def first(x, carry):
            ua[x + 1] = c * rhs[x]
            return carry

        lax.fori_loop(0, count, first, 0)
    xmask = inside_mask(geo["x0"], geo["NX"], pad)
    ymask = y_mask(rows, size, ny, geo["y0"], geo["NY"])
    mats = (mh, ml, cv)
    stiff = 0.25**level

    def r_at(x):
        return rhs[x - 1]

    def keep(x, u, delta, inv, carry):
        eb[x] = u + delta
        return carry

    sweep(ua, r_at, keep, pad - reach, nx + 2 * reach, stiff, mats, xmask, ymask, 0)
    lanes = gz.shape[2]
    fine = cyclic(iota((size, lanes), 0), size, nz)
    coarse = iota((size, lanes), 1)
    rz = jnp.where(coarse < nz // 2, restrict_matrix(fine, coarse, 0), 0.0).astype(BF16)
    ry = restrict_matrix(
        cyclic(iota((ny // 2, rows), 1), rows, ny), iota((ny // 2, rows), 0), 1
    ).astype(BF16)

    def defect(x, u, delta, inv, carry):
        g = delta * inv
        gz[x] = dot2(g, rz)
        mine = g[0:ny, 0:nz]
        return carry + mine * mine * jnp.where((x >= pad) & (x < pad + nx), 1.0, 0.0).astype(F32)

    total = sweep(
        eb, r_at, defect, pad - 1, nx + 2, stiff, mats, xmask, ymask, jnp.zeros((ny, nz), F32)
    )
    part[...] = jnp.full(part.shape, jnp.sum(total), F32)

    def put(i, value):
        r_next[i] = value

    restrict(gz, pad, nx // 2, ry, put, lanes)


def late_kernel(dims, ext, ah, al, mh, ml, cv, rhs, eb, ua):
    geo = geometry(0, dims)
    nx, ny, nz = geo["nx"], geo["ny"], geo["nz"]
    hx = HX[0]
    count, pad, reach = nx + 2 * hx, hx + 1, hx - 1
    rows, size = ua.shape[1], ua.shape[2]
    c = cv[0:1, nz:size]
    planes = chunk_of(count, rows, 448)

    def first(k, carry):
        x0 = k * planes
        r = dot3(ext[pl.ds(x0, planes)].reshape(planes * rows, size), ah[:, nz:size], al[:, nz:size])
        for p in range(planes):
            rp = r[p * rows : (p + 1) * rows]
            rhs[x0 + p, :, nz:size] = rp
            ua[x0 + p + 1, :, nz:size] = c * rp
        return carry

    lax.fori_loop(0, count // planes, first, 0)
    xmask = inside_mask(geo["x0"], geo["NX"], pad)
    ymask = y_mask(rows, size, ny, geo["y0"], geo["NY"])

    def keep(x, u, delta, inv, carry):
        eb[x, :, nz:size] = u + delta
        return carry

    sweep(
        ua, lambda x: rhs[x - 1], keep, pad - reach, nx + 2 * reach, 1.0, (mh, ml, cv), xmask, ymask,
        0, (rows, nz, size),
    )


def prolong_into(coarse_ref, coarse_first, coarse_count, pz, py, buf, error, dst, xmask):
    group = chunk_of(coarse_count, 1, 11)
    rows, size = coarse_ref.shape[1:]

    def step(k, carry):
        z = coarse_ref[pl.ds(coarse_first + k * group, group)]
        z = dot2(z.reshape(group * rows, size), pz)
        values = [dot2l(py, z[j * rows : (j + 1) * rows]) for j in range(group)]
        for j in range(group):
            buf[k * group + j] = values[j]
        return carry

    lax.fori_loop(0, coarse_count // group, step, 0)

    def join(i, carry):
        x = 1 + 2 * (i - 1)
        mid = 0.75 * buf[i]
        dst[x] = error(x) + xmask(x) * (mid + 0.25 * buf[i - 1])
        dst[x + 1] = error(x + 1) + xmask(x + 1) * (mid + 0.25 * buf[i + 1])
        return carry

    lax.fori_loop(1, coarse_count - 1, join, 0)


def coarse_kernel(dims, r2, m2h, m2l, c2, m3h, m3l, c3, u2, part, ua, ub, gz, r3, e3a, e3b, buf):
    g2 = geometry(2, dims)
    g3 = geometry(3, dims)
    N2, N3 = g2["NX"], g3["NX"]
    pad = 4
    one = lambda x: 1.0
    for ref in (ua, ub):
        zero_planes(ref, 0, N2 + 1)
    zero_planes(e3a, 0, N3 + 1)
    zero_planes(e3b, 0, N3 + 1)
    zero_planes(gz, 0, N2 + 1)
    zero_planes(u2, *range(pad), *range(N2 + pad, N2 + 2 * pad))
    mats2, mats3 = (m2h, m2l, c2), (m3h, m3l, c3)
    cc = c2[0:1, :]

    def first(x, carry):
        ua[x + 1] = cc * r2[x]
        return carry

    lax.fori_loop(0, N2, first, 0)
    r_at = lambda x: r2[x - 1]

    def into(ref, shift=0):
        def emit(x, u, delta, inv, carry):
            ref[x + shift] = u + delta
            return carry

        return emit

    s2, s3 = 0.25**2, 0.25**3
    sweep(ua, r_at, into(ub), 1, N2, s2, mats2, one, None, 0)
    NY2, NZ2, NY3, NZ3 = g2["NY"], g2["NZ"], g3["NY"], g3["NZ"]
    rz = restrict_matrix(iota((NZ2, NZ3), 0), iota((NZ2, NZ3), 1), 0).astype(BF16)
    ry = restrict_matrix(iota((NY3, NY2), 1), iota((NY3, NY2), 0), 1).astype(BF16)

    def defect(x, u, delta, inv, carry):
        g = delta * inv
        gz[x] = dot2(g, rz)
        return carry + g * g

    total = sweep(ub, r_at, defect, 1, N2, s2, mats2, one, None, jnp.zeros((NY2, NZ2), F32))
    part[...] = jnp.full(part.shape, jnp.sum(total), F32)
    c3v = c3[0:1, :]

    def put(i, value):
        r3[i] = value
        e3a[i + 1] = c3v * value

    restrict(gz, 1, N3, ry, put, NZ3)
    sweep(e3a, lambda x: r3[x - 1], into(e3b), 1, N3, s3, mats3, one, None, 0)
    pz = prolong_matrix(iota((NZ3, NZ2), 1), iota((NZ3, NZ2), 0), NZ2).astype(BF16)
    py = prolong_matrix(iota((NY2, NY3), 0), iota((NY2, NY3), 1), NY2).astype(BF16)
    prolong_into(e3b, 0, N3 + 2, pz, py, buf, lambda x: ub[x], ua, one)
    sweep(ua, r_at, into(ub), 1, N2, s2, mats2, one, None, 0)
    sweep(ub, r_at, into(u2, pad - 1), 1, N2, s2, mats2, one, None, 0)


def up_kernel(dims, u2, r1, e1, m1h, m1l, c1, rhs, e0, m0h, m0l, c0, sol, res, part,
              va, vb, vbuf, ua, ub, ubuf):
    g0, g1, g2 = geometry(0, dims), geometry(1, dims), geometry(2, dims)
    rows, size = va.shape[1], va.shape[2]
    count = g1["nx"] + 2 * HX[1]
    zero_planes(va, 0, count + 1)
    zero_planes(vb, 0, count + 1)
    xmask = inside_mask(g1["x0"], g1["NX"], HX[1] + 1)
    ymask = y_mask(rows, size, g1["ny"], g1["y0"], g1["NY"])
    NY2, NZ2 = g2["NY"], g2["NZ"]
    pz = prolong_matrix(
        cyclic(iota((NZ2, size), 1), size, g1["nz"]) + g1["z0"], iota((NZ2, size), 0), g1["NZ"]
    ).astype(BF16)
    py = prolong_matrix(
        cyclic(iota((rows, NY2), 0), rows, g1["ny"]) + g1["y0"], iota((rows, NY2), 1), g1["NY"]
    ).astype(BF16)
    first = g2["x0"] + 4 - HX[1] // 2 - 1
    prolong_into(u2, first, count // 2 + 2, pz, py, vbuf, lambda x: e1[x], va, xmask)
    mats = (m1h, m1l, c1)

    def into(ref):
        def emit(x, u, delta, inv, carry):
            ref[x] = u + delta
            return carry

        return emit

    r1_at = lambda x: r1[x - 1]
    q, n1 = HX[1] + 1, g1["nx"]
    sweep(va, r1_at, into(vb), q - 3, n1 + 6, 0.25, mats, xmask, ymask, 0)
    sweep(vb, r1_at, into(va), q - 2, n1 + 4, 0.25, mats, xmask, ymask, 0)
    rows0, size0 = ua.shape[1], ua.shape[2]
    count0 = g0["nx"] + 2 * HX[0]
    nx, ny, nz = g0["nx"], g0["ny"], g0["nz"]
    pad = HX[0] + 1
    zero_planes(ua, 0, count0 + 1)
    zero_planes(ub, 0, count0 + 1)
    xmask0 = inside_mask(g0["x0"], g0["NX"], pad)
    ymask0 = y_mask(rows0, size0, ny, g0["y0"], g0["NY"])
    pz = prolong_matrix(
        cyclic(iota((size, size0), 1), size0, nz) + g0["z0"],
        cyclic(iota((size, size0), 0), size, g1["nz"]) + g1["z0"], g0["NZ"],
    ).astype(BF16)
    py = prolong_matrix(
        cyclic(iota((rows0, rows), 0), rows0, ny) + g0["y0"],
        cyclic(iota((rows0, rows), 1), rows, g1["ny"]) + g1["y0"], g0["NY"],
    ).astype(BF16)
    first = HX[1] + 1 - HX[0] // 2 - 1
    prolong_into(va, first, count0 // 2 + 2, pz, py, ubuf, lambda x: e0[x], ua, xmask0)
    mats0 = (m0h, m0l, c0)
    r0_at = lambda x: rhs[x - 1]
    sweep(ua, r0_at, into(ub), pad - 2, nx + 4, 1.0, mats0, xmask0, ymask0, 0)
    sweep(ub, r0_at, into(ua), pad - 1, nx + 2, 1.0, mats0, xmask0, ymask0, 0)

    def final(x, u, delta, inv, carry):
        g = delta * inv
        sol[x - pad] = u
        res[x - pad] = g
        return carry + g * g

    total = sweep(
        ua, r0_at, final, pad, nx, 1.0, mats0, xmask0, ymask0, jnp.zeros((ny, nz), F32), (ny, 0, nz)
    )
    part[...] = jnp.full(part.shape, jnp.sum(total), F32)


AXES = ("gx", "gy", "gz")
MESH = pl.DeviceIdType.MESH
FIRST, WIDTH = 5 * HALF + 1, 10 * HALF


class Pair:
    def __init__(self, axis, up, down, sends, recvs, slot):
        n, me = lax.axis_size(axis), lax.axis_index(axis)
        self.has_low, self.has_high = me > 0, me < n - 1

        def copy(refs, k, target):
            return pltpu.make_async_remote_copy(
                src_ref=refs[0], dst_ref=refs[1], send_sem=sends.at[k], recv_sem=recvs.at[k],
                device_id={axis: target}, device_id_type=MESH,
            )

        self.up = copy(up, slot, lax.rem(me + 1, n))
        self.down = copy(down, slot + 1, lax.rem(me + n - 1, n))

    def start(self):
        pl.when(self.has_high)(self.up.start)
        pl.when(self.has_low)(self.down.start)

    def wait(self):
        pl.when(self.has_low)(self.up.wait_recv)
        pl.when(self.has_high)(self.down.wait_recv)

    def sent(self):
        pl.when(self.has_high)(self.up.wait_send)
        pl.when(self.has_low)(self.down.wait_send)

    def clear(self, low, high):
        @pl.when(jnp.logical_not(self.has_low))
        def _():
            low[...] = jnp.zeros(low.shape, F32)

        @pl.when(jnp.logical_not(self.has_high))
        def _():
            high[...] = jnp.zeros(high.shape, F32)


class Star:
    def __init__(self, moves, src, dst, sends, recvs):
        gx, gz = lax.axis_size("gx"), lax.axis_size("gz")
        mx, mz = lax.axis_index("gx"), lax.axis_index("gz")
        self.moves = []
        for k, (dx, dz) in enumerate(moves):
            to = (mx + dx >= 0) & (mx + dx < gx) & (mz + dz >= 0) & (mz + dz < gz)
            frm = (mx - dx >= 0) & (mx - dx < gx) & (mz - dz >= 0) & (mz - dz < gz)
            into = dst(-dx, -dz)
            copy = pltpu.make_async_remote_copy(
                src_ref=src(dx, dz), dst_ref=into, send_sem=sends.at[k], recv_sem=recvs.at[k],
                device_id={"gx": lax.rem(mx + dx + gx, gx), "gz": lax.rem(mz + dz + gz, gz)},
                device_id_type=MESH,
            )
            self.moves.append((to, frm, copy, into))

    def clear(self):
        for _, frm, _, into in self.moves:

            @pl.when(jnp.logical_not(frm))
            def _(into=into):
                into[...] = jnp.zeros(into.shape, F32)

    def start(self):
        for to, _, copy, _ in self.moves:
            pl.when(to)(copy.start)

    def wait(self):
        for _, frm, copy, _ in self.moves:
            pl.when(frm)(copy.wait_recv)

    def sent(self):
        for to, _, copy, _ in self.moves:
            pl.when(to)(copy.wait_send)


SKEW = [(dx, dz) for dx in (-1, 1) for dz in (-1, 1)]
STAR = SKEW + [(0, -1), (0, 1), (-1, 0), (1, 0)]


def star_name(prefix, d):
    return prefix + "mop"[d[0] + 1] + "mop"[d[1] + 1]


def linear():
    gy, gz = lax.axis_size("gy"), lax.axis_size("gz")
    return (lax.axis_index("gx") * gy + lax.axis_index("gy")) * gz + lax.axis_index("gz")


def coordinates(t):
    gy, gz = lax.axis_size("gy"), lax.axis_size("gz")
    return (t // (gy * gz), lax.rem(t // gz, gy), lax.rem(t, gz))


def device_count():
    return lax.axis_size("gx") * lax.axis_size("gy") * lax.axis_size("gz")


def near_devices():
    sizes, me = [lax.axis_size(a) for a in AXES], [lax.axis_index(a) for a in AXES]
    out = []
    for move in [(dx, 0, dz) for dx, dz in STAR] + [(0, -1, 0), (0, 1, 0)]:
        if all(n > 1 or d == 0 for n, d in zip(sizes, move)):
            at = [i + d for i, d in zip(me, move)]
            there = functools.reduce(jnp.logical_and, [(i >= 0) & (i < n) for i, n in zip(at, sizes)])
            out.append((there, tuple(lax.rem(i + n, n) for i, n in zip(at, sizes))))
    return out


def reached():
    return lax.axis_size("gx") <= 4 and lax.axis_size("gy") <= 2 and lax.axis_size("gz") <= 4


def signal_all():
    n, me = device_count(), linear()
    barrier = pltpu.get_barrier_semaphore()
    if reached():
        for there, device in near_devices():

            @pl.when(there)
            def _():
                pl.semaphore_signal(barrier, inc=1, device_id=device, device_id_type=MESH)

        return

    def step(k, carry):
        pl.semaphore_signal(
            barrier, inc=1, device_id=coordinates(lax.rem(me + k, n)), device_id_type=MESH
        )
        return carry

    lax.fori_loop(1, n, step, 0)


def wait_all():
    if reached():
        count = sum(there.astype(jnp.int32) for there, _ in near_devices())
        pl.semaphore_wait(pltpu.get_barrier_semaphore(), count)
        return
    pl.semaphore_wait(pltpu.get_barrier_semaphore(), device_count() - 1)


def shifted(axis, d):
    n = lax.axis_size(axis)
    t = lax.axis_index(axis) + d
    return jnp.where(t >= n, t - n, t)


def arrived(buf, count, sends, recvs, k, axis):
    part = buf.at[0:count]
    return pltpu.make_async_remote_copy(
        src_ref=part, dst_ref=part, send_sem=sends.at[k], recv_sem=recvs.at[k],
        device_id={axis: shifted(axis, 1)}, device_id_type=MESH,
    )


def spread(block, buf, slot, sends, recvs, k, sizes):
    for dx in range(sizes[0]):
        for dy in range(sizes[1]):
            for dz in range(sizes[2]):
                if dx or dy or dz:
                    pltpu.make_async_remote_copy(
                        src_ref=block, dst_ref=buf.at[slot], send_sem=sends.at[k], recv_sem=recvs.at[k],
                        device_id=(shifted("gx", dx), shifted("gy", dy), shifted("gz", dz)),
                        device_id_type=MESH,
                    ).start()


def everyone(block, buf, sends, recvs):
    n, me = device_count(), linear()
    spread(block, buf, me, sends, recvs, 0, [lax.axis_size(a) for a in AXES])
    buf[me] = block[...]
    done = arrived(buf, n - 1, sends, recvs, 0, "gz")
    done.wait_recv()
    return done


def by_columns(block, buf, sends, recvs):
    gx, gy, gz = (lax.axis_size(a) for a in AXES)
    m, y = gx * gz, lax.axis_index("gy")
    slot = y * m + lax.axis_index("gx") * gz + lax.axis_index("gz")
    spread(block, buf, slot, sends, recvs, 0, (gx, 1, gz))
    buf[slot] = block[...]
    first = arrived(buf, m - 1, sends, recvs, 0, "gz")
    mine = buf.at[pl.ds(y * m, m)]
    second = arrived(buf, (gy - 1) * m, sends, recvs, 1, "gy")

    def finish():
        first.wait_recv()
        for d in range(1, gy):
            pltpu.make_async_remote_copy(
                src_ref=mine, dst_ref=mine, send_sem=sends.at[1], recv_sem=recvs.at[1],
                device_id={"gy": shifted("gy", d)}, device_id_type=MESH,
            ).start()
        second.wait_recv()
        return first, second

    return finish


def pack_faces(data, low, high, start, stop):
    nx, ny, nz = data.shape
    width = stop - start
    slots = nz // width
    rest = jnp.zeros((ny, nz - slots * width), F32)
    for i in range(low.shape[0]):
        planes = [min(i * slots + k, nx - 1) for k in range(slots)]
        low[i] = jnp.concatenate([data[x][:, start:stop] for x in planes] + [rest], axis=1)
        high[i] = jnp.concatenate([data[x][:, nz - stop : nz - start] for x in planes] + [rest], axis=1)


def face_pieces(nx, hx, nz, width):
    slots = nz // width
    return {
        -1: slice(0, -(-hx // slots)),
        0: slice(0, -(-nx // slots)),
        1: slice((nx - hx) // slots, -(-nx // slots)),
    }


def unpack_faces(dims, parts, widths, ext, hx):
    nx, ny, nz = dims
    for dx in (-1, 0, 1):
        source = nx - hx if dx < 0 else 0
        target = {-1: 0, 0: hx, 1: hx + nx}[dx]
        for i in range(nx if dx == 0 else hx):
            ends = {}
            for dz in (-1, 1):
                ends[dz] = []
                for part, width in zip(parts, widths):
                    slots = nz // width
                    first = (nx - hx) // slots if dx < 0 else 0
                    x = source + i
                    lane = x % slots * width
                    ends[dz].append(part(dx, dz)[x // slots - first][:, lane : lane + width])
            gap = jnp.zeros((ny, nz - 2 * sum(widths)), F32)
            ext[target + i, 0:ny, nz:] = jnp.concatenate(ends[1] + [gap] + ends[-1][::-1], axis=1)


def whole_kernel(names, dims, data, weights, sol, res, norms, *scratch):
    r = dict(zip(names, scratch))
    nx, ny, nz = dims
    n, gz = device_count(), lax.axis_size("gz")
    ns, nr = r["near_send"], r["near_recv"]
    signal_all()
    pack_faces(data, r["f1_low"], r["f1_high"], 0, FIRST)
    ext, hx, weights_row = r["ext"], HX[0], iota((8, 2 * nz), 0)
    for x in range(nx):
        ext[hx + x, 0:ny, 0:nz] = data[x]
    wait_all()
    near = Pair("gz", (weights, r["w_low"]), (weights, r["w_high"]), ns, nr, 0)
    near.start()
    widths = (FIRST, WIDTH - FIRST)
    pieces = [face_pieces(nx, hx, nz, w) for w in widths]

    def faces(part):
        def send(dx, dz):
            return r["f%d_%s" % (part, "low" if dz < 0 else "high")].at[pieces[part - 1][dx]]

        def take(dx, dz):
            return r[star_name("g%d_" % part, (dx, dz))]

        return send, take

    send1, take1 = faces(1)
    send2, take2 = faces(2)

    def plane_send(dx, dz):
        if dz:
            return send1(dx, dz)
        return data.at[0:hx] if dx < 0 else data.at[nx - hx : nx]

    def plane_take(dx, dz):
        if dz:
            return take1(dx, dz)
        return ext.at[0:hx, 0:ny, 0:nz] if dx < 0 else ext.at[nx + hx : nx + 2 * hx, 0:ny, 0:nz]

    star = Star(STAR, plane_send, plane_take, r["s_send"], r["s_recv"])
    star.start()
    star.clear()
    near.clear(r["w_low"], r["w_high"])
    late = Star(STAR[:6], send2, take2, r["l_send"], r["l_recv"])
    late.clear()
    pack_faces(data, r["f2_low"], r["f2_high"], FIRST, WIDTH)
    level = [[r["m%d%s" % (k, t)] for t in "hlc"] for k in range(4)]
    near.wait()
    nearby = jnp.concatenate([r["w_low"][...], weights[...], r["w_high"][...]], axis=1)
    start = (lax.axis_index("gz") - 1) * nz
    build_level(0, nz, nz * gz, nearby, start, *level[0], r["ah"], r["al"])
    star.wait()
    late.start()
    unpack_faces(dims, (take1,), widths[:1], ext, hx)
    ys = Pair("gy", (ext.at[:, ny - 8 : ny, :], r["y_low"]), (ext.at[:, 0:8, :], r["y_high"]), ns, nr, 2)
    ys.clear(r["y_low"], r["y_high"])
    ys.start()
    ys.wait()
    star.sent()
    near.sent()
    ys.sent()
    upper = weights_row < 4

    def join(x, carry):
        ext[x, ny : ny + 8, :] = jnp.where(upper, r["y_high"][x], r["y_low"][x])
        return carry

    lax.fori_loop(0, nx + 2 * hx, join, 0)
    down_kernel(0, dims, ext, r["ah"], r["al"], *level[0], r["rhs"], r["e0"], r["r1"], r["p0"], r["ua"], r["gz0"])
    n1, m1, k1 = nx // 2, ny // 2, nz // 2
    h1 = HX[1]
    x1, r1, own = r["x1"], r["r1"], r["b_own"]
    for a in range(n1 // 2):
        own[a] = jnp.concatenate([r1[2 * a][:, :k1], r1[2 * a + 1][:, :k1]], axis=1)
    bufs = {d: r[star_name("b_", d)] for d in STAR}
    rim = h1 // 2
    cut = {-1: slice(0, rim), 0: slice(0, n1 // 2), 1: slice(n1 // 2 - rim, n1 // 2)}
    star = Star(
        STAR, lambda dx, dz: own.at[cut[dx]], lambda dx, dz: bufs[(dx, dz)], r["b_send"], r["b_recv"]
    )
    star.start()
    star.clear()
    build_level(1, nz, nz * gz, nearby, start, *level[1])
    late.wait()
    unpack_faces(dims, (take1, take2), widths, ext, hx)
    far = slice(nz, 2 * nz)
    late_ys = Pair(
        "gy", (ext.at[:, ny - 8 : ny, far], r["z_low"]), (ext.at[:, 0:8, far], r["z_high"]), ns, nr, 4
    )
    late_ys.clear(r["z_low"], r["z_high"])
    late_ys.start()
    star.wait()
    spread(weights, r["wparts"], lax.axis_index("gz"), r["w_send"], r["w_recv"], 0, (1, 1, gz))
    bufs[(0, 0)] = own
    blank = jnp.zeros((m1, k1), F32)
    for dx in (-1, 0, 1):
        base = h1 + dx * h1 if dx < 1 else h1 + n1
        for x in range(n1 if dx == 0 else h1):
            a, part = x // 2, slice((x % 2) * k1, (x % 2 + 1) * k1)
            low, mid, high = (bufs[(dx, dz)][a][:, part] for dz in (-1, 0, 1))
            x1[base + x, 0:m1, :] = jnp.concatenate([mid, high, blank, low], axis=1)
    ys = Pair(
        "gy",
        (x1.at[:, m1 - 8 : m1, :], x1.at[:, m1 + 8 : m1 + 16, :]),
        (x1.at[:, 0:8, :], x1.at[:, m1 : m1 + 8, :]),
        ns, nr, 8,
    )
    ys.clear(x1.at[:, m1 + 8 : m1 + 16, :], x1.at[:, m1 : m1 + 8, :])
    ys.start()
    ys.wait()
    star.sent()
    ys.sent()
    down_kernel(1, dims, x1, *level[1], r["e1"], r["r2"], r["p1"], r["va"], r["gz1"])
    n2, m2, k2 = nx // 4, ny // 4, nz // 4
    slots = nz // k2
    per = n2 // slots
    for a in range(per):
        r["c_own"][a] = jnp.concatenate([r["r2"][q * per + a][:, :k2] for q in range(slots)], axis=1)
    finish = by_columns(r["c_own"], r["c_all"], r["c_send"], r["c_recv"])
    late_ys.wait()

    def late_join(x, carry):
        ext[x, ny : ny + 8, far] = jnp.where(upper[:, far], r["z_high"][x], r["z_low"][x])
        return carry

    lax.fori_loop(0, nx + 2 * hx, late_join, 0)
    late_kernel(dims, ext, r["ah"], r["al"], *level[0], r["rhs"], r["e0"], r["ua"])
    r["wparts"][lax.axis_index("gz")] = weights[...]
    given = arrived(r["wparts"], gz - 1, r["w_send"], r["w_recv"], 0, "gz")
    given.wait_recv()
    wall = jnp.concatenate([r["wparts"][i] for i in range(gz)], axis=1)
    build_level(2, nz, nz * gz, wall, 0, *level[2])
    build_level(3, nz, nz * gz, wall, 0, *level[3])
    gathered = finish()
    gx, gy = lax.axis_size("gx"), lax.axis_size("gy")

    def place(i, carry):
        for j in range(gy):
            for x in range(n2):
                q, a = x // per, x % per
                r["r2all"][i * n2 + x, j * m2 : (j + 1) * m2, :] = jnp.concatenate(
                    [r["c_all"][(j * gx + i) * gz + k, a][:, q * k2 : (q + 1) * k2] for k in range(gz)],
                    axis=1,
                )
        return carry

    lax.fori_loop(0, lax.axis_size("gx"), place, 0)
    coarse_kernel(
        dims, r["r2all"], *level[2], *level[3], r["u2"], r["p2"],
        r["ca"], r["cb"], r["cz"], r["r3"], r["e3a"], r["e3b"], r["cbuf"],
    )
    up_kernel(
        dims, r["u2"], x1, r["e1"], *level[1], r["rhs"], r["e0"], *level[0], sol, res, r["p3"],
        r["va"], r["vb"], r["vbuf"], r["ua"], r["ub"], r["ubuf"],
    )
    for g in gathered + (given,):
        g.wait_send()
    late.sent()
    late_ys.sent()
    lane = iota((1, nz), 1)
    p0, p1, p2, p3 = (r["p%d" % k][0:1, :] for k in range(4))
    mine = jnp.where(lane == 0, p0, jnp.where(lane == 1, p1, p3))
    r["n_own"][...] = mine
    last = everyone(r["n_own"], r["n_all"], r["n_send"], r["n_recv"])
    total = jnp.sum(r["n_all"][...], axis=0)
    cells = float(nx * ny * nz * n)
    total = jnp.where(lane == 2, p2, total)
    scale = jnp.where(lane == 1, 8.0 / cells, jnp.where(lane == 2, 64.0 / cells, 1.0 / cells))
    norms[...] = jnp.sqrt(total * scale)
    last.wait_send()


def body(data, weights):
    dims = data.shape
    nx, ny, nz = dims
    gx, gy, gz = (lax.axis_size(a) for a in AXES)
    n = gx * gy * gz
    c0, y0, l0 = nx + 2 * HX[0], ny + 8, 2 * nz
    c1, y1 = nx // 2 + 2 * HX[1], ny // 2 + 16
    N2 = (nx // 4 * gx, ny // 4 * gy, nz // 4 * gz)
    N3 = tuple(v // 2 for v in N2)
    pad2 = (N2[0] + 2,) + N2[1:]
    pad3 = (N3[0] + 2,) + N3[1:]
    own2 = (nx // 4 // 4, ny // 4, nz)
    shapes = dict(
        ext=(c0, y0, l0), wparts=(gz, 8, nz), w_low=(8, nz), w_high=(8, nz), z_low=(c0, 8, nz), z_high=(c0, 8, nz), y_low=(c0, 8, l0), y_high=(c0, 8, l0),
        rhs=(c0, y0, l0), e0=(c0 + 2, y0, l0), r1=(nx // 2, ny // 2, nz),
        ua=(c0 + 2, y0, l0), ub=(c0 + 2, y0, l0), gz0=(c0 + 2, y0, nz), ubuf=(c0 // 2 + 2, y0, l0),
        b_own=(nx // 4, ny // 2, nz),
        x1=(c1, y1, l0), e1=(c1 + 2, y1, l0), r2=(nx // 4, ny // 4, nz),
        va=(c1 + 2, y1, l0), vb=(c1 + 2, y1, l0), gz1=(c1 + 2, y1, nz), vbuf=(c1 // 2 + 2, y1, l0),
        c_own=own2, c_all=(n,) + own2, r2all=N2, u2=(N2[0] + 8,) + N2[1:],
        ca=pad2, cb=pad2, cz=(N2[0] + 2, N2[1], N3[2]), r3=N3, e3a=pad3, e3b=pad3,
        cbuf=(N3[0] + 2,) + N2[1:], n_own=(1, nz), n_all=(n, 1, nz),
        p0=(8, nz), p1=(8, nz), p2=(8, nz), p3=(8, nz),
    )
    for part, width in ((1, FIRST), (2, WIDTH - FIRST)):
        planes = {k: v.stop - v.start for k, v in face_pieces(nx, HX[0], nz, width).items()}
        for side in ("low", "high"):
            shapes["f%d_%s" % (part, side)] = (planes[0], ny, nz)
        for d in STAR[:6]:
            shapes[star_name("g%d_" % part, d)] = (planes[-d[0]], ny, nz)
    for d in STAR:
        shapes[star_name("b_", d)] = (HX[1] // 2 if d[0] else nx // 4, ny // 2, nz)
    scratch = {k: pltpu.VMEM(v, F32) for k, v in shapes.items()}
    for k, size in enumerate((l0, l0, N2[2], N3[2])):
        scratch["m%dh" % k] = pltpu.VMEM((size, size), BF16)
        scratch["m%dl" % k] = pltpu.VMEM((size, size), BF16)
        scratch["m%dc" % k] = pltpu.VMEM((8, size), F32)
    scratch["ah"] = scratch["al"] = pltpu.VMEM((l0, l0), BF16)
    dma = pltpu.SemaphoreType.DMA
    scratch.update(near_send=dma((10,)), near_recv=dma((10,)), w_send=dma((1,)), w_recv=dma((1,)))
    for k in "bsl":
        scratch[k + "_send"] = dma((8,))
        scratch[k + "_recv"] = dma((8,))
    for k in "cn":
        scratch[k + "_send"] = dma((2,))
        scratch[k + "_recv"] = dma((2,))
    words = sum(math.prod(v) for v in shapes.values()) + 2 * l0 * l0 * 3 + N2[2] * N2[2] * 2
    vmem = pl.BlockSpec(memory_space=pltpu.VMEM)
    sol, res, norms = pl.pallas_call(
        functools.partial(whole_kernel, tuple(scratch), dims),
        out_shape=[jax.ShapeDtypeStruct(s, F32) for s in (dims, dims, (1, nz))],
        in_specs=[vmem] * 2,
        out_specs=[vmem] * 3,
        scratch_shapes=list(scratch.values()),
        compiler_params=pltpu.CompilerParams(
            collective_id=0, has_side_effects=True, vmem_limit_bytes=4 * words + 6 * 1024 * 1024
        ),
    )(data, weights)
    return sol, res, norms[0, :4]


def solution(mesh):
    in_specs = (P("gx", "gy", "gz"), P(None, "gz"))
    out_specs = (P("gx", "gy", "gz"), P("gx", "gy", "gz"), P())
    return jax.shard_map(body, mesh=mesh, in_specs=in_specs, out_specs=out_specs, check_vma=False)
```

```python
import functools
import math
import jax
import jax.numpy as jnp
from jax import lax
from jax.experimental import pallas as pl
from jax.experimental.pallas import tpu as pltpu
from jax.sharding import PartitionSpec as P

HALF = 4
RELAX = 0.45
F32 = jnp.float32
BF16 = jnp.bfloat16
HX = (4, 6)
OFFSETS = [j - HALF for j in range(HALF)] + [j - HALF + 1 for j in range(HALF, 2 * HALF)]


def iota(shape, dim):
    return lax.broadcasted_iota(jnp.int32, shape, dim)


def cyclic(index, size, own):
    cut = (size + own) // 2
    return jnp.where(index < cut, index, index - size)


def split(x):
    high = x.astype(BF16)
    return high, (x - high.astype(F32)).astype(BF16)


def dot(a, b):
    return lax.dot_general(a, b, (((1,), (0,)), ((), ())), preferred_element_type=F32)


def dot3(x, mh, ml):
    h, l = split(x)
    return dot(h, mh) + dot(h, ml) + dot(l, mh)


def dot2(x, m):
    h, l = split(x)
    return dot(h, m) + dot(l, m)


def dot2l(m, x):
    h, l = split(x)
    return dot(m, h) + dot(m, l)


def restrict_matrix(fine, coarse, axis):
    k = fine - 2 * coarse + 1
    m = jnp.where((k == 0) | (k == 3), 0.125, jnp.where((k == 1) | (k == 2), 0.375, 0.0))
    return m.astype(F32)


def prolong_matrix(fine, coarse, limit):
    centre = fine >> 1
    other = jnp.where((fine & 1) == 1, centre + 1, centre - 1)
    m = jnp.where(coarse == centre, 0.75, jnp.where(coarse == other, 0.25, 0.0))
    return jnp.where((fine >= 0) & (fine < limit), m, 0.0).astype(F32)


def build_level(level, nz, whole, wall, start, *outs):
    z0 = lax.axis_index("gz") * nz
    own = nz >> level
    total = whole >> level
    size = 2 * nz if level < 2 else total
    base = z0 >> level if level < 2 else 0

    def place(index):
        return cyclic(index, size, own) if level < 2 else index

    g = (iota((wall.shape[1], size), 0) + start) >> level
    p = place(iota((wall.shape[1], size), 1)) + base
    pick = jnp.where(g == p, 0.5**level, 0.0).astype(F32)
    w = lax.dot_general(
        wall, pick, (((1,), (0,)), ((), ())),
        preferred_element_type=F32, precision=lax.Precision.HIGHEST,
    )
    pr = place(iota((size, size), 0))
    pc = place(iota((size, size), 1))
    ok = (pr + base >= 0) & (pr + base < total) & (pc + base >= 0) & (pc + base < total)
    diff = pr - pc
    at = jnp.where(diff == 0, 1.0, 0.0).astype(F32)
    for j, offset in enumerate(OFFSETS):
        at = at + jnp.where(diff == offset, w[j : j + 1, :], 0.0)
    at = jnp.where(ok, at, 0.0)
    a = at.T
    stiff = 0.25**level
    m = lax.dot_general(
        at, a, (((1,), (0,)), ((), ())),
        preferred_element_type=F32, precision=lax.Precision.HIGHEST,
    )
    lap = jnp.where(diff == 0, 6.0, jnp.where((diff == 1) | (diff == -1), -1.0, 0.0))
    m = m + jnp.where(ok, stiff * lap, 0.0)
    d = jnp.sum(jnp.where(diff == 0, m, 0.0), axis=0, keepdims=True)
    col = place(iota((1, size), 1)) + base
    inside = (col >= 0) & (col < total)
    safe = jnp.where(inside, d, 1.0)
    c = jnp.where(inside, RELAX / safe, 0.0)
    inv = jnp.where(inside, safe * (1.0 / RELAX), 0.0)
    mh, ml = split(m * c)
    o = outs
    o[0][...] = mh
    o[1][...] = ml
    o[2][0:1, :] = c
    o[2][1:2, :] = inv
    if level == 0:
        ah, al = split(a)
        o[3][...] = ah
        o[4][...] = al


def chunk_of(count, rows, most):
    best = 1
    for planes in range(1, count + 1):
        if count % planes == 0 and planes * rows <= most:
            best = planes
    return best


def sweep(src, r_at, emit, first, count, stiff, mats, xmask, ymask, init=None, own=None, most=800):
    mh, ml, cv = mats
    rows, size = src.shape[1], src.shape[2]
    planes = chunk_of(count, rows, most)
    keep, lo, hi = own or (rows, 0, size)
    c = cv[0:1, lo:hi]
    inv = cv[1:2, lo:hi]
    yi = iota((rows, hi - lo), 0)
    cm = c if ymask is None else c * ymask[0:keep, lo:hi]

    def step(k, carry):
        x0 = first + k * planes
        u = src[pl.ds(x0, planes), 0:keep, :]
        um = dot3(u.reshape(planes * keep, size), mh[:, lo:hi], ml[:, lo:hi])
        for p in range(planes):
            x = x0 + p
            uc = src[x, :, lo:hi]
            low = pltpu.roll(uc, 1, 0)
            high = pltpu.roll(uc, rows - 1, 0)
            if ymask is None:
                low = jnp.where(yi == 0, 0.0, low)
                high = jnp.where(yi == rows - 1, 0.0, high)
            side = src[x - 1, 0:keep, lo:hi] + src[x + 1, 0:keep, lo:hi]
            nb = side + (low + high)[0:keep]
            if stiff != 1.0:
                nb = nb * stiff
            cx = cm if ymask is None else cm * xmask(x)
            delta = cx * (r_at(x)[0:keep, lo:hi] + nb) - um[p * keep : (p + 1) * keep]
            carry = emit(x, uc[0:keep], delta, inv, carry)
        return carry

    return lax.fori_loop(0, count // planes, step, init)


def restrict(gz, first, count, ry, rz, out):
    group = chunk_of(count, 1, 8)
    rows = ry.shape[0]

    def step(k, carry):
        values = []
        for j in range(group):
            x = first + 2 * (k * group + j)
            t = (gz[x - 1] + gz[x + 2] + 3.0 * (gz[x] + gz[x + 1])) * 0.125
            values.append(dot2l(ry, t))
        z = dot2(jnp.concatenate(values, axis=0), rz)
        for j in range(group):
            out(k * group + j, z[j * rows : (j + 1) * rows])
        return carry

    lax.fori_loop(0, count // group, step, 0)


def inside_mask(base, limit, pad):
    def mask(x):
        g = base + x - pad
        return jnp.where((g >= 0) & (g < limit), 1.0, 0.0).astype(F32)

    return mask


def y_mask(rows, size, own, base, limit):
    y = cyclic(iota((rows, size), 0), rows, own) + base
    return jnp.where((y >= 0) & (y < limit), 1.0, 0.0).astype(F32)


def zero_planes(ref, *planes):
    for x in planes:
        ref[x] = jnp.zeros(ref.shape[1:], F32)


def geometry(level, dims):
    nx, ny, nz = (v >> level for v in dims)
    gx, gy = lax.axis_size("gx"), lax.axis_size("gy")
    return dict(
        nx=nx, ny=ny, nz=nz, x0=lax.axis_index("gx") * nx, y0=lax.axis_index("gy") * ny,
        z0=lax.axis_index("gz") * nz, NX=nx * gx, NY=ny * gy, NZ=nz * lax.axis_size("gz"),
    )


def down_kernel(level, dims, *refs):
    if level == 0:
        ext, ah, al, mh, ml, cv, rhs, eb, r_next, part, ua, gz = refs
    else:
        rhs, mh, ml, cv, eb, r_next, part, ua, gz = refs
    geo = geometry(level, dims)
    nx, ny, nz = geo["nx"], geo["ny"], geo["nz"]
    hx = HX[level]
    count = nx + 2 * hx
    rows, size = ua.shape[1], ua.shape[2]
    pad = hx + 1
    c = cv[0:1, :]
    zero_planes(ua, 0, count + 1)
    reach = hx - 1 - level
    zero_planes(eb, *range(pad - reach), *range(pad + nx + reach, count + 2))
    if level == 0:
        planes = chunk_of(count, rows, 800)

        def first(k, carry):
            x0 = k * planes
            r = dot3(ext[pl.ds(x0, planes)].reshape(planes * rows, size), ah[...], al[...])
            for p in range(planes):
                rp = r[p * rows : (p + 1) * rows]
                rhs[x0 + p] = rp
                ua[x0 + p + 1] = c * rp
            return carry

        lax.fori_loop(0, count // planes, first, 0)
    else:

        def first(x, carry):
            ua[x + 1] = c * rhs[x]
            return carry

        lax.fori_loop(0, count, first, 0)
    xmask = inside_mask(geo["x0"], geo["NX"], pad)
    ymask = y_mask(rows, size, ny, geo["y0"], geo["NY"])
    mats = (mh, ml, cv)
    stiff = 0.25**level

    def r_at(x):
        return rhs[x - 1]

    def keep(x, u, delta, inv, carry):
        eb[x] = u + delta
        return carry

    sweep(ua, r_at, keep, pad - reach, nx + 2 * reach, stiff, mats, xmask, ymask, 0)
    lanes = dims[2]
    fine = cyclic(iota((size, lanes), 0), size, nz)
    coarse = iota((size, lanes), 1)
    rz = jnp.where(coarse < nz // 2, restrict_matrix(fine, coarse, 0), 0.0).astype(BF16)
    ry = restrict_matrix(
        cyclic(iota((ny // 2, rows), 1), rows, ny), iota((ny // 2, rows), 0), 1
    ).astype(BF16)

    def defect(x, u, delta, inv, carry):
        g = delta * inv
        gz[x] = g
        mine = g[0:ny, 0:nz]
        return carry + mine * mine * jnp.where((x >= pad) & (x < pad + nx), 1.0, 0.0).astype(F32)

    total = sweep(
        eb, r_at, defect, pad - 1, nx + 2, stiff, mats, xmask, ymask, jnp.zeros((ny, nz), F32)
    )
    part[...] = jnp.full(part.shape, jnp.sum(total), F32)

    def put(i, value):
        r_next[i] = value

    restrict(gz, pad, nx // 2, ry, rz, put)


def late_kernel(dims, ext, ah, al, mh, ml, cv, rhs, eb, ua):
    geo = geometry(0, dims)
    nx, ny, nz = geo["nx"], geo["ny"], geo["nz"]
    hx = HX[0]
    count, pad, reach = nx + 2 * hx, hx + 1, hx - 1
    rows, size = ua.shape[1], ua.shape[2]
    c = cv[0:1, nz:size]
    planes = chunk_of(count, rows, 800)

    def first(k, carry):
        x0 = k * planes
        r = dot3(ext[pl.ds(x0, planes)].reshape(planes * rows, size), ah[:, nz:size], al[:, nz:size])
        for p in range(planes):
            rp = r[p * rows : (p + 1) * rows]
            rhs[x0 + p, :, nz:size] = rp
            ua[x0 + p + 1, :, nz:size] = c * rp
        return carry

    lax.fori_loop(0, count // planes, first, 0)
    xmask = inside_mask(geo["x0"], geo["NX"], pad)
    ymask = y_mask(rows, size, ny, geo["y0"], geo["NY"])

    def keep(x, u, delta, inv, carry):
        eb[x, :, nz:size] = u + delta
        return carry

    sweep(
        ua, lambda x: rhs[x - 1], keep, pad - reach, nx + 2 * reach, 1.0, (mh, ml, cv), xmask, ymask,
        0, (rows, nz, size),
    )


def prolong_into(coarse_ref, coarse_first, coarse_count, pz, py, buf, error, dst, xmask):
    group = chunk_of(coarse_count, 1, 11)
    rows, size = coarse_ref.shape[1:]

    def step(k, carry):
        z = coarse_ref[pl.ds(coarse_first + k * group, group)]
        z = dot2(z.reshape(group * rows, size), pz)
        values = [dot2l(py, z[j * rows : (j + 1) * rows]) for j in range(group)]
        for j in range(group):
            buf[k * group + j] = values[j]
        return carry

    lax.fori_loop(0, coarse_count // group, step, 0)

    def join(i, carry):
        x = 1 + 2 * (i - 1)
        mid = 0.75 * buf[i]
        dst[x] = error(x) + xmask(x) * (mid + 0.25 * buf[i - 1])
        dst[x + 1] = error(x + 1) + xmask(x + 1) * (mid + 0.25 * buf[i + 1])
        return carry

    lax.fori_loop(1, coarse_count - 1, join, 0)


def coarse_kernel(dims, r2, m2h, m2l, c2, m3h, m3l, c3, u2, part, ua, ub, gz, r3, e3a, e3b, buf):
    g2 = geometry(2, dims)
    g3 = geometry(3, dims)
    N2, N3 = g2["NX"], g3["NX"]
    pad = 4
    one = lambda x: 1.0
    for ref in (ua, ub):
        zero_planes(ref, 0, N2 + 1)
    zero_planes(e3a, 0, N3 + 1)
    zero_planes(e3b, 0, N3 + 1)
    zero_planes(gz, 0, N2 + 1)
    zero_planes(u2, *range(pad), *range(N2 + pad, N2 + 2 * pad))
    mats2, mats3 = (m2h, m2l, c2), (m3h, m3l, c3)
    cc = c2[0:1, :]

    def first(x, carry):
        ua[x + 1] = cc * r2[x]
        return carry

    lax.fori_loop(0, N2, first, 0)
    r_at = lambda x: r2[x - 1]

    def into(ref, shift=0):
        def emit(x, u, delta, inv, carry):
            ref[x + shift] = u + delta
            return carry

        return emit

    s2, s3 = 0.25**2, 0.25**3
    sweep(ua, r_at, into(ub), 1, N2, s2, mats2, one, None, 0)
    NY2, NZ2, NY3, NZ3 = g2["NY"], g2["NZ"], g3["NY"], g3["NZ"]
    rz = restrict_matrix(iota((NZ2, NZ3), 0), iota((NZ2, NZ3), 1), 0).astype(BF16)
    ry = restrict_matrix(iota((NY3, NY2), 1), iota((NY3, NY2), 0), 1).astype(BF16)

    def defect(x, u, delta, inv, carry):
        g = delta * inv
        gz[x] = g
        return carry + g * g

    total = sweep(ub, r_at, defect, 1, N2, s2, mats2, one, None, jnp.zeros((NY2, NZ2), F32))
    part[...] = jnp.full(part.shape, jnp.sum(total), F32)
    c3v = c3[0:1, :]

    def put(i, value):
        r3[i] = value
        e3a[i + 1] = c3v * value

    restrict(gz, 1, N3, ry, rz, put)
    sweep(e3a, lambda x: r3[x - 1], into(e3b), 1, N3, s3, mats3, one, None, 0)
    pz = prolong_matrix(iota((NZ3, NZ2), 1), iota((NZ3, NZ2), 0), NZ2).astype(BF16)
    py = prolong_matrix(iota((NY2, NY3), 0), iota((NY2, NY3), 1), NY2).astype(BF16)
    prolong_into(e3b, 0, N3 + 2, pz, py, buf, lambda x: ub[x], ua, one)
    sweep(ua, r_at, into(ub), 1, N2, s2, mats2, one, None, 0)
    sweep(ub, r_at, into(u2, pad - 1), 1, N2, s2, mats2, one, None, 0)


def up_kernel(dims, u2, r1, e1, m1h, m1l, c1, rhs, e0, m0h, m0l, c0, sol, res, part,
              va, vb, vbuf, ua, ub, ubuf):
    g0, g1, g2 = geometry(0, dims), geometry(1, dims), geometry(2, dims)
    rows, size = va.shape[1], va.shape[2]
    count = g1["nx"] + 2 * HX[1]
    zero_planes(va, 0, count + 1)
    zero_planes(vb, 0, count + 1)
    xmask = inside_mask(g1["x0"], g1["NX"], HX[1] + 1)
    ymask = y_mask(rows, size, g1["ny"], g1["y0"], g1["NY"])
    NY2, NZ2 = g2["NY"], g2["NZ"]
    pz = prolong_matrix(
        cyclic(iota((NZ2, size), 1), size, g1["nz"]) + g1["z0"], iota((NZ2, size), 0), g1["NZ"]
    ).astype(BF16)
    py = prolong_matrix(
        cyclic(iota((rows, NY2), 0), rows, g1["ny"]) + g1["y0"], iota((rows, NY2), 1), g1["NY"]
    ).astype(BF16)
    first = g2["x0"] + 4 - HX[1] // 2 - 1
    prolong_into(u2, first, count // 2 + 2, pz, py, vbuf, lambda x: e1[x], va, xmask)
    mats = (m1h, m1l, c1)

    def into(ref):
        def emit(x, u, delta, inv, carry):
            ref[x] = u + delta
            return carry

        return emit

    r1_at = lambda x: r1[x - 1]
    q, n1 = HX[1] + 1, g1["nx"]
    sweep(va, r1_at, into(vb), q - 3, n1 + 6, 0.25, mats, xmask, ymask, 0)
    sweep(vb, r1_at, into(va), q - 2, n1 + 4, 0.25, mats, xmask, ymask, 0)
    rows0, size0 = ua.shape[1], ua.shape[2]
    count0 = g0["nx"] + 2 * HX[0]
    nx, ny, nz = g0["nx"], g0["ny"], g0["nz"]
    pad = HX[0] + 1
    zero_planes(ua, 0, count0 + 1)
    zero_planes(ub, 0, count0 + 1)
    xmask0 = inside_mask(g0["x0"], g0["NX"], pad)
    ymask0 = y_mask(rows0, size0, ny, g0["y0"], g0["NY"])
    pz = prolong_matrix(
        cyclic(iota((size, size0), 1), size0, nz) + g0["z0"],
        cyclic(iota((size, size0), 0), size, g1["nz"]) + g1["z0"], g0["NZ"],
    ).astype(BF16)
    py = prolong_matrix(
        cyclic(iota((rows0, rows), 0), rows0, ny) + g0["y0"],
        cyclic(iota((rows0, rows), 1), rows, g1["ny"]) + g1["y0"], g0["NY"],
    ).astype(BF16)
    first = HX[1] + 1 - HX[0] // 2 - 1
    prolong_into(va, first, count0 // 2 + 2, pz, py, ubuf, lambda x: e0[x], ua, xmask0)
    mats0 = (m0h, m0l, c0)
    r0_at = lambda x: rhs[x - 1]
    sweep(ua, r0_at, into(ub), pad - 2, nx + 4, 1.0, mats0, xmask0, ymask0, 0)
    sweep(ub, r0_at, into(ua), pad - 1, nx + 2, 1.0, mats0, xmask0, ymask0, 0)

    def final(x, u, delta, inv, carry):
        g = delta * inv
        sol[x - pad] = u
        res[x - pad] = g
        return carry + g * g

    total = sweep(
        ua, r0_at, final, pad, nx, 1.0, mats0, xmask0, ymask0, jnp.zeros((ny, nz), F32), (ny, 0, nz)
    )
    part[...] = jnp.full(part.shape, jnp.sum(total), F32)


AXES = ("gx", "gy", "gz")
MESH = pl.DeviceIdType.MESH
FIRST, WIDTH = 5 * HALF + 1, 10 * HALF


class Pair:
    def __init__(self, axis, up, down, sends, recvs, slot):
        n, me = lax.axis_size(axis), lax.axis_index(axis)
        self.has_low, self.has_high = me > 0, me < n - 1

        def copy(refs, k, target):
            return pltpu.make_async_remote_copy(
                src_ref=refs[0], dst_ref=refs[1], send_sem=sends.at[k], recv_sem=recvs.at[k],
                device_id={axis: target}, device_id_type=MESH,
            )

        self.up = copy(up, slot, lax.rem(me + 1, n))
        self.down = copy(down, slot + 1, lax.rem(me + n - 1, n))

    def start(self):
        pl.when(self.has_high)(self.up.start)
        pl.when(self.has_low)(self.down.start)

    def wait(self):
        pl.when(self.has_low)(self.up.wait_recv)
        pl.when(self.has_high)(self.down.wait_recv)

    def sent(self):
        pl.when(self.has_high)(self.up.wait_send)
        pl.when(self.has_low)(self.down.wait_send)

    def clear(self, low, high):
        @pl.when(jnp.logical_not(self.has_low))
        def _():
            low[...] = jnp.zeros(low.shape, F32)

        @pl.when(jnp.logical_not(self.has_high))
        def _():
            high[...] = jnp.zeros(high.shape, F32)


class Star:
    def __init__(self, moves, src, dst, sends, recvs):
        gx, gz = lax.axis_size("gx"), lax.axis_size("gz")
        mx, mz = lax.axis_index("gx"), lax.axis_index("gz")
        self.moves = []
        for k, (dx, dz) in enumerate(moves):
            to = (mx + dx >= 0) & (mx + dx < gx) & (mz + dz >= 0) & (mz + dz < gz)
            frm = (mx - dx >= 0) & (mx - dx < gx) & (mz - dz >= 0) & (mz - dz < gz)
            into = dst(-dx, -dz)
            copy = pltpu.make_async_remote_copy(
                src_ref=src(dx, dz), dst_ref=into, send_sem=sends.at[k], recv_sem=recvs.at[k],
                device_id={"gx": lax.rem(mx + dx + gx, gx), "gz": lax.rem(mz + dz + gz, gz)},
                device_id_type=MESH,
            )
            self.moves.append((to, frm, copy, into))

    def clear(self):
        for _, frm, _, into in self.moves:

            @pl.when(jnp.logical_not(frm))
            def _(into=into):
                into[...] = jnp.zeros(into.shape, F32)

    def start(self):
        for to, _, copy, _ in self.moves:
            pl.when(to)(copy.start)

    def wait(self):
        for _, frm, copy, _ in self.moves:
            pl.when(frm)(copy.wait_recv)

    def sent(self):
        for to, _, copy, _ in self.moves:
            pl.when(to)(copy.wait_send)


SKEW = [(dx, dz) for dx in (-1, 1) for dz in (-1, 1)]
STAR = SKEW + [(0, -1), (0, 1), (-1, 0), (1, 0)]


def star_name(prefix, d):
    return prefix + "mop"[d[0] + 1] + "mop"[d[1] + 1]


def linear():
    gy, gz = lax.axis_size("gy"), lax.axis_size("gz")
    return (lax.axis_index("gx") * gy + lax.axis_index("gy")) * gz + lax.axis_index("gz")


def coordinates(t):
    gy, gz = lax.axis_size("gy"), lax.axis_size("gz")
    return (t // (gy * gz), lax.rem(t // gz, gy), lax.rem(t, gz))


def device_count():
    return lax.axis_size("gx") * lax.axis_size("gy") * lax.axis_size("gz")


def near_devices():
    sizes, me = [lax.axis_size(a) for a in AXES], [lax.axis_index(a) for a in AXES]
    out = []
    for move in [(dx, 0, dz) for dx, dz in STAR] + [(0, -1, 0), (0, 1, 0)]:
        if all(n > 1 or d == 0 for n, d in zip(sizes, move)):
            at = [i + d for i, d in zip(me, move)]
            there = functools.reduce(jnp.logical_and, [(i >= 0) & (i < n) for i, n in zip(at, sizes)])
            out.append((there, tuple(lax.rem(i + n, n) for i, n in zip(at, sizes))))
    return out


def reached():
    return lax.axis_size("gx") <= 4 and lax.axis_size("gy") <= 2 and lax.axis_size("gz") <= 4


def signal_all():
    n, me = device_count(), linear()
    barrier = pltpu.get_barrier_semaphore()
    if reached():
        for there, device in near_devices():

            @pl.when(there)
            def _():
                pl.semaphore_signal(barrier, inc=1, device_id=device, device_id_type=MESH)

        return

    def step(k, carry):
        pl.semaphore_signal(
            barrier, inc=1, device_id=coordinates(lax.rem(me + k, n)), device_id_type=MESH
        )
        return carry

    lax.fori_loop(1, n, step, 0)


def wait_all():
    if reached():
        count = sum(there.astype(jnp.int32) for there, _ in near_devices())
        pl.semaphore_wait(pltpu.get_barrier_semaphore(), count)
        return
    pl.semaphore_wait(pltpu.get_barrier_semaphore(), device_count() - 1)


def shifted(axis, d):
    n = lax.axis_size(axis)
    t = lax.axis_index(axis) + d
    return jnp.where(t >= n, t - n, t)


def arrived(buf, count, sends, recvs, k, axis):
    part = buf.at[0:count]
    return pltpu.make_async_remote_copy(
        src_ref=part, dst_ref=part, send_sem=sends.at[k], recv_sem=recvs.at[k],
        device_id={axis: shifted(axis, 1)}, device_id_type=MESH,
    )


def spread(block, buf, slot, sends, recvs, k, sizes):
    for dx in range(sizes[0]):
        for dy in range(sizes[1]):
            for dz in range(sizes[2]):
                if dx or dy or dz:
                    pltpu.make_async_remote_copy(
                        src_ref=block, dst_ref=buf.at[slot], send_sem=sends.at[k], recv_sem=recvs.at[k],
                        device_id=(shifted("gx", dx), shifted("gy", dy), shifted("gz", dz)),
                        device_id_type=MESH,
                    ).start()


def everyone(block, buf, sends, recvs):
    n, me = device_count(), linear()
    spread(block, buf, me, sends, recvs, 0, [lax.axis_size(a) for a in AXES])
    buf[me] = block[...]
    done = arrived(buf, n - 1, sends, recvs, 0, "gz")
    done.wait_recv()
    return done


def by_columns(block, buf, sends, recvs):
    gx, gy, gz = (lax.axis_size(a) for a in AXES)
    m, y = gx * gz, lax.axis_index("gy")
    slot = y * m + lax.axis_index("gx") * gz + lax.axis_index("gz")
    spread(block, buf, slot, sends, recvs, 0, (gx, 1, gz))
    buf[slot] = block[...]
    first = arrived(buf, m - 1, sends, recvs, 0, "gz")
    mine = buf.at[pl.ds(y * m, m)]
    second = arrived(buf, (gy - 1) * m, sends, recvs, 1, "gy")

    def finish():
        first.wait_recv()
        for d in range(1, gy):
            pltpu.make_async_remote_copy(
                src_ref=mine, dst_ref=mine, send_sem=sends.at[1], recv_sem=recvs.at[1],
                device_id={"gy": shifted("gy", d)}, device_id_type=MESH,
            ).start()
        second.wait_recv()
        return first, second

    return finish


def pack_faces(data, low, high, start, stop):
    nx, ny, nz = data.shape
    width = stop - start
    slots = nz // width
    rest = jnp.zeros((ny, nz - slots * width), F32)
    for i in range(low.shape[0]):
        planes = [min(i * slots + k, nx - 1) for k in range(slots)]
        low[i] = jnp.concatenate([data[x][:, start:stop] for x in planes] + [rest], axis=1)
        high[i] = jnp.concatenate([data[x][:, nz - stop : nz - start] for x in planes] + [rest], axis=1)


def face_pieces(nx, hx, nz, width):
    slots = nz // width
    return {
        -1: slice(0, -(-hx // slots)),
        0: slice(0, -(-nx // slots)),
        1: slice((nx - hx) // slots, -(-nx // slots)),
    }


def unpack_faces(dims, parts, widths, ext, hx):
    nx, ny, nz = dims
    for dx in (-1, 0, 1):
        source = nx - hx if dx < 0 else 0
        target = {-1: 0, 0: hx, 1: hx + nx}[dx]
        for i in range(nx if dx == 0 else hx):
            ends = {}
            for dz in (-1, 1):
                ends[dz] = []
                for part, width in zip(parts, widths):
                    slots = nz // width
                    first = (nx - hx) // slots if dx < 0 else 0
                    x = source + i
                    lane = x % slots * width
                    ends[dz].append(part(dx, dz)[x // slots - first][:, lane : lane + width])
            gap = jnp.zeros((ny, nz - 2 * sum(widths)), F32)
            ext[target + i, 0:ny, nz:] = jnp.concatenate(ends[1] + [gap] + ends[-1][::-1], axis=1)


def whole_kernel(names, dims, data, weights, sol, res, norms, *scratch):
    r = dict(zip(names, scratch))
    nx, ny, nz = dims
    n, gz = device_count(), lax.axis_size("gz")
    ns, nr = r["near_send"], r["near_recv"]
    signal_all()
    pack_faces(data, r["f1_low"], r["f1_high"], 0, FIRST)
    ext, hx, weights_row = r["ext"], HX[0], iota((8, 2 * nz), 0)
    for x in range(nx):
        ext[hx + x, 0:ny, 0:nz] = data[x]
    wait_all()
    near = Pair("gz", (weights, r["w_low"]), (weights, r["w_high"]), ns, nr, 0)
    near.start()
    widths = (FIRST, WIDTH - FIRST)
    pieces = [face_pieces(nx, hx, nz, w) for w in widths]

    def faces(part):
        def send(dx, dz):
            return r["f%d_%s" % (part, "low" if dz < 0 else "high")].at[pieces[part - 1][dx]]

        def take(dx, dz):
            return r[star_name("g%d_" % part, (dx, dz))]

        return send, take

    send1, take1 = faces(1)
    send2, take2 = faces(2)

    def plane_send(dx, dz):
        if dz:
            return send1(dx, dz)
        return data.at[0:hx] if dx < 0 else data.at[nx - hx : nx]

    def plane_take(dx, dz):
        if dz:
            return take1(dx, dz)
        return ext.at[0:hx, 0:ny, 0:nz] if dx < 0 else ext.at[nx + hx : nx + 2 * hx, 0:ny, 0:nz]

    star = Star(STAR, plane_send, plane_take, r["s_send"], r["s_recv"])
    star.start()
    star.clear()
    near.clear(r["w_low"], r["w_high"])
    late = Star(STAR[:6], send2, take2, r["l_send"], r["l_recv"])
    late.clear()
    pack_faces(data, r["f2_low"], r["f2_high"], FIRST, WIDTH)
    level = [[r["m%d%s" % (k, t)] for t in "hlc"] for k in range(4)]
    near.wait()
    nearby = jnp.concatenate([r["w_low"][...], weights[...], r["w_high"][...]], axis=1)
    start = (lax.axis_index("gz") - 1) * nz
    build_level(0, nz, nz * gz, nearby, start, *level[0], r["ah"], r["al"])
    star.wait()
    late.start()
    unpack_faces(dims, (take1,), widths[:1], ext, hx)
    ys = Pair("gy", (ext.at[:, ny - 8 : ny, :], r["y_low"]), (ext.at[:, 0:8, :], r["y_high"]), ns, nr, 2)
    ys.clear(r["y_low"], r["y_high"])
    ys.start()
    ys.wait()
    star.sent()
    near.sent()
    ys.sent()
    upper = weights_row < 4

    def join(x, carry):
        ext[x, ny : ny + 8, :] = jnp.where(upper, r["y_high"][x], r["y_low"][x])
        return carry

    lax.fori_loop(0, nx + 2 * hx, join, 0)
    down_kernel(0, dims, ext, r["ah"], r["al"], *level[0], r["rhs"], r["e0"], r["r1"], r["p0"], r["ua"], r["gz0"])
    n1, m1, k1 = nx // 2, ny // 2, nz // 2
    h1 = HX[1]
    x1, r1, own = r["x1"], r["r1"], r["b_own"]
    for a in range(n1 // 2):
        own[a] = jnp.concatenate([r1[2 * a][:, :k1], r1[2 * a + 1][:, :k1]], axis=1)
    bufs = {d: r[star_name("b_", d)] for d in STAR}
    rim = h1 // 2
    cut = {-1: slice(0, rim), 0: slice(0, n1 // 2), 1: slice(n1 // 2 - rim, n1 // 2)}
    star = Star(
        STAR, lambda dx, dz: own.at[cut[dx]], lambda dx, dz: bufs[(dx, dz)], r["b_send"], r["b_recv"]
    )
    star.start()
    star.clear()
    build_level(1, nz, nz * gz, nearby, start, *level[1])
    late.wait()
    unpack_faces(dims, (take1, take2), widths, ext, hx)
    far = slice(nz, 2 * nz)
    late_ys = Pair(
        "gy", (ext.at[:, ny - 8 : ny, far], r["z_low"]), (ext.at[:, 0:8, far], r["z_high"]), ns, nr, 4
    )
    late_ys.clear(r["z_low"], r["z_high"])
    late_ys.start()
    star.wait()
    spread(weights, r["wparts"], lax.axis_index("gz"), r["w_send"], r["w_recv"], 0, (1, 1, gz))
    bufs[(0, 0)] = own
    blank = jnp.zeros((m1, k1), F32)
    for dx in (-1, 0, 1):
        base = h1 + dx * h1 if dx < 1 else h1 + n1
        for x in range(n1 if dx == 0 else h1):
            a, part = x // 2, slice((x % 2) * k1, (x % 2 + 1) * k1)
            low, mid, high = (bufs[(dx, dz)][a][:, part] for dz in (-1, 0, 1))
            x1[base + x, 0:m1, :] = jnp.concatenate([mid, high, blank, low], axis=1)
    ys = Pair(
        "gy",
        (x1.at[:, m1 - 8 : m1, :], x1.at[:, m1 + 8 : m1 + 16, :]),
        (x1.at[:, 0:8, :], x1.at[:, m1 : m1 + 8, :]),
        ns, nr, 8,
    )
    ys.clear(x1.at[:, m1 + 8 : m1 + 16, :], x1.at[:, m1 : m1 + 8, :])
    ys.start()
    ys.wait()
    star.sent()
    ys.sent()
    down_kernel(1, dims, x1, *level[1], r["e1"], r["r2"], r["p1"], r["va"], r["gz1"])
    n2, m2, k2 = nx // 4, ny // 4, nz // 4
    slots = nz // k2
    per = n2 // slots
    for a in range(per):
        r["c_own"][a] = jnp.concatenate([r["r2"][q * per + a][:, :k2] for q in range(slots)], axis=1)
    finish = by_columns(r["c_own"], r["c_all"], r["c_send"], r["c_recv"])
    late_ys.wait()

    def late_join(x, carry):
        ext[x, ny : ny + 8, far] = jnp.where(upper[:, far], r["z_high"][x], r["z_low"][x])
        return carry

    lax.fori_loop(0, nx + 2 * hx, late_join, 0)
    late_kernel(dims, ext, r["ah"], r["al"], *level[0], r["rhs"], r["e0"], r["ua"])
    r["wparts"][lax.axis_index("gz")] = weights[...]
    given = arrived(r["wparts"], gz - 1, r["w_send"], r["w_recv"], 0, "gz")
    given.wait_recv()
    wall = jnp.concatenate([r["wparts"][i] for i in range(gz)], axis=1)
    build_level(2, nz, nz * gz, wall, 0, *level[2])
    build_level(3, nz, nz * gz, wall, 0, *level[3])
    gathered = finish()
    gx, gy = lax.axis_size("gx"), lax.axis_size("gy")

    def place(i, carry):
        for j in range(gy):
            for x in range(n2):
                q, a = x // per, x % per
                r["r2all"][i * n2 + x, j * m2 : (j + 1) * m2, :] = jnp.concatenate(
                    [r["c_all"][(j * gx + i) * gz + k, a][:, q * k2 : (q + 1) * k2] for k in range(gz)],
                    axis=1,
                )
        return carry

    lax.fori_loop(0, lax.axis_size("gx"), place, 0)
    coarse_kernel(
        dims, r["r2all"], *level[2], *level[3], r["u2"], r["p2"],
        r["ca"], r["cb"], r["cz"], r["r3"], r["e3a"], r["e3b"], r["cbuf"],
    )
    up_kernel(
        dims, r["u2"], x1, r["e1"], *level[1], r["rhs"], r["e0"], *level[0], sol, res, r["p3"],
        r["va"], r["vb"], r["vbuf"], r["ua"], r["ub"], r["ubuf"],
    )
    for g in gathered + (given,):
        g.wait_send()
    late.sent()
    late_ys.sent()
    lane = iota((1, nz), 1)
    p0, p1, p2, p3 = (r["p%d" % k][0:1, :] for k in range(4))
    mine = jnp.where(lane == 0, p0, jnp.where(lane == 1, p1, p3))
    r["n_own"][...] = mine
    last = everyone(r["n_own"], r["n_all"], r["n_send"], r["n_recv"])
    total = jnp.sum(r["n_all"][...], axis=0)
    cells = float(nx * ny * nz * n)
    total = jnp.where(lane == 2, p2, total)
    scale = jnp.where(lane == 1, 8.0 / cells, jnp.where(lane == 2, 64.0 / cells, 1.0 / cells))
    norms[...] = jnp.sqrt(total * scale)
    last.wait_send()


def body(data, weights):
    dims = data.shape
    nx, ny, nz = dims
    gx, gy, gz = (lax.axis_size(a) for a in AXES)
    n = gx * gy * gz
    c0, y0, l0 = nx + 2 * HX[0], ny + 8, 2 * nz
    c1, y1 = nx // 2 + 2 * HX[1], ny // 2 + 16
    N2 = (nx // 4 * gx, ny // 4 * gy, nz // 4 * gz)
    N3 = tuple(v // 2 for v in N2)
    pad2 = (N2[0] + 2,) + N2[1:]
    pad3 = (N3[0] + 2,) + N3[1:]
    own2 = (nx // 4 // 4, ny // 4, nz)
    shapes = dict(
        ext=(c0, y0, l0), wparts=(gz, 8, nz), w_low=(8, nz), w_high=(8, nz), z_low=(c0, 8, nz), z_high=(c0, 8, nz), y_low=(c0, 8, l0), y_high=(c0, 8, l0),
        rhs=(c0, y0, l0), e0=(c0 + 2, y0, l0), r1=(nx // 2, ny // 2, nz),
        ua=(c0 + 2, y0, l0), ub=(c0 + 2, y0, l0), gz0=(c0 + 2, y0, l0), ubuf=(c0 // 2 + 2, y0, l0),
        b_own=(nx // 4, ny // 2, nz),
        x1=(c1, y1, l0), e1=(c1 + 2, y1, l0), r2=(nx // 4, ny // 4, nz),
        va=(c1 + 2, y1, l0), vb=(c1 + 2, y1, l0), gz1=(c1 + 2, y1, l0), vbuf=(c1 // 2 + 2, y1, l0),
        c_own=own2, c_all=(n,) + own2, r2all=N2, u2=(N2[0] + 8,) + N2[1:],
        ca=pad2, cb=pad2, cz=pad2, r3=N3, e3a=pad3, e3b=pad3,
        cbuf=(N3[0] + 2,) + N2[1:], n_own=(1, nz), n_all=(n, 1, nz),
        p0=(8, nz), p1=(8, nz), p2=(8, nz), p3=(8, nz),
    )
    for part, width in ((1, FIRST), (2, WIDTH - FIRST)):
        planes = {k: v.stop - v.start for k, v in face_pieces(nx, HX[0], nz, width).items()}
        for side in ("low", "high"):
            shapes["f%d_%s" % (part, side)] = (planes[0], ny, nz)
        for d in STAR[:6]:
            shapes[star_name("g%d_" % part, d)] = (planes[-d[0]], ny, nz)
    for d in STAR:
        shapes[star_name("b_", d)] = (HX[1] // 2 if d[0] else nx // 4, ny // 2, nz)
    scratch = {k: pltpu.VMEM(v, F32) for k, v in shapes.items()}
    for k, size in enumerate((l0, l0, N2[2], N3[2])):
        scratch["m%dh" % k] = pltpu.VMEM((size, size), BF16)
        scratch["m%dl" % k] = pltpu.VMEM((size, size), BF16)
        scratch["m%dc" % k] = pltpu.VMEM((8, size), F32)
    scratch["ah"] = scratch["al"] = pltpu.VMEM((l0, l0), BF16)
    dma = pltpu.SemaphoreType.DMA
    scratch.update(near_send=dma((10,)), near_recv=dma((10,)), w_send=dma((1,)), w_recv=dma((1,)))
    for k in "bsl":
        scratch[k + "_send"] = dma((8,))
        scratch[k + "_recv"] = dma((8,))
    for k in "cn":
        scratch[k + "_send"] = dma((2,))
        scratch[k + "_recv"] = dma((2,))
    words = sum(math.prod(v) for v in shapes.values()) + 2 * l0 * l0 * 3 + N2[2] * N2[2] * 2
    vmem = pl.BlockSpec(memory_space=pltpu.VMEM)
    sol, res, norms = pl.pallas_call(
        functools.partial(whole_kernel, tuple(scratch), dims),
        out_shape=[jax.ShapeDtypeStruct(s, F32) for s in (dims, dims, (1, nz))],
        in_specs=[vmem] * 2,
        out_specs=[vmem] * 3,
        scratch_shapes=list(scratch.values()),
        compiler_params=pltpu.CompilerParams(
            collective_id=0, has_side_effects=True, vmem_limit_bytes=4 * words + 6 * 1024 * 1024
        ),
    )(data, weights)
    return sol, res, norms[0, :4]


def solution(mesh):
    in_specs = (P("gx", "gy", "gz"), P(None, "gz"))
    out_specs = (P("gx", "gy", "gz"), P("gx", "gy", "gz"), P())
    return jax.shard_map(body, mesh=mesh, in_specs=in_specs, out_specs=out_specs, check_vma=False)
```

```python
import functools
import math
import jax
import jax.numpy as jnp
from jax import lax
from jax.experimental import pallas as pl
from jax.experimental.pallas import tpu as pltpu
from jax.sharding import PartitionSpec as P

HALF = 4
RELAX = 0.45
F32 = jnp.float32
BF16 = jnp.bfloat16
HX = (4, 6)
OFFSETS = [j - HALF for j in range(HALF)] + [j - HALF + 1 for j in range(HALF, 2 * HALF)]


def iota(shape, dim):
    return lax.broadcasted_iota(jnp.int32, shape, dim)


def cyclic(index, size, own):
    cut = (size + own) // 2
    return jnp.where(index < cut, index, index - size)


def split(x):
    high = x.astype(BF16)
    return high, (x - high.astype(F32)).astype(BF16)


def dot(a, b):
    return lax.dot_general(a, b, (((1,), (0,)), ((), ())), preferred_element_type=F32)


def dot3(x, mh, ml):
    h, l = split(x)
    return dot(h, mh) + dot(h, ml) + dot(l, mh)


def dot2(x, m):
    h, l = split(x)
    return dot(h, m) + dot(l, m)


def dot2l(m, x):
    h, l = split(x)
    return dot(m, h) + dot(m, l)


def restrict_matrix(fine, coarse, axis):
    k = fine - 2 * coarse + 1
    m = jnp.where((k == 0) | (k == 3), 0.125, jnp.where((k == 1) | (k == 2), 0.375, 0.0))
    return m.astype(F32)


def prolong_matrix(fine, coarse, limit):
    centre = fine >> 1
    other = jnp.where((fine & 1) == 1, centre + 1, centre - 1)
    m = jnp.where(coarse == centre, 0.75, jnp.where(coarse == other, 0.25, 0.0))
    return jnp.where((fine >= 0) & (fine < limit), m, 0.0).astype(F32)


def build_level(level, nz, whole, wall, start, *outs):
    z0 = lax.axis_index("gz") * nz
    own = nz >> level
    total = whole >> level
    size = 2 * nz if level < 2 else total
    base = z0 >> level if level < 2 else 0

    def place(index):
        return cyclic(index, size, own) if level < 2 else index

    g = (iota((wall.shape[1], size), 0) + start) >> level
    p = place(iota((wall.shape[1], size), 1)) + base
    pick = jnp.where(g == p, 0.5**level, 0.0).astype(F32)
    w = lax.dot_general(
        wall, pick, (((1,), (0,)), ((), ())),
        preferred_element_type=F32, precision=lax.Precision.HIGHEST,
    )
    pr = place(iota((size, size), 0))
    pc = place(iota((size, size), 1))
    ok = (pr + base >= 0) & (pr + base < total) & (pc + base >= 0) & (pc + base < total)
    diff = pr - pc
    at = jnp.where(diff == 0, 1.0, 0.0).astype(F32)
    for j, offset in enumerate(OFFSETS):
        at = at + jnp.where(diff == offset, w[j : j + 1, :], 0.0)
    at = jnp.where(ok, at, 0.0)
    a = at.T
    stiff = 0.25**level
    m = lax.dot_general(
        at, a, (((1,), (0,)), ((), ())),
        preferred_element_type=F32, precision=lax.Precision.HIGHEST,
    )
    lap = jnp.where(diff == 0, 6.0, jnp.where((diff == 1) | (diff == -1), -1.0, 0.0))
    m = m + jnp.where(ok, stiff * lap, 0.0)
    d = jnp.sum(jnp.where(diff == 0, m, 0.0), axis=0, keepdims=True)
    col = place(iota((1, size), 1)) + base
    inside = (col >= 0) & (col < total)
    safe = jnp.where(inside, d, 1.0)
    c = jnp.where(inside, RELAX / safe, 0.0)
    inv = jnp.where(inside, safe * (1.0 / RELAX), 0.0)
    mh, ml = split(m * c)
    o = outs
    o[0][...] = mh
    o[1][...] = ml
    o[2][0:1, :] = c
    o[2][1:2, :] = inv
    if level == 0:
        ah, al = split(a)
        o[3][...] = ah
        o[4][...] = al


def chunk_of(count, rows, most):
    best = 1
    for planes in range(1, count + 1):
        if count % planes == 0 and planes * rows <= most:
            best = planes
    return best


def sweep(src, r_at, emit, first, count, stiff, mats, xmask, ymask, init=None, own=None, most=800):
    mh, ml, cv = mats
    rows, size = src.shape[1], src.shape[2]
    planes = chunk_of(count, rows, most)
    keep, lo, hi = own or (rows, 0, size)
    c = cv[0:1, lo:hi]
    inv = cv[1:2, lo:hi]
    yi = iota((rows, hi - lo), 0)
    cm = c if ymask is None else c * ymask[0:keep, lo:hi]

    def step(k, carry):
        x0 = first + k * planes
        u = src[pl.ds(x0, planes), 0:keep, :]
        um = dot3(u.reshape(planes * keep, size), mh[:, lo:hi], ml[:, lo:hi])
        for p in range(planes):
            x = x0 + p
            uc = src[x, :, lo:hi]
            low = pltpu.roll(uc, 1, 0)
            high = pltpu.roll(uc, rows - 1, 0)
            if ymask is None:
                low = jnp.where(yi == 0, 0.0, low)
                high = jnp.where(yi == rows - 1, 0.0, high)
            side = src[x - 1, 0:keep, lo:hi] + src[x + 1, 0:keep, lo:hi]
            nb = side + (low + high)[0:keep]
            if stiff != 1.0:
                nb = nb * stiff
            cx = cm if ymask is None else cm * xmask(x)
            delta = cx * (r_at(x)[0:keep, lo:hi] + nb) - um[p * keep : (p + 1) * keep]
            carry = emit(x, uc[0:keep], delta, inv, carry)
        return carry

    return lax.fori_loop(0, count // planes, step, init)


def restrict(gz, first, count, ry, rz, out):
    group = chunk_of(count, 1, 8)
    rows = ry.shape[0]

    def step(k, carry):
        values = []
        for j in range(group):
            x = first + 2 * (k * group + j)
            t = (gz[x - 1] + gz[x + 2] + 3.0 * (gz[x] + gz[x + 1])) * 0.125
            values.append(dot2l(ry, t))
        z = dot2(jnp.concatenate(values, axis=0), rz)
        for j in range(group):
            out(k * group + j, z[j * rows : (j + 1) * rows])
        return carry

    lax.fori_loop(0, count // group, step, 0)


def inside_mask(base, limit, pad):
    def mask(x):
        g = base + x - pad
        return jnp.where((g >= 0) & (g < limit), 1.0, 0.0).astype(F32)

    return mask


def y_mask(rows, size, own, base, limit):
    y = cyclic(iota((rows, size), 0), rows, own) + base
    return jnp.where((y >= 0) & (y < limit), 1.0, 0.0).astype(F32)


def zero_planes(ref, *planes):
    for x in planes:
        ref[x] = jnp.zeros(ref.shape[1:], F32)


def geometry(level, dims):
    nx, ny, nz = (v >> level for v in dims)
    gx, gy = lax.axis_size("gx"), lax.axis_size("gy")
    return dict(
        nx=nx, ny=ny, nz=nz, x0=lax.axis_index("gx") * nx, y0=lax.axis_index("gy") * ny,
        z0=lax.axis_index("gz") * nz, NX=nx * gx, NY=ny * gy, NZ=nz * lax.axis_size("gz"),
    )


def down_kernel(level, dims, *refs):
    if level == 0:
        ext, ah, al, mh, ml, cv, rhs, eb, r_next, part, ua, gz = refs
    else:
        rhs, mh, ml, cv, eb, r_next, part, ua, gz = refs
    geo = geometry(level, dims)
    nx, ny, nz = geo["nx"], geo["ny"], geo["nz"]
    hx = HX[level]
    count = nx + 2 * hx
    rows, size = ua.shape[1], ua.shape[2]
    pad = hx + 1
    c = cv[0:1, :]
    zero_planes(ua, 0, count + 1)
    reach = hx - 1 - level
    zero_planes(eb, *range(pad - reach), *range(pad + nx + reach, count + 2))
    if level == 0:
        planes = chunk_of(count, rows, 800)

        def first(k, carry):
            x0 = k * planes
            r = dot3(ext[pl.ds(x0, planes)].reshape(planes * rows, size), ah[...], al[...])
            for p in range(planes):
                rp = r[p * rows : (p + 1) * rows]
                rhs[x0 + p] = rp
                ua[x0 + p + 1] = c * rp
            return carry

        lax.fori_loop(0, count // planes, first, 0)
    else:

        def first(x, carry):
            ua[x + 1] = c * rhs[x]
            return carry

        lax.fori_loop(0, count, first, 0)
    xmask = inside_mask(geo["x0"], geo["NX"], pad)
    ymask = y_mask(rows, size, ny, geo["y0"], geo["NY"])
    mats = (mh, ml, cv)
    stiff = 0.25**level

    def r_at(x):
        return rhs[x - 1]

    def keep(x, u, delta, inv, carry):
        eb[x] = u + delta
        return carry

    sweep(ua, r_at, keep, pad - reach, nx + 2 * reach, stiff, mats, xmask, ymask, 0)
    lanes = dims[2]
    fine = cyclic(iota((size, lanes), 0), size, nz)
    coarse = iota((size, lanes), 1)
    rz = jnp.where(coarse < nz // 2, restrict_matrix(fine, coarse, 0), 0.0).astype(BF16)
    ry = restrict_matrix(
        cyclic(iota((ny // 2, rows), 1), rows, ny), iota((ny // 2, rows), 0), 1
    ).astype(BF16)

    def defect(x, u, delta, inv, carry):
        g = delta * inv
        gz[x] = g
        mine = g[0:ny, 0:nz]
        return carry + mine * mine * jnp.where((x >= pad) & (x < pad + nx), 1.0, 0.0).astype(F32)

    total = sweep(
        eb, r_at, defect, pad - 1, nx + 2, stiff, mats, xmask, ymask, jnp.zeros((ny, nz), F32)
    )
    part[...] = jnp.full(part.shape, jnp.sum(total), F32)

    def put(i, value):
        r_next[i] = value

    restrict(gz, pad, nx // 2, ry, rz, put)


def late_kernel(dims, ext, ah, al, mh, ml, cv, rhs, eb, ua):
    geo = geometry(0, dims)
    nx, ny, nz = geo["nx"], geo["ny"], geo["nz"]
    hx = HX[0]
    count, pad, reach = nx + 2 * hx, hx + 1, hx - 1
    rows, size = ua.shape[1], ua.shape[2]
    c = cv[0:1, nz:size]
    planes = chunk_of(count, rows, 800)

    def first(k, carry):
        x0 = k * planes
        r = dot3(ext[pl.ds(x0, planes)].reshape(planes * rows, size), ah[:, nz:size], al[:, nz:size])
        for p in range(planes):
            rp = r[p * rows : (p + 1) * rows]
            rhs[x0 + p, :, nz:size] = rp
            ua[x0 + p + 1, :, nz:size] = c * rp
        return carry

    lax.fori_loop(0, count // planes, first, 0)
    xmask = inside_mask(geo["x0"], geo["NX"], pad)
    ymask = y_mask(rows, size, ny, geo["y0"], geo["NY"])

    def keep(x, u, delta, inv, carry):
        eb[x, :, nz:size] = u + delta
        return carry

    sweep(
        ua, lambda x: rhs[x - 1], keep, pad - reach, nx + 2 * reach, 1.0, (mh, ml, cv), xmask, ymask,
        0, (rows, nz, size),
    )


def prolong_into(coarse_ref, coarse_first, coarse_count, pz, py, buf, error, dst, xmask):
    group = chunk_of(coarse_count, 1, 11)
    rows, size = coarse_ref.shape[1:]

    def step(k, carry):
        z = coarse_ref[pl.ds(coarse_first + k * group, group)]
        z = dot2(z.reshape(group * rows, size), pz)
        values = [dot2l(py, z[j * rows : (j + 1) * rows]) for j in range(group)]
        for j in range(group):
            buf[k * group + j] = values[j]
        return carry

    lax.fori_loop(0, coarse_count // group, step, 0)

    def join(i, carry):
        x = 1 + 2 * (i - 1)
        mid = 0.75 * buf[i]
        dst[x] = error(x) + xmask(x) * (mid + 0.25 * buf[i - 1])
        dst[x + 1] = error(x + 1) + xmask(x + 1) * (mid + 0.25 * buf[i + 1])
        return carry

    lax.fori_loop(1, coarse_count - 1, join, 0)


def coarse_kernel(dims, r2, m2h, m2l, c2, m3h, m3l, c3, u2, part, ua, ub, gz, r3, e3a, e3b, buf):
    g2 = geometry(2, dims)
    g3 = geometry(3, dims)
    N2, N3 = g2["NX"], g3["NX"]
    pad = 4
    one = lambda x: 1.0
    for ref in (ua, ub):
        zero_planes(ref, 0, N2 + 1)
    zero_planes(e3a, 0, N3 + 1)
    zero_planes(e3b, 0, N3 + 1)
    zero_planes(gz, 0, N2 + 1)
    zero_planes(u2, *range(pad), *range(N2 + pad, N2 + 2 * pad))
    mats2, mats3 = (m2h, m2l, c2), (m3h, m3l, c3)
    cc = c2[0:1, :]

    def first(x, carry):
        ua[x + 1] = cc * r2[x]
        return carry

    lax.fori_loop(0, N2, first, 0)
    r_at = lambda x: r2[x - 1]

    def into(ref, shift=0):
        def emit(x, u, delta, inv, carry):
            ref[x + shift] = u + delta
            return carry

        return emit

    s2, s3 = 0.25**2, 0.25**3
    sweep(ua, r_at, into(ub), 1, N2, s2, mats2, one, None, 0)
    NY2, NZ2, NY3, NZ3 = g2["NY"], g2["NZ"], g3["NY"], g3["NZ"]
    rz = restrict_matrix(iota((NZ2, NZ3), 0), iota((NZ2, NZ3), 1), 0).astype(BF16)
    ry = restrict_matrix(iota((NY3, NY2), 1), iota((NY3, NY2), 0), 1).astype(BF16)

    def defect(x, u, delta, inv, carry):
        g = delta * inv
        gz[x] = g
        return carry + g * g

    total = sweep(ub, r_at, defect, 1, N2, s2, mats2, one, None, jnp.zeros((NY2, NZ2), F32))
    part[...] = jnp.full(part.shape, jnp.sum(total), F32)
    c3v = c3[0:1, :]

    def put(i, value):
        r3[i] = value
        e3a[i + 1] = c3v * value

    restrict(gz, 1, N3, ry, rz, put)
    sweep(e3a, lambda x: r3[x - 1], into(e3b), 1, N3, s3, mats3, one, None, 0)
    pz = prolong_matrix(iota((NZ3, NZ2), 1), iota((NZ3, NZ2), 0), NZ2).astype(BF16)
    py = prolong_matrix(iota((NY2, NY3), 0), iota((NY2, NY3), 1), NY2).astype(BF16)
    prolong_into(e3b, 0, N3 + 2, pz, py, buf, lambda x: ub[x], ua, one)
    sweep(ua, r_at, into(ub), 1, N2, s2, mats2, one, None, 0)
    sweep(ub, r_at, into(u2, pad - 1), 1, N2, s2, mats2, one, None, 0)


def up_kernel(dims, u2, r1, e1, m1h, m1l, c1, rhs, e0, m0h, m0l, c0, sol, res, part,
              va, vb, vbuf, ua, ub, ubuf):
    g0, g1, g2 = geometry(0, dims), geometry(1, dims), geometry(2, dims)
    rows, size = va.shape[1], va.shape[2]
    count = g1["nx"] + 2 * HX[1]
    zero_planes(va, 0, count + 1)
    zero_planes(vb, 0, count + 1)
    xmask = inside_mask(g1["x0"], g1["NX"], HX[1] + 1)
    ymask = y_mask(rows, size, g1["ny"], g1["y0"], g1["NY"])
    NY2, NZ2 = g2["NY"], g2["NZ"]
    pz = prolong_matrix(
        cyclic(iota((NZ2, size), 1), size, g1["nz"]) + g1["z0"], iota((NZ2, size), 0), g1["NZ"]
    ).astype(BF16)
    py = prolong_matrix(
        cyclic(iota((rows, NY2), 0), rows, g1["ny"]) + g1["y0"], iota((rows, NY2), 1), g1["NY"]
    ).astype(BF16)
    first = g2["x0"] + 4 - HX[1] // 2 - 1
    prolong_into(u2, first, count // 2 + 2, pz, py, vbuf, lambda x: e1[x], va, xmask)
    mats = (m1h, m1l, c1)

    def into(ref):
        def emit(x, u, delta, inv, carry):
            ref[x] = u + delta
            return carry

        return emit

    r1_at = lambda x: r1[x - 1]
    q, n1 = HX[1] + 1, g1["nx"]
    sweep(va, r1_at, into(vb), q - 3, n1 + 6, 0.25, mats, xmask, ymask, 0)
    sweep(vb, r1_at, into(va), q - 2, n1 + 4, 0.25, mats, xmask, ymask, 0)
    rows0, size0 = ua.shape[1], ua.shape[2]
    count0 = g0["nx"] + 2 * HX[0]
    nx, ny, nz = g0["nx"], g0["ny"], g0["nz"]
    pad = HX[0] + 1
    zero_planes(ua, 0, count0 + 1)
    zero_planes(ub, 0, count0 + 1)
    xmask0 = inside_mask(g0["x0"], g0["NX"], pad)
    ymask0 = y_mask(rows0, size0, ny, g0["y0"], g0["NY"])
    pz = prolong_matrix(
        cyclic(iota((size, size0), 1), size0, nz) + g0["z0"],
        cyclic(iota((size, size0), 0), size, g1["nz"]) + g1["z0"], g0["NZ"],
    ).astype(BF16)
    py = prolong_matrix(
        cyclic(iota((rows0, rows), 0), rows0, ny) + g0["y0"],
        cyclic(iota((rows0, rows), 1), rows, g1["ny"]) + g1["y0"], g0["NY"],
    ).astype(BF16)
    first = HX[1] + 1 - HX[0] // 2 - 1
    prolong_into(va, first, count0 // 2 + 2, pz, py, ubuf, lambda x: e0[x], ua, xmask0)
    mats0 = (m0h, m0l, c0)
    r0_at = lambda x: rhs[x - 1]
    sweep(ua, r0_at, into(ub), pad - 2, nx + 4, 1.0, mats0, xmask0, ymask0, 0)
    sweep(ub, r0_at, into(ua), pad - 1, nx + 2, 1.0, mats0, xmask0, ymask0, 0)

    def final(x, u, delta, inv, carry):
        g = delta * inv
        sol[x - pad] = u
        res[x - pad] = g
        return carry + g * g

    total = sweep(
        ua, r0_at, final, pad, nx, 1.0, mats0, xmask0, ymask0, jnp.zeros((ny, nz), F32), (ny, 0, nz)
    )
    part[...] = jnp.full(part.shape, jnp.sum(total), F32)


AXES = ("gx", "gy", "gz")
MESH = pl.DeviceIdType.MESH
FIRST, WIDTH = 5 * HALF + 1, 10 * HALF


class Pair:
    def __init__(self, axis, up, down, sends, recvs, slot):
        n, me = lax.axis_size(axis), lax.axis_index(axis)
        self.has_low, self.has_high = me > 0, me < n - 1

        def copy(refs, k, target):
            return pltpu.make_async_remote_copy(
                src_ref=refs[0], dst_ref=refs[1], send_sem=sends.at[k], recv_sem=recvs.at[k],
                device_id={axis: target}, device_id_type=MESH,
            )

        self.up = copy(up, slot, lax.rem(me + 1, n))
        self.down = copy(down, slot + 1, lax.rem(me + n - 1, n))

    def start(self):
        pl.when(self.has_high)(self.up.start)
        pl.when(self.has_low)(self.down.start)

    def wait(self):
        pl.when(self.has_low)(self.up.wait_recv)
        pl.when(self.has_high)(self.down.wait_recv)

    def sent(self):
        pl.when(self.has_high)(self.up.wait_send)
        pl.when(self.has_low)(self.down.wait_send)

    def clear(self, low, high):
        @pl.when(jnp.logical_not(self.has_low))
        def _():
            low[...] = jnp.zeros(low.shape, F32)

        @pl.when(jnp.logical_not(self.has_high))
        def _():
            high[...] = jnp.zeros(high.shape, F32)


class Star:
    def __init__(self, moves, src, dst, sends, recvs):
        gx, gz = lax.axis_size("gx"), lax.axis_size("gz")
        mx, mz = lax.axis_index("gx"), lax.axis_index("gz")
        self.moves = []
        for k, (dx, dz) in enumerate(moves):
            to = (mx + dx >= 0) & (mx + dx < gx) & (mz + dz >= 0) & (mz + dz < gz)
            frm = (mx - dx >= 0) & (mx - dx < gx) & (mz - dz >= 0) & (mz - dz < gz)
            into = dst(-dx, -dz)
            copy = pltpu.make_async_remote_copy(
                src_ref=src(dx, dz), dst_ref=into, send_sem=sends.at[k], recv_sem=recvs.at[k],
                device_id={"gx": lax.rem(mx + dx + gx, gx), "gz": lax.rem(mz + dz + gz, gz)},
                device_id_type=MESH,
            )
            self.moves.append((to, frm, copy, into))

    def clear(self):
        for _, frm, _, into in self.moves:

            @pl.when(jnp.logical_not(frm))
            def _(into=into):
                into[...] = jnp.zeros(into.shape, F32)

    def start(self):
        for to, _, copy, _ in self.moves:
            pl.when(to)(copy.start)

    def wait(self, skew=None):
        chosen = {None: self.moves, True: self.moves[:4], False: self.moves[4:]}[skew]
        for _, frm, copy, _ in chosen:
            pl.when(frm)(copy.wait_recv)

    def sent(self):
        for to, _, copy, _ in self.moves:
            pl.when(to)(copy.wait_send)


SKEW = [(dx, dz) for dx in (-1, 1) for dz in (-1, 1)]
STAR = SKEW + [(0, -1), (0, 1), (-1, 0), (1, 0)]


def star_name(prefix, d):
    return prefix + "mop"[d[0] + 1] + "mop"[d[1] + 1]


def linear():
    gy, gz = lax.axis_size("gy"), lax.axis_size("gz")
    return (lax.axis_index("gx") * gy + lax.axis_index("gy")) * gz + lax.axis_index("gz")


def coordinates(t):
    gy, gz = lax.axis_size("gy"), lax.axis_size("gz")
    return (t // (gy * gz), lax.rem(t // gz, gy), lax.rem(t, gz))


def device_count():
    return lax.axis_size("gx") * lax.axis_size("gy") * lax.axis_size("gz")


def near_devices():
    sizes, me = [lax.axis_size(a) for a in AXES], [lax.axis_index(a) for a in AXES]
    out = []
    for move in [(dx, 0, dz) for dx, dz in STAR] + [(0, -1, 0), (0, 1, 0)]:
        if all(n > 1 or d == 0 for n, d in zip(sizes, move)):
            at = [i + d for i, d in zip(me, move)]
            there = functools.reduce(jnp.logical_and, [(i >= 0) & (i < n) for i, n in zip(at, sizes)])
            out.append((there, tuple(lax.rem(i + n, n) for i, n in zip(at, sizes))))
    return out


def reached():
    return lax.axis_size("gx") <= 4 and lax.axis_size("gy") <= 2 and lax.axis_size("gz") <= 4


def signal_all():
    n, me = device_count(), linear()
    barrier = pltpu.get_barrier_semaphore()
    if reached():
        for there, device in near_devices():

            @pl.when(there)
            def _():
                pl.semaphore_signal(barrier, inc=1, device_id=device, device_id_type=MESH)

        return

    def step(k, carry):
        pl.semaphore_signal(
            barrier, inc=1, device_id=coordinates(lax.rem(me + k, n)), device_id_type=MESH
        )
        return carry

    lax.fori_loop(1, n, step, 0)


def wait_all():
    if reached():
        count = sum(there.astype(jnp.int32) for there, _ in near_devices())
        pl.semaphore_wait(pltpu.get_barrier_semaphore(), count)
        return
    pl.semaphore_wait(pltpu.get_barrier_semaphore(), device_count() - 1)


def shifted(axis, d):
    n = lax.axis_size(axis)
    t = lax.axis_index(axis) + d
    return jnp.where(t >= n, t - n, t)


def arrived(buf, count, sends, recvs, k, axis):
    part = buf.at[0:count]
    return pltpu.make_async_remote_copy(
        src_ref=part, dst_ref=part, send_sem=sends.at[k], recv_sem=recvs.at[k],
        device_id={axis: shifted(axis, 1)}, device_id_type=MESH,
    )


def spread(block, buf, slot, sends, recvs, k, sizes):
    for dx in range(sizes[0]):
        for dy in range(sizes[1]):
            for dz in range(sizes[2]):
                if dx or dy or dz:
                    pltpu.make_async_remote_copy(
                        src_ref=block, dst_ref=buf.at[slot], send_sem=sends.at[k], recv_sem=recvs.at[k],
                        device_id=(shifted("gx", dx), shifted("gy", dy), shifted("gz", dz)),
                        device_id_type=MESH,
                    ).start()


def everyone(block, buf, sends, recvs):
    n, me = device_count(), linear()
    spread(block, buf, me, sends, recvs, 0, [lax.axis_size(a) for a in AXES])
    buf[me] = block[...]
    done = arrived(buf, n - 1, sends, recvs, 0, "gz")
    done.wait_recv()
    return done


def by_columns(block, buf, sends, recvs):
    gx, gy, gz = (lax.axis_size(a) for a in AXES)
    m, y = gx * gz, lax.axis_index("gy")
    slot = y * m + lax.axis_index("gx") * gz + lax.axis_index("gz")
    spread(block, buf, slot, sends, recvs, 0, (gx, 1, gz))
    buf[slot] = block[...]
    first = arrived(buf, m - 1, sends, recvs, 0, "gz")
    mine = buf.at[pl.ds(y * m, m)]
    second = arrived(buf, (gy - 1) * m, sends, recvs, 1, "gy")

    def finish():
        first.wait_recv()
        for d in range(1, gy):
            pltpu.make_async_remote_copy(
                src_ref=mine, dst_ref=mine, send_sem=sends.at[1], recv_sem=recvs.at[1],
                device_id={"gy": shifted("gy", d)}, device_id_type=MESH,
            ).start()
        second.wait_recv()
        return first, second

    return finish


def row_starts(nx, slots):
    per = -(-nx // slots)
    return [i * slots if 2 * i < per else nx - (per - i) * slots for i in range(per)]


def find_plane(nx, slots, x, end):
    starts = row_starts(nx, slots)
    rows = [i for i, v in enumerate(starts) if v <= x < v + slots]
    i = rows[-1] if end else rows[0]
    return i, x - starts[i]


def pack_faces(data, low, high, start, stop):
    nx, ny, nz = data.shape
    width = stop - start
    slots = nz // width
    rest = jnp.zeros((ny, nz - slots * width), F32)
    for i in range(low.shape[0]):
        planes = [row_starts(nx, slots)[i] + k for k in range(slots)]
        low[i] = jnp.concatenate([data[x][:, start:stop] for x in planes] + [rest], axis=1)
        high[i] = jnp.concatenate([data[x][:, nz - stop : nz - start] for x in planes] + [rest], axis=1)


def face_pieces(nx, hx, nz, width):
    slots = nz // width
    per, rim = -(-nx // slots), -(-hx // slots)
    return {-1: slice(0, rim), 0: slice(0, per), 1: slice(per - rim, per)}


def unpack_faces(dims, parts, widths, ext, hx, sides=(-1, 0, 1)):
    nx, ny, nz = dims
    for dx in sides:
        source = nx - hx if dx < 0 else 0
        target = {-1: 0, 0: hx, 1: hx + nx}[dx]
        for i in range(nx if dx == 0 else hx):
            ends = {}
            for dz in (-1, 1):
                ends[dz] = []
                for part, width in zip(parts, widths):
                    slots = nz // width
                    first = -(-nx // slots) - -(-hx // slots) if dx < 0 else 0
                    row, lane = find_plane(nx, slots, source + i, dx < 0)
                    lane = lane * width
                    ends[dz].append(part(dx, dz)[row - first][:, lane : lane + width])
            gap = jnp.zeros((ny, nz - 2 * sum(widths)), F32)
            ext[target + i, 0:ny, nz:] = jnp.concatenate(ends[1] + [gap] + ends[-1][::-1], axis=1)


def whole_kernel(names, dims, data, weights, sol, res, norms, *scratch):
    r = dict(zip(names, scratch))
    nx, ny, nz = dims
    n, gz = device_count(), lax.axis_size("gz")
    ns, nr = r["near_send"], r["near_recv"]
    signal_all()
    pack_faces(data, r["f1_low"], r["f1_high"], 0, FIRST)
    ext, hx, weights_row = r["ext"], HX[0], iota((8, 2 * nz), 0)
    for x in range(nx):
        ext[hx + x, 0:ny, 0:nz] = data[x]
    wait_all()
    near = Pair("gz", (weights, r["w_low"]), (weights, r["w_high"]), ns, nr, 0)
    near.start()
    widths = (FIRST, WIDTH - FIRST)
    pieces = [face_pieces(nx, hx, nz, w) for w in widths]

    def faces(part):
        def send(dx, dz):
            return r["f%d_%s" % (part, "low" if dz < 0 else "high")].at[pieces[part - 1][dx]]

        def take(dx, dz):
            return r[star_name("g%d_" % part, (dx, dz))]

        return send, take

    send1, take1 = faces(1)
    send2, take2 = faces(2)

    def plane_send(dx, dz):
        if dz:
            return send1(dx, dz)
        return data.at[0:hx] if dx < 0 else data.at[nx - hx : nx]

    def plane_take(dx, dz):
        if dz:
            return take1(dx, dz)
        return ext.at[0:hx, 0:ny, 0:nz] if dx < 0 else ext.at[nx + hx : nx + 2 * hx, 0:ny, 0:nz]

    star = Star(STAR, plane_send, plane_take, r["s_send"], r["s_recv"])
    star.start()
    star.clear()
    near.clear(r["w_low"], r["w_high"])
    late = Star(STAR[:6], send2, take2, r["l_send"], r["l_recv"])
    late.clear()
    pack_faces(data, r["f2_low"], r["f2_high"], FIRST, WIDTH)
    level = [[r["m%d%s" % (k, t)] for t in "hlc"] for k in range(4)]
    near.wait()
    nearby = jnp.concatenate([r["w_low"][...], weights[...], r["w_high"][...]], axis=1)
    start = (lax.axis_index("gz") - 1) * nz
    build_level(0, nz, nz * gz, nearby, start, *level[0], r["ah"], r["al"])
    star.wait(False)
    unpack_faces(dims, (take1,), widths[:1], ext, hx, (0,))

    def y_pair(planes, slot):
        return Pair(
            "gy",
            (ext.at[planes, ny - 8 : ny, :], r["y_low"].at[planes]),
            (ext.at[planes, 0:8, :], r["y_high"].at[planes]),
            ns, nr, slot,
        )

    ys = [y_pair(slice(a, b), k) for a, b, k in ((hx, hx + nx, 2), (0, hx, 6), (hx + nx, nx + 2 * hx, 8))]
    ys[0].clear(r["y_low"], r["y_high"])
    ys[0].start()
    star.wait(True)
    late.start()
    unpack_faces(dims, (take1,), widths[:1], ext, hx, (-1, 1))
    for y in ys[1:]:
        y.start()
    for y in ys:
        y.wait()
    star.sent()
    near.sent()
    for y in ys:
        y.sent()
    upper = weights_row < 4

    def join(x, carry):
        ext[x, ny : ny + 8, :] = jnp.where(upper, r["y_high"][x], r["y_low"][x])
        return carry

    lax.fori_loop(0, nx + 2 * hx, join, 0)
    down_kernel(0, dims, ext, r["ah"], r["al"], *level[0], r["rhs"], r["e0"], r["r1"], r["p0"], r["ua"], r["gz0"])
    n1, m1, k1 = nx // 2, ny // 2, nz // 2
    h1 = HX[1]
    x1, r1, own = r["x1"], r["r1"], r["b_own"]
    for a in range(n1 // 2):
        own[a] = jnp.concatenate([r1[2 * a][:, :k1], r1[2 * a + 1][:, :k1]], axis=1)
    bufs = {d: r[star_name("b_", d)] for d in STAR}
    rim = h1 // 2
    cut = {-1: slice(0, rim), 0: slice(0, n1 // 2), 1: slice(n1 // 2 - rim, n1 // 2)}
    star = Star(
        STAR, lambda dx, dz: own.at[cut[dx]], lambda dx, dz: bufs[(dx, dz)], r["b_send"], r["b_recv"]
    )
    star.start()
    star.clear()
    build_level(1, nz, nz * gz, nearby, start, *level[1])
    late.wait()
    unpack_faces(dims, (take1, take2), widths, ext, hx)
    far = slice(nz, 2 * nz)
    late_ys = Pair(
        "gy", (ext.at[:, ny - 8 : ny, far], r["z_low"]), (ext.at[:, 0:8, far], r["z_high"]), ns, nr, 4
    )
    late_ys.clear(r["z_low"], r["z_high"])
    late_ys.start()
    star.wait(False)
    blank = jnp.zeros((m1, k1), F32)
    bufs[(0, 0)] = own

    def widen(dx):
        base = h1 + dx * h1 if dx < 1 else h1 + n1
        for x in range(n1 if dx == 0 else h1):
            a, part = x // 2, slice((x % 2) * k1, (x % 2 + 1) * k1)
            low, mid, high = (bufs[(dx, dz)][a][:, part] for dz in (-1, 0, 1))
            x1[base + x, 0:m1, :] = jnp.concatenate([mid, high, blank, low], axis=1)

    widen(0)
    star.wait(True)
    spread(weights, r["wparts"], lax.axis_index("gz"), r["w_send"], r["w_recv"], 0, (1, 1, gz))
    widen(-1)
    widen(1)
    ys = Pair(
        "gy",
        (x1.at[:, m1 - 8 : m1, :], x1.at[:, m1 + 8 : m1 + 16, :]),
        (x1.at[:, 0:8, :], x1.at[:, m1 : m1 + 8, :]),
        ns, nr, 10,
    )
    ys.clear(x1.at[:, m1 + 8 : m1 + 16, :], x1.at[:, m1 : m1 + 8, :])
    ys.start()
    ys.wait()
    star.sent()
    ys.sent()
    down_kernel(1, dims, x1, *level[1], r["e1"], r["r2"], r["p1"], r["va"], r["gz1"])
    n2, m2, k2 = nx // 4, ny // 4, nz // 4
    slots = nz // k2
    per = n2 // slots
    for a in range(per):
        r["c_own"][a] = jnp.concatenate([r["r2"][q * per + a][:, :k2] for q in range(slots)], axis=1)
    finish = by_columns(r["c_own"], r["c_all"], r["c_send"], r["c_recv"])
    late_ys.wait()

    def late_join(x, carry):
        ext[x, ny : ny + 8, far] = jnp.where(upper[:, far], r["z_high"][x], r["z_low"][x])
        return carry

    lax.fori_loop(0, nx + 2 * hx, late_join, 0)
    late_kernel(dims, ext, r["ah"], r["al"], *level[0], r["rhs"], r["e0"], r["ua"])
    r["wparts"][lax.axis_index("gz")] = weights[...]
    given = arrived(r["wparts"], gz - 1, r["w_send"], r["w_recv"], 0, "gz")
    given.wait_recv()
    wall = jnp.concatenate([r["wparts"][i] for i in range(gz)], axis=1)
    build_level(2, nz, nz * gz, wall, 0, *level[2])
    build_level(3, nz, nz * gz, wall, 0, *level[3])
    gathered = finish()
    gx, gy = lax.axis_size("gx"), lax.axis_size("gy")

    def place(i, carry):
        for j in range(gy):
            for x in range(n2):
                q, a = x // per, x % per
                r["r2all"][i * n2 + x, j * m2 : (j + 1) * m2, :] = jnp.concatenate(
                    [r["c_all"][(j * gx + i) * gz + k, a][:, q * k2 : (q + 1) * k2] for k in range(gz)],
                    axis=1,
                )
        return carry

    lax.fori_loop(0, lax.axis_size("gx"), place, 0)
    coarse_kernel(
        dims, r["r2all"], *level[2], *level[3], r["u2"], r["p2"],
        r["ca"], r["cb"], r["cz"], r["r3"], r["e3a"], r["e3b"], r["cbuf"],
    )
    up_kernel(
        dims, r["u2"], x1, r["e1"], *level[1], r["rhs"], r["e0"], *level[0], sol, res, r["p3"],
        r["va"], r["vb"], r["vbuf"], r["ua"], r["ub"], r["ubuf"],
    )
    for g in gathered + (given,):
        g.wait_send()
    late.sent()
    late_ys.sent()
    lane = iota((1, nz), 1)
    p0, p1, p2, p3 = (r["p%d" % k][0:1, :] for k in range(4))
    mine = jnp.where(lane == 0, p0, jnp.where(lane == 1, p1, p3))
    r["n_own"][...] = mine
    last = everyone(r["n_own"], r["n_all"], r["n_send"], r["n_recv"])
    total = jnp.sum(r["n_all"][...], axis=0)
    cells = float(nx * ny * nz * n)
    total = jnp.where(lane == 2, p2, total)
    scale = jnp.where(lane == 1, 8.0 / cells, jnp.where(lane == 2, 64.0 / cells, 1.0 / cells))
    norms[...] = jnp.sqrt(total * scale)
    last.wait_send()


def body(data, weights):
    dims = data.shape
    nx, ny, nz = dims
    gx, gy, gz = (lax.axis_size(a) for a in AXES)
    n = gx * gy * gz
    c0, y0, l0 = nx + 2 * HX[0], ny + 8, 2 * nz
    c1, y1 = nx // 2 + 2 * HX[1], ny // 2 + 16
    N2 = (nx // 4 * gx, ny // 4 * gy, nz // 4 * gz)
    N3 = tuple(v // 2 for v in N2)
    pad2 = (N2[0] + 2,) + N2[1:]
    pad3 = (N3[0] + 2,) + N3[1:]
    own2 = (nx // 4 // 4, ny // 4, nz)
    shapes = dict(
        ext=(c0, y0, l0), wparts=(gz, 8, nz), w_low=(8, nz), w_high=(8, nz), z_low=(c0, 8, nz), z_high=(c0, 8, nz), y_low=(c0, 8, l0), y_high=(c0, 8, l0),
        rhs=(c0, y0, l0), e0=(c0 + 2, y0, l0), r1=(nx // 2, ny // 2, nz),
        ua=(c0 + 2, y0, l0), ub=(c0 + 2, y0, l0), gz0=(c0 + 2, y0, l0), ubuf=(c0 // 2 + 2, y0, l0),
        b_own=(nx // 4, ny // 2, nz),
        x1=(c1, y1, l0), e1=(c1 + 2, y1, l0), r2=(nx // 4, ny // 4, nz),
        va=(c1 + 2, y1, l0), vb=(c1 + 2, y1, l0), gz1=(c1 + 2, y1, l0), vbuf=(c1 // 2 + 2, y1, l0),
        c_own=own2, c_all=(n,) + own2, r2all=N2, u2=(N2[0] + 8,) + N2[1:],
        ca=pad2, cb=pad2, cz=pad2, r3=N3, e3a=pad3, e3b=pad3,
        cbuf=(N3[0] + 2,) + N2[1:], n_own=(1, nz), n_all=(n, 1, nz),
        p0=(8, nz), p1=(8, nz), p2=(8, nz), p3=(8, nz),
    )
    for part, width in ((1, FIRST), (2, WIDTH - FIRST)):
        planes = {k: v.stop - v.start for k, v in face_pieces(nx, HX[0], nz, width).items()}
        for side in ("low", "high"):
            shapes["f%d_%s" % (part, side)] = (planes[0], ny, nz)
        for d in STAR[:6]:
            shapes[star_name("g%d_" % part, d)] = (planes[-d[0]], ny, nz)
    for d in STAR:
        shapes[star_name("b_", d)] = (HX[1] // 2 if d[0] else nx // 4, ny // 2, nz)
    scratch = {k: pltpu.VMEM(v, F32) for k, v in shapes.items()}
    for k, size in enumerate((l0, l0, N2[2], N3[2])):
        scratch["m%dh" % k] = pltpu.VMEM((size, size), BF16)
        scratch["m%dl" % k] = pltpu.VMEM((size, size), BF16)
        scratch["m%dc" % k] = pltpu.VMEM((8, size), F32)
    scratch["ah"] = scratch["al"] = pltpu.VMEM((l0, l0), BF16)
    dma = pltpu.SemaphoreType.DMA
    scratch.update(near_send=dma((12,)), near_recv=dma((12,)), w_send=dma((1,)), w_recv=dma((1,)))
    for k in "bsl":
        scratch[k + "_send"] = dma((8,))
        scratch[k + "_recv"] = dma((8,))
    for k in "cn":
        scratch[k + "_send"] = dma((2,))
        scratch[k + "_recv"] = dma((2,))
    words = sum(math.prod(v) for v in shapes.values()) + 2 * l0 * l0 * 3 + N2[2] * N2[2] * 2
    vmem = pl.BlockSpec(memory_space=pltpu.VMEM)
    sol, res, norms = pl.pallas_call(
        functools.partial(whole_kernel, tuple(scratch), dims),
        out_shape=[jax.ShapeDtypeStruct(s, F32) for s in (dims, dims, (1, nz))],
        in_specs=[vmem] * 2,
        out_specs=[vmem] * 3,
        scratch_shapes=list(scratch.values()),
        compiler_params=pltpu.CompilerParams(
            collective_id=0, has_side_effects=True, vmem_limit_bytes=4 * words + 6 * 1024 * 1024
        ),
    )(data, weights)
    return sol, res, norms[0, :4]


def solution(mesh):
    in_specs = (P("gx", "gy", "gz"), P(None, "gz"))
    out_specs = (P("gx", "gy", "gz"), P("gx", "gy", "gz"), P())
    return jax.shard_map(body, mesh=mesh, in_specs=in_specs, out_specs=out_specs, check_vma=False)
```
